8 devices in a mesh: dp: 8 (over z, y, x, core).
Axes of the slice: x: 2, y: 2, z: 1, core: 2. Of those that a mesh axis runs over, the one named last changes fastest.
Arguments:
- grad_wq: bfloat16 [8, 2, 896, 896], P('dp')
- grad_wk: bfloat16 [8, 2, 896, 128], P('dp')
- grad_wv: bfloat16 [8, 2, 896, 128], P('dp')
- grad_wo: bfloat16 [8, 2, 896, 896], P('dp')
- grad_gate: bfloat16 [8, 2, 896, 4864], P('dp')
- grad_up: bfloat16 [8, 2, 896, 4864], P('dp')
- grad_down: bfloat16 [8, 2, 4864, 896], P('dp')
- grad_attn_norm: bfloat16 [8, 2, 896], P('dp')
- grad_mlp_norm: bfloat16 [8, 2, 896], P('dp')
- grad_final_norm: bfloat16 [8, 896], P('dp')
- master: float32 [29824000], P('dp')
- exp_avg: float32 [29824000], P('dp')
- exp_avg_sq: float32 [29824000], P('dp')
- learn_rate: float32 [], replicated
Outputs:
- output 1: float32 [29824000], P('dp')
- output 2: float32 [29824000], P('dp')
- output 3: float32 [29824000], P('dp')
- output 4: bfloat16 [2, 896, 896], replicated
- output 5: bfloat16 [2, 896, 128], replicated
- output 6: bfloat16 [2, 896, 128], replicated
- output 7: bfloat16 [2, 896, 896], replicated
- output 8: bfloat16 [2, 896, 4864], replicated
- output 9: bfloat16 [2, 896, 4864], replicated
- output 10: bfloat16 [2, 4864, 896], replicated
- output 11: bfloat16 [2, 896], replicated
- output 12: bfloat16 [2, 896], replicated
- output 13: bfloat16 [896], replicated
- output 14: float32 [], replicated
All inputs are finite; a program needn't handle non-finite values.
Results may differ from the reference program's by a relative error of at most 0.001.
Values sent between devices are 32-bit elements.
A program may use at most 1 GiB of HBM per device.

```python
import math
import jax
import jax.numpy as jnp

DP = 8
LAYERS = 2
D = 896
HEADS = 14
KV_HEADS = 2
HEAD = 64
FF = 4864
STEP = 4

Q_DIM = HEADS * HEAD
KV_DIM = KV_HEADS * HEAD
MATRIX_COUNT = LAYERS * (2 * D * Q_DIM + 2 * D * KV_DIM + 3 * D * FF)
TOTAL = MATRIX_COUNT + 2 * LAYERS * D + D
PADDED = -(-TOTAL // (DP * 128)) * DP * 128
BETA_ONE = 0.9
BETA_TWO = 0.95
ADAM_EPS = 1e-8
WEIGHT_DECAY = 0.1
MAX_NORM = 1.0
CLIP_EPS = 1e-6
BIAS_ONE = 1.0 - BETA_ONE ** STEP
BIAS_TWO = 1.0 - BETA_TWO ** STEP
GRAD_NAMES = ("grad_wq", "grad_wk", "grad_wv", "grad_wo", "grad_gate", "grad_up", "grad_down", "grad_attn_norm", "grad_mlp_norm", "grad_final_norm")


def param_shapes():
    return [(LAYERS, D, Q_DIM), (LAYERS, D, KV_DIM), (LAYERS, D, KV_DIM), (LAYERS, Q_DIM, D), (LAYERS, D, FF), (LAYERS, D, FF), (LAYERS, FF, D), (LAYERS, D), (LAYERS, D), (D,)]


def split_flat(flat_vec):
    tensors = []
    offset = 0
    for piece_shape in param_shapes():
        piece_size = math.prod(piece_shape)
        tensors.append(flat_vec[offset:offset + piece_size].reshape(piece_shape))
        offset += piece_size
    return tensors


def setup_inputs(seed: int = 0) -> dict:
    key_list = jax.random.split(jax.random.key(seed), 15)
    norm_target = 3.0 * jnp.power(3.0, jax.random.uniform(key_list[14], (), jnp.float32))
    grad_scale = norm_target * math.sqrt(DP / TOTAL)
    inputs = {}
    for position, (arg_name, arg_shape) in enumerate(zip(GRAD_NAMES, param_shapes())):
        sample = jax.random.normal(key_list[position], (DP,) + arg_shape, jnp.float32)
        inputs[arg_name] = (grad_scale * sample).astype(jnp.bfloat16)
    valid_mask = (jnp.arange(PADDED) < TOTAL).astype(jnp.float32)
    grad_unit = 1.0 / math.sqrt(TOTAL)
    inputs["master"] = 0.02 * jax.random.normal(key_list[10], (PADDED,), jnp.float32) * valid_mask
    inputs["exp_avg"] = 0.1 * grad_unit * jax.random.normal(key_list[11], (PADDED,), jnp.float32) * valid_mask
    inputs["exp_avg_sq"] = 0.05 * grad_unit * grad_unit * (0.5 + jax.random.uniform(key_list[12], (PADDED,), jnp.float32)) * valid_mask
    inputs["learn_rate"] = 1e-2 * jnp.power(4.0, jax.random.uniform(key_list[13], (), jnp.float32))
    return inputs


def reference(grad_wq, grad_wk, grad_wv, grad_wo, grad_gate, grad_up, grad_down, grad_attn_norm, grad_mlp_norm, grad_final_norm, master, exp_avg, exp_avg_sq, learn_rate):
    local_grads = [grad_wq, grad_wk, grad_wv, grad_wo, grad_gate, grad_up, grad_down, grad_attn_norm, grad_mlp_norm, grad_final_norm]
    pieces = [jnp.sum(local_grad, axis=0, dtype=jnp.float32).reshape(-1) for local_grad in local_grads]
    pieces.append(jnp.zeros((PADDED - TOTAL,), jnp.float32))
    mean_grad = jnp.concatenate(pieces) / DP
    grad_norm = jnp.sqrt(jnp.sum(mean_grad * mean_grad))
    clip_coef = jnp.minimum(1.0, MAX_NORM / (grad_norm + CLIP_EPS))
    clipped = clip_coef * mean_grad
    new_avg = BETA_ONE * exp_avg + (1.0 - BETA_ONE) * clipped
    new_avg_sq = BETA_TWO * exp_avg_sq + (1.0 - BETA_TWO) * clipped * clipped
    decay_mask = (jnp.arange(PADDED) < MATRIX_COUNT).astype(jnp.float32)
    adam_dir = (new_avg / BIAS_ONE) / (jnp.sqrt(new_avg_sq / BIAS_TWO) + ADAM_EPS)
    new_master = master - learn_rate * (WEIGHT_DECAY * decay_mask * master + adam_dir)
    param_wq, param_wk, param_wv, param_wo, param_gate, param_up, param_down, param_attn_norm, param_mlp_norm, param_final_norm = split_flat(new_master[:TOTAL].astype(jnp.bfloat16))
    return (new_master, new_avg, new_avg_sq, param_wq, param_wk, param_wv, param_wo, param_gate, param_up, param_down, param_attn_norm, param_mlp_norm, param_final_norm, grad_norm)
```

```python
import functools
import math
import jax
import jax.numpy as jnp
from jax import lax
from jax.experimental import pallas as pl
from jax.experimental.pallas import tpu as pltpu
from jax.sharding import PartitionSpec as P

BETA_ONE = 0.9
BETA_TWO = 0.95
ADAM_EPS = 1e-8
WEIGHT_DECAY = 0.1
MAX_NORM = 1.0
CLIP_EPS = 1e-6
STEP = 4
BIAS_ONE = 1.0 - BETA_ONE ** STEP
BIAS_TWO = 1.0 - BETA_TWO ** STEP

MESH = pl.DeviceIdType.MESH
F32 = jnp.float32
BF16 = jnp.bfloat16
LANES = 128

SHAPES = [(2, 896, 896), (2, 896, 128), (2, 896, 128), (2, 896, 896), (2, 896, 4864), (2, 896, 4864), (2, 4864, 896)]
NAMES_ROWS = [math.prod(s[:-1]) for s in SHAPES]
WIDTHS = [s[-1] // LANES for s in SHAPES]
OFFSETS = [sum(r * w for r, w in zip(NAMES_ROWS[:t], WIDTHS[:t])) for t in range(7)]
BLOCK_ROWS = [448, 1792, 1792, 448, 128, 128, 608]
MATRIX_ROWS = 232960
FLAT_ROWS = 233000
SEG = 29125
NDEV = 8

BLOCKS = [(t, b, BLOCK_ROWS[t]) for t in range(7) for b in range(0, NAMES_ROWS[t], BLOCK_ROWS[t])]
STAGE_ROWS = max(br * WIDTHS[t] for t, br in enumerate(BLOCK_ROWS))

ANY = pl.BlockSpec(memory_space=pl.ANY)
VMEM_SPEC = pl.BlockSpec(memory_space=pltpu.VMEM)
SMEM_SPEC = pl.BlockSpec(memory_space=pltpu.SMEM)
DMA = pltpu.SemaphoreType.DMA


def tile_scratch(slots, dtype):
    return [pltpu.VMEM((slots, 128, 4864), dtype), pltpu.VMEM((slots, 608, 896), dtype), pltpu.VMEM((slots, 1792, 128), dtype)]


def width_slot(width):
    return {38: 0, 7: 1, 1: 2}[width]


def pack_kernel(*refs):
    grads, norms, flat = refs[:7], refs[7:10], refs[10]
    tiles, stage, tail, in_sem, out_sem, tail_sem = refs[11:14], refs[14], refs[15], refs[16], refs[17], refs[18]

    def load(b):
        t, row, rows = BLOCKS[b]
        return pltpu.make_async_copy(grads[t].at[pl.ds(row, rows)], tiles[width_slot(WIDTHS[t])].at[b % 2, pl.ds(0, rows)], in_sem.at[b % 2])

    def store(b):
        t, row, rows = BLOCKS[b]
        w = WIDTHS[t]
        return pltpu.make_async_copy(stage.at[b % 2, pl.ds(0, rows * w)], flat.at[pl.ds(OFFSETS[t] + row * w, rows * w), 0], out_sem.at[b % 2])

    load(0).start()
    load(1).start()
    tail[...] = jnp.zeros_like(tail)
    for n, base in ((0, 0), (1, 14)):
        for layer in range(2):
            for j in range(7):
                tail[base + layer * 7 + j:base + layer * 7 + j + 1, :] = norms[n][layer:layer + 1, j * LANES:(j + 1) * LANES].astype(F32)
    for j in range(7):
        tail[28 + j:29 + j, :] = norms[2][:, j * LANES:(j + 1) * LANES].astype(F32)
    tail_copy = pltpu.make_async_copy(tail, flat.at[pl.ds(MATRIX_ROWS, 40), 0], tail_sem)
    tail_copy.start()
    for b, (t, row, rows) in enumerate(BLOCKS):
        w = WIDTHS[t]
        tile = tiles[width_slot(w)]
        group = 16 if w == 38 else (32 if w == 7 else 128)
        load(b).wait()
        if b >= 2:
            store(b - 2).wait()

        @pl.loop(0, rows // group)
        def _(i):
            for j in range(w):
                block = tile[b % 2, pl.ds(pl.multiple_of(i * group, 16), group), j * LANES:(j + 1) * LANES].astype(F32)
                if w == 1:
                    stage[b % 2, pl.ds(pl.multiple_of(i * group, 16), group), :] = block
                else:
                    stage[b % 2, pl.ds(i * (group * w) + j, group, stride=w), :] = block

        store(b).start()
        if b + 2 < len(BLOCKS):
            load(b + 2).start()
    tail_copy.wait()
    store(len(BLOCKS) - 2).wait()
    store(len(BLOCKS) - 1).wait()


def pack(grads, norms):
    return pl.pallas_call(
        pack_kernel,
        name="pack",
        out_shape=jax.ShapeDtypeStruct((FLAT_ROWS, 1, LANES), F32),
        in_specs=[ANY] * 7 + [VMEM_SPEC] * 3,
        out_specs=ANY,
        scratch_shapes=tile_scratch(2, BF16) + [pltpu.VMEM((2, STAGE_ROWS, LANES), F32), pltpu.VMEM((40, LANES), F32), DMA((2,)), DMA((2,)), DMA],
        compiler_params=pltpu.CompilerParams(vmem_limit_bytes=40 * 1024 * 1024),
        cost_estimate=pl.CostEstimate(flops=FLAT_ROWS * 128, bytes_accessed=FLAT_ROWS * 128 * 6, transcendentals=0),
    )(*grads, *norms)


def unpack_kernel(flat, *refs):
    outs, norms = refs[:7], refs[7:10]
    tiles, stage, tail, in_sem, out_sem, tail_sem = refs[10:13], refs[13], refs[14], refs[15], refs[16], refs[17]

    def load(b):
        t, row, rows = BLOCKS[b]
        w = WIDTHS[t]
        return pltpu.make_async_copy(flat.at[pl.ds(OFFSETS[t] + row * w, rows * w), 0], stage.at[b % 2, pl.ds(0, rows * w)], in_sem.at[b % 2])

    def store(b):
        t, row, rows = BLOCKS[b]
        return pltpu.make_async_copy(tiles[width_slot(WIDTHS[t])].at[b % 2, pl.ds(0, rows)], outs[t].at[pl.ds(row, rows)], out_sem.at[b % 2])

    tail_copy = pltpu.make_async_copy(flat.at[pl.ds(MATRIX_ROWS, 40), 0], tail, tail_sem)
    tail_copy.start()
    load(0).start()
    load(1).start()
    tail_copy.wait()
    for n, base in ((0, 0), (1, 14)):
        for j in range(7):
            pair = jnp.concatenate([tail[base + j:base + j + 1, :], tail[base + 7 + j:base + 8 + j, :]], axis=0)
            norms[n][:, j * LANES:(j + 1) * LANES] = pair.astype(BF16)
    for j in range(7):
        norms[2][:, j * LANES:(j + 1) * LANES] = tail[28 + j:29 + j, :].astype(BF16)
    for b, (t, row, rows) in enumerate(BLOCKS):
        w = WIDTHS[t]
        tile = tiles[width_slot(w)]
        group = 16 if w == 38 else (32 if w == 7 else 128)
        load(b).wait()
        if b >= 2:
            store(b - 2).wait()

        @pl.loop(0, rows // group)
        def _(i):
            for j in range(w):
                if w == 1:
                    block = stage[b % 2, pl.ds(pl.multiple_of(i * group, 16), group), :]
                else:
                    block = stage[b % 2, pl.ds(i * (group * w) + j, group, stride=w), :]
                tile[b % 2, pl.ds(pl.multiple_of(i * group, 16), group), j * LANES:(j + 1) * LANES] = block.astype(BF16)

        store(b).start()
        if b + 2 < len(BLOCKS):
            load(b + 2).start()
    store(len(BLOCKS) - 2).wait()
    store(len(BLOCKS) - 1).wait()


def unpack(flat):
    shapes = [jax.ShapeDtypeStruct((r, w * LANES), BF16) for r, w in zip(NAMES_ROWS, WIDTHS)]
    shapes += [jax.ShapeDtypeStruct((2, 896), BF16)] * 2 + [jax.ShapeDtypeStruct((1, 896), BF16)]
    return pl.pallas_call(
        unpack_kernel,
        name="unpack",
        out_shape=shapes,
        in_specs=[ANY],
        out_specs=[ANY] * 7 + [VMEM_SPEC] * 3,
        scratch_shapes=tile_scratch(2, BF16) + [pltpu.VMEM((2, STAGE_ROWS, LANES), F32), pltpu.VMEM((40, LANES), F32), DMA((2,)), DMA((2,)), DMA],
        compiler_params=pltpu.CompilerParams(vmem_limit_bytes=40 * 1024 * 1024),
        cost_estimate=pl.CostEstimate(flops=FLAT_ROWS * 128, bytes_accessed=FLAT_ROWS * 128 * 6, transcendentals=0),
    )(flat)


def neighbours():
    me = lax.axis_index("dp")
    core, x, y = lax.rem(me, 2), lax.rem(me // 2, 2), me // 4
    other = 1 - 2 * core
    step_x, step_y = 2 - 4 * x, 4 - 8 * y
    return me, other, me + step_x, me + step_y, me + step_x + step_y


RS_ROWS = 1821
RS_HALF_START = SEG - 8 * RS_ROWS
KIND_D, KIND_N, KIND_S, KIND_O = range(4)


def reduce_kernel(flat, g_out, norm_out, land_p, land_d, land_n, land_s,
                  mine, part, first, second, sums, g_buf, ss, ss_all,
                  p_send, p_recv, i_send, i_recv, load_sem, g_sem, ss_send, ss_recv):
    me, other, dev_x, dev_y, dev_d = neighbours()
    barrier = pltpu.get_barrier_semaphore()
    for d in range(1, NDEV):
        pl.semaphore_signal(barrier, inc=1, device_id=(lax.rem(me + d, NDEV),), device_id_type=MESH)
    pl.semaphore_wait(barrier, NDEV - 1)

    def segment(kind, h):
        return ((dev_d, dev_d), (dev_x, dev_y), (dev_y, dev_x), (me, me))[kind][h]

    def start_row(h, i):
        return RS_HALF_START * h + RS_ROWS * i

    def partner_copy(kind, h, i):
        row = SEG * (segment(kind, h) + other) + start_row(h, i)
        return pltpu.make_async_remote_copy(
            src_ref=flat.at[pl.ds(row, RS_ROWS)], dst_ref=land_p.at[kind, h, i],
            send_sem=p_send.at[kind, h, i], recv_sem=p_recv.at[kind, h, i],
            device_id=(me + other,), device_id_type=MESH)

    def link_copy(kind, h, i):
        land = (land_d, land_n, land_s)[kind]
        to = ((dev_x, dev_y), (dev_x, dev_y), (dev_y, dev_x))[kind][h]
        return pltpu.make_async_remote_copy(
            src_ref=sums.at[kind, h, i], dst_ref=land.at[h, i, pl.ds(0, RS_ROWS), 0],
            send_sem=i_send.at[kind, h, i], recv_sem=i_recv.at[kind, h, i],
            device_id=(to,), device_id_type=MESH)

    def load_mine(kind, h, i):
        row = SEG * segment(kind, h) + start_row(h, i)
        return pltpu.make_async_copy(flat.at[pl.ds(row, RS_ROWS), 0], mine.at[h], load_sem.at[0, h])

    def load_part(kind, h, i):
        return pltpu.make_async_copy(land_p.at[kind, h, i, pl.ds(0, RS_ROWS), 0], part.at[h], load_sem.at[1, h])

    def load_link(land, buf, n, h, i):
        return pltpu.make_async_copy(land.at[h, i, pl.ds(0, RS_ROWS), 0], buf.at[h], load_sem.at[n, h])

    def store_g(h, i):
        return pltpu.make_async_copy(g_buf.at[h], g_out.at[pl.ds(start_row(h, i), RS_ROWS), 0], g_sem.at[h])

    @pl.loop(0, 8)
    def _(i):
        for h in range(2):
            partner_copy(KIND_D, h, i).start()

    for kind in (KIND_D, KIND_N, KIND_S):
        @pl.loop(0, 8)
        def _(i):
            for h in range(2):
                load_mine(kind, h, i).start()
                partner_copy(kind + 1, h, i).start()
            for h in range(2):
                partner_copy(kind, h, i).wait_recv()
                load_part(kind, h, i).start()
                if kind == KIND_S:
                    link_copy(KIND_D, h, i).wait_recv()
                    load_link(land_d, first, 2, h, i).start()
            for h in range(2):
                load_mine(kind, h, i).wait()
                load_part(kind, h, i).wait()
                total = mine[h] + part[h]
                if kind == KIND_S:
                    load_link(land_d, first, 2, h, i).wait()
                    total = total + first[h]
                sums[kind, h, i] = total
                link_copy(kind, h, i).start()

    def last(i, acc):
        for h in range(2):
            load_mine(KIND_O, h, i).start()
            partner_copy(KIND_O, h, i).wait_recv()
            load_part(KIND_O, h, i).start()
        for h in range(2):
            link_copy(KIND_N, h, i).wait_recv()
            load_link(land_n, first, 2, h, i).start()
        for h in range(2):
            link_copy(KIND_S, h, i).wait_recv()
            load_link(land_s, second, 3, h, i).start()
            load_mine(KIND_O, h, i).wait()
            load_part(KIND_O, h, i).wait()
            load_link(land_n, first, 2, h, i).wait()
            load_link(land_s, second, 3, h, i).wait()

            @pl.when(i > 0)
            def _():
                store_g(h, i - 1).wait()

            g = ((mine[h] + part[h]) + (first[h] + second[h])) * (1.0 / NDEV)
            g_buf[h] = g
            store_g(h, i).start()
            square = g * g
            if h == 1:
                row = lax.broadcasted_iota(jnp.int32, (RS_ROWS, LANES), 0) + RS_ROWS * i
                square = jnp.where(row >= 8 * RS_ROWS - RS_HALF_START, square, 0.0)
            acc = acc + jnp.sum(square, axis=0, keepdims=True)
        return acc

    acc = lax.fori_loop(0, 8, last, jnp.zeros((1, LANES), F32))
    ss[...] = jnp.broadcast_to(acc, (8, LANES))
    for h in range(2):
        store_g(h, 7).wait()

    @pl.loop(0, 8)
    def _(i):
        for h in range(2):
            for kind in range(4):
                partner_copy(kind, h, i).wait_send()
            for kind in range(3):
                link_copy(kind, h, i).wait_send()

    def norm_copy(d):
        return pltpu.make_async_remote_copy(
            src_ref=ss, dst_ref=ss_all.at[d], send_sem=ss_send.at[d], recv_sem=ss_recv.at[d],
            device_id=(lax.rem(me + d, NDEV),), device_id_type=MESH)

    for d in range(1, NDEV):
        norm_copy(d).start()
    ss_all[0] = ss[...]
    for d in range(1, NDEV):
        norm_copy(d).wait()
    total = jnp.zeros((8, LANES), F32)
    for dev in range(NDEV):
        total = total + ss_all[lax.rem(me - dev + NDEV, NDEV)]
    norm_out[...] = jnp.broadcast_to(jnp.sqrt(jnp.sum(total, axis=1, keepdims=True)), (8, LANES))


def reduce_grads(flat):
    land = jax.ShapeDtypeStruct((2, 8, RS_ROWS, 1, LANES), F32)
    buf = pltpu.VMEM((2, RS_ROWS, LANES), F32)
    outs = pl.pallas_call(
        reduce_kernel,
        name="reduce_grads",
        out_shape=[jax.ShapeDtypeStruct((SEG, 1, LANES), F32), jax.ShapeDtypeStruct((8, LANES), F32),
                   jax.ShapeDtypeStruct((4, 2, 8, RS_ROWS, 1, LANES), F32), land, land, land],
        in_specs=[ANY],
        out_specs=[ANY, VMEM_SPEC, ANY, ANY, ANY, ANY],
        scratch_shapes=[buf, buf, buf, buf, pltpu.VMEM((3, 2, 8, RS_ROWS, LANES), F32), buf,
                        pltpu.VMEM((8, LANES), F32), pltpu.VMEM((NDEV, 8, LANES), F32),
                        DMA((4, 2, 8)), DMA((4, 2, 8)), DMA((3, 2, 8)), DMA((3, 2, 8)), DMA((4, 2)), DMA((2,)), DMA((NDEV,)), DMA((NDEV,))],
        compiler_params=pltpu.CompilerParams(collective_id=0, has_side_effects=True, vmem_limit_bytes=63 * 1024 * 1024),
        cost_estimate=pl.CostEstimate(flops=10 ** 9, bytes_accessed=4 * 10 ** 8, transcendentals=0),
    )(flat)
    return outs[0], outs[1]


def adam_rows(g, m, v, p, norm_row, lr, decay):
    clip = jnp.minimum(1.0, MAX_NORM / (norm_row + CLIP_EPS))
    clipped = clip * g
    new_m = BETA_ONE * m + (1.0 - BETA_ONE) * clipped
    new_v = BETA_TWO * v + (1.0 - BETA_TWO) * clipped * clipped
    adam_dir = (new_m / BIAS_ONE) / (jnp.sqrt(new_v / BIAS_TWO) + ADAM_EPS)
    decay_term = jnp.where(decay, WEIGHT_DECAY * p, 0.0)
    return p - lr * (decay_term + adam_dir), new_m, new_v


UP_ROWS = 1824
UP_LAST = SEG - 15 * UP_ROWS
SUB = 152


def decay_rows(me, start, rows):
    return lax.broadcasted_iota(jnp.int32, (rows, LANES), 0) + (SEG * me + start) < MATRIX_ROWS


def gather_kernel(g, m, v, p, norm, lr, full, gb, mb, vb, pb, new_p,
                  load_sem, own_sem, own_send, own_recv, fwd_send, fwd_recv, p_send, p_recv):
    me, other, dev_x, dev_y, dev_d = neighbours()
    partner = me + other
    barrier = pltpu.get_barrier_semaphore()
    for dev in (partner, dev_x, dev_y):
        pl.semaphore_signal(barrier, inc=1, device_id=(dev,), device_id_type=MESH)
    pl.semaphore_wait(barrier, 3)
    to = (dev_x, dev_y, partner)
    sources = (me, dev_x, dev_y, dev_d)

    def start_row(h, i):
        return UP_ROWS * (8 * h + i)

    def size(h, i):
        return UP_LAST if h == 1 and not isinstance(i, jax.Array) and i == 7 else UP_ROWS

    def rows_of(dev, h, i):
        return full.at[pl.ds(SEG * dev + start_row(h, i), size(h, i)), 0]

    def loads(h, i):
        rows = size(h, i)
        start = pl.multiple_of(start_row(h, i), 8)
        copies = [pltpu.make_async_copy(g.at[pl.ds(start_row(h, i), rows), 0], gb.at[h, pl.ds(0, rows)], load_sem.at[0, h])]
        for n, (src, buf) in enumerate(((m, mb), (v, vb), (p, pb))):
            copies.append(pltpu.make_async_copy(src.at[pl.ds(start, rows)], buf.at[h, pl.ds(0, rows)], load_sem.at[n + 1, h]))
        return copies

    def own_copy(n, h, i):
        return pltpu.make_async_remote_copy(
            src_ref=new_p.at[h, i, pl.ds(0, size(h, i))], dst_ref=rows_of(me, h, i),
            send_sem=own_send.at[n, h, i], recv_sem=own_recv.at[n, h, i], device_id=(to[n],), device_id_type=MESH)

    def own_store(h, i):
        return pltpu.make_async_copy(new_p.at[h, i, pl.ds(0, size(h, i))], rows_of(me, h, i), own_sem.at[h, i])

    def forward(h, i):
        src = rows_of((dev_y, dev_x)[h], h, i)
        return pltpu.make_async_remote_copy(
            src_ref=src, dst_ref=src, send_sem=fwd_send.at[h, i], recv_sem=fwd_recv.at[h, i],
            device_id=((dev_x, dev_y)[h],), device_id_type=MESH)

    def arrival(n, h, i):
        src = rows_of((dev_x, dev_y, partner)[n], h, i)
        return pltpu.make_async_remote_copy(
            src_ref=src, dst_ref=src, send_sem=own_send.at[n, h, i], recv_sem=own_recv.at[n, h, i],
            device_id=(to[n],), device_id_type=MESH)

    def forward_arrival(h, i):
        src = rows_of(dev_d, h, i)
        return pltpu.make_async_remote_copy(
            src_ref=src, dst_ref=src, send_sem=fwd_send.at[h, i], recv_sem=fwd_recv.at[h, i],
            device_id=((dev_x, dev_y)[h],), device_id_type=MESH)

    def partner_copy(q, h, i):
        src = rows_of(sources[q], h, i)
        return pltpu.make_async_remote_copy(
            src_ref=src, dst_ref=src, send_sem=p_send.at[q - 1, h, i], recv_sem=p_recv.at[q - 1, h, i],
            device_id=(partner,), device_id_type=MESH)

    def partner_arrival(q, h, i):
        src = rows_of(sources[q] + other, h, i)
        return pltpu.make_async_remote_copy(
            src_ref=src, dst_ref=src, send_sem=p_send.at[q - 1, h, i], recv_sem=p_recv.at[q - 1, h, i],
            device_id=(partner,), device_id_type=MESH)

    def each(body):
        @pl.loop(0, 7)
        def _(i):
            body(i)

        body(7)

    norm_row = norm[0:1, :]
    for h in range(2):
        for copy in loads(h, 0):
            copy.start()

    def update(i):
        for h in range(2):
            for copy in loads(h, i):
                copy.wait()

            @pl.loop(0, UP_ROWS // SUB)
            def _(s):
                start = pl.multiple_of(s * SUB, 8)
                sub = pl.ds(start, SUB)
                new_p[h, i, sub] = adam_rows(gb[h, sub], mb[h, sub], vb[h, sub], pb[h, sub], norm_row, lr[0],
                                             decay_rows(me, start_row(h, i) + start, SUB))[0]

            for n in ((1, 0, 2) if h == 0 else (0, 1, 2)):
                own_copy(n, h, i).start()
            own_store(h, i).start()
            if isinstance(i, int):
                continue
            for last in (False, True):
                @pl.when((i == 6) == last)
                def _():
                    for copy in loads(h, 7 if last else i + 1):
                        copy.start()

    each(update)

    def pass_on(i):
        arrival(1, 0, i).wait_recv()
        forward(0, i).start()
        partner_copy(2, 0, i).start()
        arrival(0, 1, i).wait_recv()
        forward(1, i).start()
        partner_copy(1, 1, i).start()
        arrival(0, 0, i).wait_recv()
        partner_copy(1, 0, i).start()
        arrival(1, 1, i).wait_recv()
        partner_copy(2, 1, i).start()

    each(pass_on)

    def pass_last(i):
        for h in range(2):
            forward_arrival(h, i).wait_recv()
            partner_copy(3, h, i).start()

    each(pass_last)

    def finish(i):
        for h in range(2):
            own_store(h, i).wait()
            arrival(2, h, i).wait_recv()
            for n in range(3):
                own_copy(n, h, i).wait_send()
            forward(h, i).wait_send()
            for q in range(1, 4):
                partner_copy(q, h, i).wait_send()
                partner_arrival(q, h, i).wait_recv()

    each(finish)


def gather_params(g, m, v, p, norm, lr):
    buf = pltpu.VMEM((2, UP_ROWS, LANES), F32)
    return pl.pallas_call(
        gather_kernel,
        name="gather_params",
        out_shape=jax.ShapeDtypeStruct((FLAT_ROWS, 1, LANES), F32),
        in_specs=[ANY] * 4 + [VMEM_SPEC, SMEM_SPEC],
        out_specs=ANY,
        scratch_shapes=[buf, buf, buf, buf, pltpu.VMEM((2, 8, UP_ROWS, LANES), F32),
                        DMA((4, 2)), DMA((2, 8)), DMA((3, 2, 8)), DMA((3, 2, 8)), DMA((2, 8)), DMA((2, 8)), DMA((3, 2, 8)), DMA((3, 2, 8))],
        compiler_params=pltpu.CompilerParams(collective_id=1, has_side_effects=True, vmem_limit_bytes=48 * 1024 * 1024),
        cost_estimate=pl.CostEstimate(flops=10 ** 9, bytes_accessed=4 * 10 ** 8, transcendentals=0),
    )(g, m, v, p, norm, lr)


def state_kernel(g, m, v, p, norm, lr, new_p, new_m, new_v, gb, g_sem):
    me = lax.axis_index("dp")
    i = pl.program_id(0)

    def load(j, last):
        rows = UP_LAST if last else UP_ROWS
        return pltpu.make_async_copy(g.at[pl.ds(j * UP_ROWS, rows), 0], gb.at[lax.rem(j, 2), pl.ds(0, rows)], g_sem.at[lax.rem(j, 2)])

    @pl.when(i == 0)
    def _():
        load(i, False).start()

    @pl.when(i < 14)
    def _():
        load(i + 1, False).start()

    @pl.when(i == 14)
    def _():
        load(i + 1, True).start()

    @pl.when(i < 15)
    def _():
        load(i, False).wait()

    @pl.when(i == 15)
    def _():
        load(i, True).wait()

    norm_row = norm[0:1, :]

    @pl.loop(0, UP_ROWS // SUB)
    def _(s):
        start = pl.multiple_of(s * SUB, 8)
        rows = pl.ds(start, SUB)
        new_p[rows], new_m[rows], new_v[rows] = adam_rows(
            gb[lax.rem(i, 2), rows], m[rows], v[rows], p[rows], norm_row, lr[0], decay_rows(me, i * UP_ROWS + start, SUB))


def new_state(g, m, v, p, norm, lr):
    block = pl.BlockSpec((UP_ROWS, LANES), lambda i: (i, 0))
    return pl.pallas_call(
        state_kernel,
        name="new_state",
        grid=(16,),
        out_shape=[jax.ShapeDtypeStruct((SEG, LANES), F32)] * 3,
        in_specs=[ANY, block, block, block, pl.BlockSpec((8, LANES), lambda i: (0, 0)), SMEM_SPEC],
        out_specs=[block] * 3,
        scratch_shapes=[pltpu.VMEM((2, UP_ROWS, LANES), F32), DMA((2,))],
        compiler_params=pltpu.CompilerParams(vmem_limit_bytes=32 * 1024 * 1024),
        cost_estimate=pl.CostEstimate(flops=20 * SEG * 128, bytes_accessed=28 * SEG * 128, transcendentals=0),
    )(g, m, v, p, norm, lr)


def solution(mesh):
    def local_step(*arrays):
        grads = [a.reshape(r, w * LANES) for a, r, w in zip(arrays[:7], NAMES_ROWS, WIDTHS)]
        norms = [arrays[7].reshape(2, 896), arrays[8].reshape(2, 896), arrays[9].reshape(1, 896)]
        master, exp_avg, exp_avg_sq = [a.reshape(SEG, LANES) for a in arrays[10:13]]
        lr = arrays[13].reshape(1)
        flat = pack(grads, norms)
        g, norm = reduce_grads(flat)
        full = gather_params(g, exp_avg, exp_avg_sq, master, norm, lr)
        state = new_state(g, exp_avg, exp_avg_sq, master, norm, lr)
        params = unpack(full)
        shapes = SHAPES + [(2, 896), (2, 896), (896,)]
        return tuple([a.reshape(-1) for a in state] + [a.reshape(s) for a, s in zip(params, shapes)] + [norm[0, 0]])

    return jax.shard_map(local_step, mesh=mesh, in_specs=(P("dp"),) * 13 + (P(),), out_specs=(P("dp"),) * 3 + (P(),) * 11, check_vma=False)
```

```python
import functools
import math
import jax
import jax.numpy as jnp
from jax import lax
from jax.experimental import pallas as pl
from jax.experimental.pallas import tpu as pltpu
from jax.sharding import PartitionSpec as P

BETA_ONE = 0.9
BETA_TWO = 0.95
ADAM_EPS = 1e-8
WEIGHT_DECAY = 0.1
MAX_NORM = 1.0
CLIP_EPS = 1e-6
STEP = 4
BIAS_ONE = 1.0 - BETA_ONE ** STEP
BIAS_TWO = 1.0 - BETA_TWO ** STEP

MESH = pl.DeviceIdType.MESH
F32 = jnp.float32
BF16 = jnp.bfloat16
LANES = 128

LAYERS, D, KV, FF = 2, 896, 128, 4864
SHAPES = [(LAYERS, D, D), (LAYERS, D, KV), (LAYERS, D, KV), (LAYERS, D, D), (LAYERS, D, FF), (LAYERS, D, FF), (LAYERS, FF, D)]
GAINS = [(LAYERS, D), (LAYERS, D), (1, D)]
TAIL = 40
HALVES, TENSORS, COLUMNS = range(2), range(7), range(7)
NAMES_ROWS = [math.prod(s[:-1]) for s in SHAPES]
WIDTHS = [s[-1] // LANES for s in SHAPES]
OFFSETS = [sum(r * w for r, w in zip(NAMES_ROWS[:t], WIDTHS[:t])) for t in TENSORS]
BLOCK_ROWS = [448, 1792, 1792, 448, 128, 128, 608]
MATRIX_ROWS = 232960
FLAT_ROWS = 233000
SEG = 29125
NDEV = 8

WIDTH_ORDER = (38, 7, 1)
GROUPS = {38: (16,), 7: (16, 32, 64), 1: (16, 128, 256)}
STAGE_ROWS = max(br * WIDTHS[t] for t, br in enumerate(BLOCK_ROWS))

def split(refs, counts):
    refs = list(refs)
    return [[refs.pop(0) for _ in range(n)] for n in counts]


ANY = pl.BlockSpec(memory_space=pl.ANY)
VMEM_SPEC = pl.BlockSpec(memory_space=pltpu.VMEM)
SMEM_SPEC = pl.BlockSpec(memory_space=pltpu.SMEM)
DMA = pltpu.SemaphoreType.DMA
VMEM_LIMIT = 63 * 1024 * 1024
COST = pl.CostEstimate(flops=2 * 10 ** 8, bytes_accessed=10 ** 8, transcendentals=0)


def tile_scratch(slots, rows):
    return [pltpu.VMEM((slots, r, w * LANES), BF16) for r, w in zip(rows, WIDTH_ORDER)]


def width_slot(width):
    return WIDTH_ORDER.index(width)


def row_group(rows, width):
    return max(g for g in GROUPS[width] if rows % g == 0)


PIECE = 912
PIECES = 32
LATE_FIRST, LATE_END = 25, 31
LATE_ROWS = PIECE * (LATE_END - LATE_FIRST) + 16
PIECE_LAST = SEG - (PIECES - 1) * PIECE
HALF = (PIECES - LATE_END + LATE_FIRST) // 2
LATE_RANGES = [((SEG * s + PIECE * LATE_FIRST) // 8 * 8, -(-(SEG * s + PIECE * LATE_END) // 8) * 8) for s in range(NDEV)]


def unpack_blocks():
    early, late = [], []
    for t in TENSORS:
        w, offset, total = WIDTHS[t], OFFSETS[t], NAMES_ROWS[t]
        cuts = {0, total}
        spans = []
        for low, high in LATE_RANGES:
            first = max(0, (low - offset) // (16 * w) * 16)
            end = min(total, -(-(high - offset) // (16 * w)) * 16)
            if first < end:
                spans.append((first, end))
                cuts |= {first, end}
        cuts = sorted(cuts)
        for begin, end in zip(cuts[:-1], cuts[1:]):
            is_late = any(first <= begin and end <= last for first, last in spans)
            count = -(-(end - begin) // BLOCK_ROWS[t])
            step = -(-(end - begin) // (16 * count)) * 16
            for row in range(begin, end, step):
                rows = min(step, end - row)
                low, high = offset + row * w, offset + (row + rows) * w
                edges = sorted({low, high} | {e for r in LATE_RANGES for e in r if low < e < high})
                sources = []
                for e0, e1 in zip(edges[:-1], edges[1:]):
                    seg = [s for s, (l, h) in enumerate(LATE_RANGES) if l <= e0 and e1 <= h]
                    start = LATE_ROWS * seg[0] + e0 - SEG * seg[0] - PIECE * LATE_FIRST + 8 if seg else e0
                    sources.append((bool(seg), start, e0 - low, e1 - e0))
                (late if is_late else early).append((t, row, rows, sources))
    return early, late


EARLY_BLOCKS, LATE_BLOCKS = unpack_blocks()
LATE_TENSORS = sorted({t for t, _, _, _ in LATE_BLOCKS})
SLOTS = 4


def unpack_body(blocks, sources, outs, tiles, stage, in_sem, out_sem):
    def loads(b):
        return [pltpu.make_async_copy(sources[late].at[pl.ds(start, rows), 0], stage.at[b % SLOTS, pl.ds(to, rows)], in_sem.at[b % SLOTS, n])
                for n, (late, start, to, rows) in enumerate(blocks[b][3])]

    def store(b):
        t, row, rows, _ = blocks[b]
        return pltpu.make_async_copy(tiles[width_slot(WIDTHS[t])].at[b % SLOTS, pl.ds(0, rows)], outs[t].at[pl.ds(row, rows)], out_sem.at[b % SLOTS])

    for b in range(min(SLOTS, len(blocks))):
        for copy in loads(b):
            copy.start()
    yield
    for b, (t, row, rows, _) in enumerate(blocks):
        w = WIDTHS[t]
        tile = tiles[width_slot(w)]
        group = row_group(rows, w)
        for copy in loads(b):
            copy.wait()
        if b >= SLOTS:
            store(b - SLOTS).wait()

        @pl.loop(0, rows // group)
        def _(i):
            for j in range(w):
                if w == 1:
                    block = stage[b % SLOTS, pl.ds(pl.multiple_of(i * group, 16), group), :]
                else:
                    block = stage[b % SLOTS, pl.ds(i * (group * w) + j, group, stride=w), :]
                tile[b % SLOTS, pl.ds(pl.multiple_of(i * group, 16), group), pl.ds(j * LANES, LANES)] = block.astype(BF16)

        store(b).start()
        if b + SLOTS < len(blocks):
            for copy in loads(b + SLOTS):
                copy.start()
    for b in range(max(0, len(blocks) - SLOTS), len(blocks)):
        store(b).wait()


UNPACK_SCRATCH = tile_scratch(SLOTS, (128, 608, 1792)) + [pltpu.VMEM((SLOTS, STAGE_ROWS, LANES), F32)]
TENSOR_TYPES = [jax.ShapeDtypeStruct((r, w * LANES), BF16) for r, w in zip(NAMES_ROWS, WIDTHS)]


def unpack_early_kernel(flat, *refs):
    outs, norms = refs[:7], refs[7:10]
    tiles, stage, tail, in_sem, out_sem, tail_sem = refs[10:13], refs[13], refs[14], refs[15], refs[16], refs[17]
    tail_copy = pltpu.make_async_copy(flat.at[pl.ds(MATRIX_ROWS, TAIL), 0], tail, tail_sem)
    tail_copy.start()
    work = unpack_body(EARLY_BLOCKS, (flat, None), outs, tiles, stage, in_sem, out_sem)
    next(work)
    tail_copy.wait()
    base = 0
    for n in norms:
        for j in COLUMNS:
            lines = [tail[pl.ds(base + j + 7 * layer, 1), :] for layer in range(n.shape[0])]
            n[:, pl.ds(j * LANES, LANES)] = jnp.concatenate(lines, axis=0).astype(BF16)
        base += 7 * n.shape[0]
    for _ in work:
        pass


def unpack_early(flat):
    return pl.pallas_call(
        unpack_early_kernel,
        name="unpack_early",
        out_shape=TENSOR_TYPES + [jax.ShapeDtypeStruct(s, BF16) for s in GAINS],
        in_specs=[ANY],
        out_specs=[ANY] * 7 + [VMEM_SPEC] * 3,
        scratch_shapes=UNPACK_SCRATCH + [pltpu.VMEM((TAIL, LANES), F32), DMA((SLOTS, 3)), DMA((SLOTS,)), DMA],
        compiler_params=pltpu.CompilerParams(vmem_limit_bytes=VMEM_LIMIT),
        cost_estimate=COST,
    )(flat)


def unpack_late_kernel(flat, late, *refs):
    count = len(LATE_TENSORS)
    outs = dict(zip(LATE_TENSORS, refs[count:2 * count]))
    tiles, stage, in_sem, out_sem = refs[2 * count:2 * count + 3], refs[2 * count + 3], refs[2 * count + 4], refs[2 * count + 5]
    for _ in unpack_body(LATE_BLOCKS, (flat, late), outs, tiles, stage, in_sem, out_sem):
        pass


def unpack_late(flat, late, params):
    count = len(LATE_TENSORS)
    outs = pl.pallas_call(
        unpack_late_kernel,
        name="unpack_late",
        out_shape=[TENSOR_TYPES[t] for t in LATE_TENSORS],
        in_specs=[ANY] * (2 + count),
        out_specs=[ANY] * count,
        input_output_aliases={2 + n: n for n in range(count)},
        scratch_shapes=UNPACK_SCRATCH + [DMA((SLOTS, 3)), DMA((SLOTS,))],
        compiler_params=pltpu.CompilerParams(vmem_limit_bytes=VMEM_LIMIT),
        cost_estimate=COST,
    )(flat, late, *[params[t] for t in LATE_TENSORS])
    params = list(params)
    for t, out in zip(LATE_TENSORS, outs):
        params[t] = out
    return params


def neighbours():
    me = lax.axis_index("dp")
    core, x, y = lax.rem(me, 2), lax.rem(me // 2, 2), me // 4
    other = 1 - 2 * core
    step_x, step_y = 2 - 4 * x, 4 - 8 * y
    return me, other, me + step_x, me + step_y, me + step_x + step_y


RS_ROWS = 1821
RS_HALF_START = SEG - 8 * RS_ROWS
KIND_D, KIND_N, KIND_S, KIND_O = range(4)
CHIP_D, CHIP_X, CHIP_Y, CHIP_OWN = range(4)
QUARTER = 4 * RS_ROWS
MARGIN = 16 * 38
PACK_ROWS = {38: 112, 7: 608, 1: 896}
PACK_STAGE = 112 * 38


def pack_blocks(chip, quarter):
    blocks = []
    for parity in HALVES:
        for h in HALVES:
            begin = SEG * (2 * chip + parity) + RS_HALF_START * h + QUARTER * quarter
            for t in TENSORS:
                w, offset, total = WIDTHS[t], OFFSETS[t], NAMES_ROWS[t]
                low, high = max(begin, offset), min(begin + QUARTER, offset + total * w)
                if low >= high:
                    continue
                first = (low - offset) // (16 * w) * 16
                end = -(-(high - offset) // (16 * w)) * 16
                step = -(-(end - first) // (16 * -(-(end - first) // PACK_ROWS[w]))) * 16
                for row in range(first, end, step):
                    blocks.append((t, row, min(step, end - row), parity, h, offset + row * w - begin + MARGIN))
    return blocks


def reduce_kernel(*refs):
    (grads, norms, (g_out, norm_out, flat, land_p, land_d, land_n, land_s),
     (mine, part, first, second, sums, g_buf, ss, ss_all), tiles, (stage, tail),
     (p_send, p_recv, i_send, i_recv, load_sem, g_sem, ss_send, ss_recv, in_sem, out_sem, tail_sem)) = split(refs, (7, 3, 7, 8, 3, 2, 11))
    me, other, dev_x, dev_y, dev_d = neighbours()
    core, x, y = lax.rem(me, 2), lax.rem(me // 2, 2), me // 4
    barrier = pltpu.get_barrier_semaphore()
    for d in range(1, NDEV):
        pl.semaphore_signal(barrier, inc=1, device_id=(lax.rem(me + d, NDEV),), device_id_type=MESH)

    tail[...] = jnp.zeros_like(tail)
    line = 0
    for n in norms:
        for layer in range(n.shape[0]):
            for j in COLUMNS:
                tail[pl.ds(line, 1), :] = n[pl.ds(layer, 1), pl.ds(j * LANES, LANES)].astype(F32)
                line += 1

    def pack(place, chip, quarter):
        blocks = pack_blocks(chip, quarter)

        def load(b):
            t, row, rows = blocks[b][:3]
            return pltpu.make_async_copy(grads[t].at[pl.ds(row, rows)], tiles[width_slot(WIDTHS[t])].at[b % 2, pl.ds(0, rows)], in_sem.at[b % 2])

        def store(b):
            t, _, rows, parity, h, to = blocks[b]
            size = rows * WIDTHS[t]
            return pltpu.make_async_copy(stage.at[b % 2, pl.ds(0, size)], flat.at[place, quarter, parity, h, pl.ds(to, size), 0], out_sem.at[b % 2])

        load(0).start()
        load(1).start()
        tail_copies = [pltpu.make_async_copy(tail, flat.at[place, quarter, quarter, quarter, pl.ds(MARGIN + QUARTER - TAIL, TAIL), 0], tail_sem)
                       for _ in range(chip * quarter // 3)]
        for copy in tail_copies:
            copy.start()
        for b, block in enumerate(blocks):
            t, rows = block[0], block[2]
            w = WIDTHS[t]
            tile = tiles[width_slot(w)]
            group = row_group(rows, w)
            load(b).wait()
            if b >= 2:
                store(b - 2).wait()

            @pl.loop(0, rows // group)
            def _(i):
                for j in range(w):
                    values = tile[b % 2, pl.ds(pl.multiple_of(i * group, 16), group), pl.ds(j * LANES, LANES)].astype(F32)
                    if w == 1:
                        stage[b % 2, pl.ds(pl.multiple_of(i * group, 16), group), :] = values
                    else:
                        stage[b % 2, pl.ds(i * (group * w) + j, group, stride=w), :] = values

            store(b).start()
            if b + 2 < len(blocks):
                load(b + 2).start()
        store(len(blocks) - 2).wait()
        store(len(blocks) - 1).wait()
        for copy in tail_copies:
            copy.wait()

    def place_of(kind, h):
        return ((CHIP_D, CHIP_D), (CHIP_X, CHIP_Y), (CHIP_Y, CHIP_X), (CHIP_OWN, CHIP_OWN))[kind][h]

    def chunk(kind, h, i, parity):
        return flat.at[place_of(kind, h), i // 4, parity, h, pl.ds(MARGIN + RS_ROWS * lax.rem(i, 4), RS_ROWS)]

    def start_row(h, i):
        return RS_HALF_START * h + RS_ROWS * i

    def partner_copy(kind, h, i):
        return pltpu.make_async_remote_copy(
            src_ref=chunk(kind, h, i, 1 - core), dst_ref=land_p.at[kind, h, i],
            send_sem=p_send.at[kind, h, i], recv_sem=p_recv.at[kind, h, i],
            device_id=(me + other,), device_id_type=MESH)

    def link_copy(kind, h, i):
        land = (land_d, land_n, land_s)[kind]
        to = ((dev_x, dev_y), (dev_x, dev_y), (dev_y, dev_x))[kind][h]
        return pltpu.make_async_remote_copy(
            src_ref=sums.at[kind, h, i], dst_ref=land.at[h, i, pl.ds(0, RS_ROWS), 0],
            send_sem=i_send.at[kind, h, i], recv_sem=i_recv.at[kind, h, i],
            device_id=(to,), device_id_type=MESH)

    def load_mine(kind, h, i):
        return pltpu.make_async_copy(chunk(kind, h, i, core).at[:, 0], mine.at[h], load_sem.at[0, h])

    def load_part(kind, h, i):
        return pltpu.make_async_copy(land_p.at[kind, h, i, pl.ds(0, RS_ROWS), 0], part.at[h], load_sem.at[1, h])

    def load_link(land, buf, n, h, i):
        return pltpu.make_async_copy(land.at[h, i, pl.ds(0, RS_ROWS), 0], buf.at[h], load_sem.at[n, h])

    def store_g(h, i):
        return pltpu.make_async_copy(g_buf.at[h], g_out.at[pl.ds(start_row(h, i), RS_ROWS), 0], g_sem.at[h])

    def exchange(kinds, begin, end):
        @pl.loop(begin, end)
        def _(i):
            for kind in kinds:
                for h in HALVES:
                    partner_copy(kind, h, i).start()

    def send(kind, begin, end):
        @pl.loop(begin, end)
        def _(i):
            for h in HALVES:
                load_mine(kind, h, i).start()
            for h in HALVES:
                partner_copy(kind, h, i).wait_recv()
                load_part(kind, h, i).start()
                if kind == KIND_S:
                    link_copy(KIND_D, h, i).wait_recv()
                    load_link(land_d, first, 2, h, i).start()
            for h in HALVES:
                load_mine(kind, h, i).wait()
                load_part(kind, h, i).wait()
                total = mine[h] + part[h]
                if kind == KIND_S:
                    load_link(land_d, first, 2, h, i).wait()
                    total = total + first[h]
                sums[kind, h, i] = total
                link_copy(kind, h, i).start()

    @pl.loop(0, 8)
    def _(unit):
        place, quarter = unit // 2, lax.rem(unit, 2)
        flip_x, flip_y = 1 - place // 2, 1 - lax.rem(place, 2)
        chip = (x + flip_x * (1 - 2 * x)) + 2 * (y + flip_y * (1 - 2 * y))
        for case in range(8):
            @pl.when(2 * chip + quarter == case)
            def _():
                pack(place, case // 2, case % 2)

        @pl.when(unit == 0)
        def _():
            pl.semaphore_wait(barrier, NDEV - 1)

        @pl.when(unit < 2)
        def _():
            exchange((KIND_D,), 4 * quarter, 4 * quarter + 4)
            send(KIND_D, 4 * quarter, 4 * quarter + 4)

    exchange((KIND_N, KIND_S), 0, 8)
    exchange((KIND_O,), 0, 8)
    send(KIND_N, 0, 8)
    send(KIND_S, 0, 8)

    def last(i, acc):
        for h in HALVES:
            load_mine(KIND_O, h, i).start()
            partner_copy(KIND_O, h, i).wait_recv()
            load_part(KIND_O, h, i).start()
        for h in HALVES:
            link_copy(KIND_N, h, i).wait_recv()
            load_link(land_n, first, 2, h, i).start()
        for h in HALVES:
            link_copy(KIND_S, h, i).wait_recv()
            load_link(land_s, second, 3, h, i).start()
            load_mine(KIND_O, h, i).wait()
            load_part(KIND_O, h, i).wait()
            load_link(land_n, first, 2, h, i).wait()
            load_link(land_s, second, 3, h, i).wait()

            @pl.when(i > 0)
            def _():
                store_g(h, i - 1).wait()

            g = ((mine[h] + part[h]) + (first[h] + second[h])) * (1.0 / NDEV)
            g_buf[h] = g
            store_g(h, i).start()
            square = g * g
            if h == 1:
                row = lax.broadcasted_iota(jnp.int32, (RS_ROWS, LANES), 0) + RS_ROWS * i
                square = jnp.where(row >= 8 * RS_ROWS - RS_HALF_START, square, 0.0)
            acc = acc + jnp.sum(square, axis=0, keepdims=True)
        return acc

    acc = lax.fori_loop(0, 8, last, jnp.zeros((1, LANES), F32))
    ss[...] = jnp.broadcast_to(acc, (8, LANES))
    for h in HALVES:
        store_g(h, 7).wait()

    @pl.loop(0, 8)
    def _(i):
        for h in HALVES:
            for kind in range(4):
                partner_copy(kind, h, i).wait_send()
            for kind in range(3):
                link_copy(kind, h, i).wait_send()

    def norm_copy(d):
        return pltpu.make_async_remote_copy(
            src_ref=ss, dst_ref=ss_all.at[d], send_sem=ss_send.at[d], recv_sem=ss_recv.at[d],
            device_id=(lax.rem(me + d, NDEV),), device_id_type=MESH)

    for d in range(1, NDEV):
        norm_copy(d).start()
    ss_all[0] = ss[...]
    for d in range(1, NDEV):
        norm_copy(d).wait()
    total = jnp.zeros((8, LANES), F32)
    for dev in range(NDEV):
        total = total + ss_all[lax.rem(me - dev + NDEV, NDEV)]
    norm_out[...] = jnp.broadcast_to(jnp.sqrt(jnp.sum(total, axis=1, keepdims=True)), (8, LANES))


def reduce_grads(grads, norms):
    land = jax.ShapeDtypeStruct((2, 8, RS_ROWS, 1, LANES), F32)
    land_p = jax.ShapeDtypeStruct((4, 2, 8, RS_ROWS, 1, LANES), F32)
    flat = jax.ShapeDtypeStruct((4, 2, 2, 2, QUARTER + 2 * MARGIN, 1, LANES), F32)
    buf = pltpu.VMEM((2, RS_ROWS, LANES), F32)
    partner, link, pair, all_devs = DMA((4, 2, 8)), DMA((3, 2, 8)), DMA((2,)), DMA((NDEV,))
    outs = pl.pallas_call(
        reduce_kernel,
        name="reduce_grads",
        out_shape=[jax.ShapeDtypeStruct((SEG, 1, LANES), F32), jax.ShapeDtypeStruct((8, LANES), F32), flat, land_p, land, land, land],
        in_specs=[ANY] * 7 + [VMEM_SPEC] * 3,
        out_specs=[ANY, VMEM_SPEC] + [ANY] * 5,
        scratch_shapes=[buf] * 4 + [pltpu.VMEM((3, 2, 8, RS_ROWS, LANES), F32), buf, pltpu.VMEM((8, LANES), F32), pltpu.VMEM((NDEV, 8, LANES), F32)]
        + tile_scratch(2, PACK_ROWS.values()) + [pltpu.VMEM((2, PACK_STAGE, LANES), F32), pltpu.VMEM((TAIL, LANES), F32)]
        + [partner, partner, link, link, DMA((4, 2)), pair, all_devs, all_devs, pair, pair, DMA],
        compiler_params=pltpu.CompilerParams(collective_id=0, has_side_effects=True, vmem_limit_bytes=VMEM_LIMIT),
        cost_estimate=COST,
    )(*grads, *norms)
    return outs[0], outs[1]


def adam_rows(g, m, v, p, norm_row, lr, decay):
    clip = jnp.minimum(1.0, MAX_NORM / (norm_row + CLIP_EPS))
    clipped = clip * g
    new_m = BETA_ONE * m + (1.0 - BETA_ONE) * clipped
    new_v = BETA_TWO * v + (1.0 - BETA_TWO) * clipped * clipped
    adam_dir = (new_m / BIAS_ONE) / (jnp.sqrt(new_v / BIAS_TWO) + ADAM_EPS)
    decay_term = jnp.where(decay, WEIGHT_DECAY * p, 0.0)
    return p - lr * (decay_term + adam_dir), new_m, new_v


UP_ROWS = 1824
UP_LAST = SEG - 15 * UP_ROWS
SUB = 152


def decay_rows(me, start, rows):
    return lax.broadcasted_iota(jnp.int32, (rows, LANES), 0) + (SEG * me + start) < MATRIX_ROWS


def gather_kernel(g, m, v, p, norm, lr, full, late, gb, mb, vb, pb, new_p, late_p,
                  load_sem, own_sem, late_sem, own_send, own_recv, fwd_send, fwd_recv, p_send, p_recv):
    me, other, dev_x, dev_y, dev_d = neighbours()
    partner = me + other
    barrier = pltpu.get_barrier_semaphore()
    for dev in (partner, dev_x, dev_y):
        pl.semaphore_signal(barrier, inc=1, device_id=(dev,), device_id_type=MESH)
    pl.semaphore_wait(barrier, 3)
    to = (dev_x, dev_y, partner)
    sources = (me, dev_x, dev_y, dev_d)

    def is_last(h, i):
        return h == 1 and isinstance(i, int) and i == HALF - 1

    def start_row(h, i):
        return PIECE * (PIECES - 1) if is_last(h, i) else PIECE * (HALF * h + i)

    def size(h, i):
        return PIECE_LAST if is_last(h, i) else PIECE

    def rows_of(dev, h, i):
        return full.at[pl.ds(SEG * dev + start_row(h, i), size(h, i)), 0]

    def loads(h, i):
        return loads_at(h, start_row(h, i), size(h, i))

    def loads_at(h, start, rows):
        start = pl.multiple_of(start, 8)
        copies = [pltpu.make_async_copy(g.at[pl.ds(start, rows), 0], gb.at[h, pl.ds(0, rows)], load_sem.at[0, h])]
        for n, (src, buf) in enumerate(((m, mb), (v, vb), (p, pb))):
            copies.append(pltpu.make_async_copy(src.at[pl.ds(start, rows)], buf.at[h, pl.ds(0, rows)], load_sem.at[n + 1, h]))
        return copies

    def own_copy(n, h, i):
        return pltpu.make_async_remote_copy(
            src_ref=new_p.at[h, i, pl.ds(0, size(h, i))], dst_ref=rows_of(me, h, i),
            send_sem=own_send.at[n, h, i], recv_sem=own_recv.at[n, h, i], device_id=(to[n],), device_id_type=MESH)

    def own_store(h, i):
        return pltpu.make_async_copy(new_p.at[h, i, pl.ds(0, size(h, i))], rows_of(me, h, i), own_sem.at[h, i])

    def forward(h, i):
        src = rows_of((dev_y, dev_x)[h], h, i)
        return pltpu.make_async_remote_copy(
            src_ref=src, dst_ref=src, send_sem=fwd_send.at[h, i], recv_sem=fwd_recv.at[h, i],
            device_id=((dev_x, dev_y)[h],), device_id_type=MESH)

    def arrival(n, h, i):
        src = rows_of((dev_x, dev_y, partner)[n], h, i)
        return pltpu.make_async_remote_copy(
            src_ref=src, dst_ref=src, send_sem=own_send.at[n, h, i], recv_sem=own_recv.at[n, h, i],
            device_id=(to[n],), device_id_type=MESH)

    def forward_arrival(h, i):
        src = rows_of(dev_d, h, i)
        return pltpu.make_async_remote_copy(
            src_ref=src, dst_ref=src, send_sem=fwd_send.at[h, i], recv_sem=fwd_recv.at[h, i],
            device_id=((dev_x, dev_y)[h],), device_id_type=MESH)

    def partner_copy(q, h, i):
        src = rows_of(sources[q], h, i)
        return pltpu.make_async_remote_copy(
            src_ref=src, dst_ref=src, send_sem=p_send.at[q - 1, h, i], recv_sem=p_recv.at[q - 1, h, i],
            device_id=(partner,), device_id_type=MESH)

    def partner_arrival(q, h, i):
        src = rows_of(sources[q] + other, h, i)
        return pltpu.make_async_remote_copy(
            src_ref=src, dst_ref=src, send_sem=p_send.at[q - 1, h, i], recv_sem=p_recv.at[q - 1, h, i],
            device_id=(partner,), device_id_type=MESH)

    def each(body):
        @pl.loop(0, HALF - 1)
        def _(i):
            body(i)

        body(HALF - 1)

    norm_row = norm[0:1, :]
    for h in HALVES:
        for copy in loads(h, 0):
            copy.start()

    def compute(h, out, first):
        @pl.loop(0, PIECE // SUB)
        def _(s):
            start = pl.multiple_of(s * SUB, 8)
            sub = pl.ds(start, SUB)
            out[sub] = adam_rows(gb[h, sub], mb[h, sub], vb[h, sub], pb[h, sub], norm_row, lr[0], decay_rows(me, first + start, SUB))[0]

    def update(i):
        for h in HALVES:
            for copy in loads(h, i):
                copy.wait()

            compute(h, new_p.at[h, i], start_row(h, i))
            for n in ((1, 0, 2) if h == 0 else (0, 1, 2)):
                own_copy(n, h, i).start()
            own_store(h, i).start()
            if isinstance(i, int):
                continue
            for last in (False, True):
                @pl.when((i == HALF - 2) == last)
                def _():
                    for copy in loads(h, HALF - 1 if last else i + 1):
                        copy.start()

    each(update)

    def late_store(src, to, n):
        return pltpu.make_async_copy(src, late.at[pl.ds(to, src.shape[0]), 0], late_sem.at[n])

    def late_piece(j):
        return late_store(late_p.at[j], 8 + PIECE * j, j)

    edges = [late_store(new_p.at[1, HALF - 2, pl.ds(PIECE - 8, 8)], 0, 6),
             late_store(new_p.at[1, HALF - 1, pl.ds(0, 8)], LATE_ROWS - 8, 7)]
    for copy in edges:
        copy.start()

    @pl.loop(0, LATE_END - LATE_FIRST)
    def _(j):
        first = PIECE * (LATE_FIRST + j)
        for copy in loads_at(0, first, PIECE):
            copy.start()
        for copy in loads_at(0, first, PIECE):
            copy.wait()
        compute(0, late_p.at[j], first)
        late_piece(j).start()

    def pass_on(i):
        arrival(1, 0, i).wait_recv()
        forward(0, i).start()
        partner_copy(2, 0, i).start()
        arrival(0, 1, i).wait_recv()
        forward(1, i).start()
        partner_copy(1, 1, i).start()
        arrival(0, 0, i).wait_recv()
        partner_copy(1, 0, i).start()
        arrival(1, 1, i).wait_recv()
        partner_copy(2, 1, i).start()

    each(pass_on)

    def pass_last(i):
        for h in HALVES:
            forward_arrival(h, i).wait_recv()
            partner_copy(3, h, i).start()

    each(pass_last)

    def finish(i):
        for h in HALVES:
            own_store(h, i).wait()
            arrival(2, h, i).wait_recv()
            for n in range(3):
                own_copy(n, h, i).wait_send()
            forward(h, i).wait_send()
            for q in range(1, 4):
                partner_copy(q, h, i).wait_send()
                partner_arrival(q, h, i).wait_recv()

    each(finish)
    for copy in edges:
        copy.wait()

    @pl.loop(0, LATE_END - LATE_FIRST)
    def _(j):
        late_piece(j).wait()


def gather_params(g, m, v, p, norm, lr):
    buf = pltpu.VMEM((2, PIECE, LANES), F32)
    pairs = DMA((2, HALF))
    triples = DMA((3, 2, HALF))
    return pl.pallas_call(
        gather_kernel,
        name="gather_params",
        out_shape=[jax.ShapeDtypeStruct((FLAT_ROWS, 1, LANES), F32), jax.ShapeDtypeStruct((LATE_ROWS, 1, LANES), F32)],
        in_specs=[ANY] * 4 + [VMEM_SPEC, SMEM_SPEC],
        out_specs=[ANY, ANY],
        scratch_shapes=[buf, buf, buf, buf, pltpu.VMEM((2, HALF, PIECE, LANES), F32), pltpu.VMEM((LATE_END - LATE_FIRST, PIECE, LANES), F32),
                        DMA((4, 2)), pairs, DMA((8,)), triples, triples, pairs, pairs, triples, triples],
        compiler_params=pltpu.CompilerParams(collective_id=1, has_side_effects=True, vmem_limit_bytes=VMEM_LIMIT),
        cost_estimate=COST,
    )(g, m, v, p, norm, lr)


def state_kernel(g, m, v, p, norm, lr, new_p, new_m, new_v, gb, g_sem):
    me = lax.axis_index("dp")
    i = pl.program_id(0)

    def load(j, last):
        rows = UP_LAST if last else UP_ROWS
        return pltpu.make_async_copy(g.at[pl.ds(j * UP_ROWS, rows), 0], gb.at[lax.rem(j, 2), pl.ds(0, rows)], g_sem.at[lax.rem(j, 2)])

    @pl.when(i == 0)
    def _():
        load(i, False).start()

    @pl.when(i < 14)
    def _():
        load(i + 1, False).start()

    @pl.when(i == 14)
    def _():
        load(i + 1, True).start()

    @pl.when(i < 15)
    def _():
        load(i, False).wait()

    @pl.when(i == 15)
    def _():
        load(i, True).wait()

    norm_row = norm[0:1, :]

    @pl.loop(0, UP_ROWS // SUB)
    def _(s):
        start = pl.multiple_of(s * SUB, 8)
        rows = pl.ds(start, SUB)
        new_p[rows], new_m[rows], new_v[rows] = adam_rows(
            gb[lax.rem(i, 2), rows], m[rows], v[rows], p[rows], norm_row, lr[0], decay_rows(me, i * UP_ROWS + start, SUB))


def new_state(g, m, v, p, norm, lr):
    block = pl.BlockSpec((UP_ROWS, LANES), lambda i: (i, 0))
    return pl.pallas_call(
        state_kernel,
        name="new_state",
        grid=(16,),
        out_shape=[jax.ShapeDtypeStruct((SEG, LANES), F32)] * 3,
        in_specs=[ANY, block, block, block, pl.BlockSpec((8, LANES), lambda i: (0, 0)), SMEM_SPEC],
        out_specs=[block] * 3,
        scratch_shapes=[pltpu.VMEM((2, UP_ROWS, LANES), F32), DMA((2,))],
        compiler_params=pltpu.CompilerParams(vmem_limit_bytes=VMEM_LIMIT),
        cost_estimate=COST,
    )(g, m, v, p, norm, lr)


def solution(mesh):
    def local_step(*arrays):
        grads = [a.reshape(r, w * LANES) for a, r, w in zip(arrays[:7], NAMES_ROWS, WIDTHS)]
        norms = [a.reshape(s) for a, s in zip(arrays[7:10], GAINS)]
        master, exp_avg, exp_avg_sq = [a.reshape(SEG, LANES) for a in arrays[10:13]]
        lr = arrays[13].reshape(1)
        g, norm = reduce_grads(grads, norms)
        full, late = gather_params(g, exp_avg, exp_avg_sq, master, norm, lr)
        late = lax.all_gather(late, "dp", tiled=True)
        state = new_state(g, exp_avg, exp_avg_sq, master, norm, lr)
        params = unpack_late(full, late, unpack_early(full))
        shapes = SHAPES + GAINS[:2] + [(D,)]
        return tuple([a.reshape(-1) for a in state] + [a.reshape(s) for a, s in zip(params, shapes)] + [norm[0, 0]])

    return jax.shard_map(local_step, mesh=mesh, in_specs=(P("dp"),) * 13 + (P(),), out_specs=(P("dp"),) * 3 + (P(),) * 11, check_vma=False)
```

```python
import functools
import math
import jax
import jax.numpy as jnp
from jax import lax
from jax.experimental import pallas as pl
from jax.experimental.pallas import tpu as pltpu
from jax.sharding import PartitionSpec as P

BETA_ONE = 0.9
BETA_TWO = 0.95
ADAM_EPS = 1e-8
WEIGHT_DECAY = 0.1
MAX_NORM = 1.0
CLIP_EPS = 1e-6
STEP = 4
BIAS_ONE = 1.0 - BETA_ONE ** STEP
BIAS_TWO = 1.0 - BETA_TWO ** STEP

MESH = pl.DeviceIdType.MESH
F32 = jnp.float32
BF16 = jnp.bfloat16
LANES = 128

LAYERS, D, KV, FF = 2, 896, 128, 4864
SHAPES = [(LAYERS, D, D), (LAYERS, D, KV), (LAYERS, D, KV), (LAYERS, D, D), (LAYERS, D, FF), (LAYERS, D, FF), (LAYERS, FF, D)]
GAINS = [(LAYERS, D), (LAYERS, D), (1, D)]
TAIL = 40
HALVES, TENSORS, COLUMNS = range(2), range(7), range(7)
NAMES_ROWS = [math.prod(s[:-1]) for s in SHAPES]
WIDTHS = [s[-1] // LANES for s in SHAPES]
OFFSETS = [sum(r * w for r, w in zip(NAMES_ROWS[:t], WIDTHS[:t])) for t in TENSORS]
BLOCK_ROWS = [448, 1792, 1792, 448, 128, 128, 608]
MATRIX_ROWS = 232960
FLAT_ROWS = 233000
SEG = 29125
NDEV = 8

WIDTH_ORDER = (38, 7, 1)
GROUPS = {38: (16,), 7: (16, 32, 64), 1: (16, 128, 256)}
STAGE_ROWS = max(br * WIDTHS[t] for t, br in enumerate(BLOCK_ROWS))

def split(refs, counts):
    refs = list(refs)
    return [[refs.pop(0) for _ in range(n)] for n in counts]


ANY = pl.BlockSpec(memory_space=pl.ANY)
VMEM_SPEC = pl.BlockSpec(memory_space=pltpu.VMEM)
SMEM_SPEC = pl.BlockSpec(memory_space=pltpu.SMEM)
DMA = pltpu.SemaphoreType.DMA
VMEM_LIMIT = 63 * 1024 * 1024
COST = pl.CostEstimate(flops=2 * 10 ** 8, bytes_accessed=10 ** 8, transcendentals=0)


def tile_scratch(slots, rows):
    return [pltpu.VMEM((slots, r, w * LANES), BF16) for r, w in zip(rows, WIDTH_ORDER)]


def width_slot(width):
    return WIDTH_ORDER.index(width)


def row_group(rows, width):
    return max(g for g in GROUPS[width] if rows % g == 0)


PIECE = 912
PIECES = 32
LATE_FIRST, LATE_END = 25, 31
LATE_ROWS = PIECE * (LATE_END - LATE_FIRST) + 16
PIECE_LAST = SEG - (PIECES - 1) * PIECE
HALF = (PIECES - LATE_END + LATE_FIRST) // 2
LATE_RANGES = [((SEG * s + PIECE * LATE_FIRST) // 8 * 8, -(-(SEG * s + PIECE * LATE_END) // 8) * 8) for s in range(NDEV)]


def unpack_blocks():
    early, late = [], []
    for t in TENSORS:
        w, offset, total = WIDTHS[t], OFFSETS[t], NAMES_ROWS[t]
        cuts = {0, total}
        spans = []
        for low, high in LATE_RANGES:
            first = max(0, (low - offset) // (16 * w) * 16)
            end = min(total, -(-(high - offset) // (16 * w)) * 16)
            if first < end:
                spans.append((first, end))
                cuts |= {first, end}
        cuts = sorted(cuts)
        for begin, end in zip(cuts[:-1], cuts[1:]):
            is_late = any(first <= begin and end <= last for first, last in spans)
            count = -(-(end - begin) // BLOCK_ROWS[t])
            step = -(-(end - begin) // (16 * count)) * 16
            for row in range(begin, end, step):
                rows = min(step, end - row)
                low, high = offset + row * w, offset + (row + rows) * w
                edges = sorted({low, high} | {e for r in LATE_RANGES for e in r if low < e < high})
                sources = []
                for e0, e1 in zip(edges[:-1], edges[1:]):
                    seg = [s for s, (l, h) in enumerate(LATE_RANGES) if l <= e0 and e1 <= h]
                    start = LATE_ROWS * seg[0] + e0 - SEG * seg[0] - PIECE * LATE_FIRST + 8 if seg else e0
                    sources.append((bool(seg), start, e0 - low, e1 - e0))
                (late if is_late else early).append((t, row, rows, sources))
    return early, late


EARLY_BLOCKS, LATE_BLOCKS = unpack_blocks()
LATE_TENSORS = sorted({t for t, _, _, _ in LATE_BLOCKS})
SLOTS = 4


def unpack_body(blocks, sources, outs, tiles, stage, in_sem, out_sem):
    def loads(b):
        return [pltpu.make_async_copy(sources[late].at[pl.ds(start, rows), 0], stage.at[b % SLOTS, pl.ds(to, rows)], in_sem.at[b % SLOTS, n])
                for n, (late, start, to, rows) in enumerate(blocks[b][3])]

    def store(b):
        t, row, rows, _ = blocks[b]
        return pltpu.make_async_copy(tiles[width_slot(WIDTHS[t])].at[b % SLOTS, pl.ds(0, rows)], outs[t].at[pl.ds(row, rows)], out_sem.at[b % SLOTS])

    for b in range(min(SLOTS, len(blocks))):
        for copy in loads(b):
            copy.start()
    yield
    for b, (t, row, rows, _) in enumerate(blocks):
        w = WIDTHS[t]
        tile = tiles[width_slot(w)]
        group = row_group(rows, w)
        for copy in loads(b):
            copy.wait()
        if b >= SLOTS:
            store(b - SLOTS).wait()

        @pl.loop(0, rows // group)
        def _(i):
            for j in range(w):
                if w == 1:
                    block = stage[b % SLOTS, pl.ds(pl.multiple_of(i * group, 16), group), :]
                else:
                    block = stage[b % SLOTS, pl.ds(i * (group * w) + j, group, stride=w), :]
                tile[b % SLOTS, pl.ds(pl.multiple_of(i * group, 16), group), pl.ds(j * LANES, LANES)] = block.astype(BF16)

        store(b).start()
        if b + SLOTS < len(blocks):
            for copy in loads(b + SLOTS):
                copy.start()
    for b in range(max(0, len(blocks) - SLOTS), len(blocks)):
        store(b).wait()


UNPACK_SCRATCH = tile_scratch(SLOTS, (128, 608, 1792)) + [pltpu.VMEM((SLOTS, STAGE_ROWS, LANES), F32)]
TENSOR_TYPES = [jax.ShapeDtypeStruct((r, w * LANES), BF16) for r, w in zip(NAMES_ROWS, WIDTHS)]


def unpack_early_kernel(flat, *refs):
    outs, norms = refs[:7], refs[7:10]
    tiles, stage, tail, in_sem, out_sem, tail_sem = refs[10:13], refs[13], refs[14], refs[15], refs[16], refs[17]
    tail_copy = pltpu.make_async_copy(flat.at[pl.ds(MATRIX_ROWS, TAIL), 0], tail, tail_sem)
    tail_copy.start()
    work = unpack_body(EARLY_BLOCKS, (flat, None), outs, tiles, stage, in_sem, out_sem)
    next(work)
    tail_copy.wait()
    base = 0
    for n in norms:
        for j in COLUMNS:
            lines = [tail[pl.ds(base + j + 7 * layer, 1), :] for layer in range(n.shape[0])]
            n[:, pl.ds(j * LANES, LANES)] = jnp.concatenate(lines, axis=0).astype(BF16)
        base += 7 * n.shape[0]
    for _ in work:
        pass


def unpack_early(flat):
    return pl.pallas_call(
        unpack_early_kernel,
        name="unpack_early",
        out_shape=TENSOR_TYPES + [jax.ShapeDtypeStruct(s, BF16) for s in GAINS],
        in_specs=[ANY],
        out_specs=[ANY] * 7 + [VMEM_SPEC] * 3,
        scratch_shapes=UNPACK_SCRATCH + [pltpu.VMEM((TAIL, LANES), F32), DMA((SLOTS, 3)), DMA((SLOTS,)), DMA],
        compiler_params=pltpu.CompilerParams(vmem_limit_bytes=VMEM_LIMIT),
        cost_estimate=COST,
    )(flat)


def unpack_late_kernel(flat, late, *refs):
    count = len(LATE_TENSORS)
    outs = dict(zip(LATE_TENSORS, refs[count:2 * count]))
    tiles, stage, in_sem, out_sem = refs[2 * count:2 * count + 3], refs[2 * count + 3], refs[2 * count + 4], refs[2 * count + 5]
    for _ in unpack_body(LATE_BLOCKS, (flat, late), outs, tiles, stage, in_sem, out_sem):
        pass


def unpack_late(flat, late, params):
    count = len(LATE_TENSORS)
    outs = pl.pallas_call(
        unpack_late_kernel,
        name="unpack_late",
        out_shape=[TENSOR_TYPES[t] for t in LATE_TENSORS],
        in_specs=[ANY] * (2 + count),
        out_specs=[ANY] * count,
        input_output_aliases={2 + n: n for n in range(count)},
        scratch_shapes=UNPACK_SCRATCH + [DMA((SLOTS, 3)), DMA((SLOTS,))],
        compiler_params=pltpu.CompilerParams(vmem_limit_bytes=VMEM_LIMIT),
        cost_estimate=COST,
    )(flat, late, *[params[t] for t in LATE_TENSORS])
    params = list(params)
    for t, out in zip(LATE_TENSORS, outs):
        params[t] = out
    return params


def neighbours():
    me = lax.axis_index("dp")
    core, x, y = lax.rem(me, 2), lax.rem(me // 2, 2), me // 4
    other = 1 - 2 * core
    step_x, step_y = 2 - 4 * x, 4 - 8 * y
    return me, other, me + step_x, me + step_y, me + step_x + step_y


CHUNKS = 16
RS_ROWS = 911
RS_HALF_START = SEG - CHUNKS * RS_ROWS
UNITS = CHUNKS // 4
KIND_D, KIND_N, KIND_S, KIND_O = range(4)
CHIP_D, CHIP_X, CHIP_Y, CHIP_OWN = range(4)
UNIT_ROWS = 4 * RS_ROWS
MARGIN = 16 * 38
PACK_ROWS = {38: 112, 7: 608, 1: 896}
PACK_STAGE = 112 * 38
PACK_SLOTS = 3


def pack_blocks(chip, unit):
    blocks = []
    for parity in HALVES:
        for h in HALVES:
            begin = SEG * (2 * chip + parity) + RS_HALF_START * h + UNIT_ROWS * unit
            for t in TENSORS:
                w, offset, total = WIDTHS[t], OFFSETS[t], NAMES_ROWS[t]
                low, high = max(begin, offset), min(begin + UNIT_ROWS, offset + total * w)
                if low >= high:
                    continue
                first = (low - offset) // (16 * w) * 16
                end = -(-(high - offset) // (16 * w)) * 16
                step = -(-(end - first) // (16 * -(-(end - first) // PACK_ROWS[w]))) * 16
                for row in range(first, end, step):
                    blocks.append((t, row, min(step, end - row), parity, h, offset + row * w - begin + MARGIN))
    return blocks


def reduce_kernel(*refs):
    (grads, norms, (g_out, norm_out, flat, land_p, land_d, land_n, land_s),
     (mine, part, first, second, sums, g_buf, ss, ss_all), tiles, (stage, tail),
     (p_send, p_recv, i_send, i_recv, load_sem, g_sem, ss_send, ss_recv, in_sem, out_sem, tail_sem)) = split(refs, (7, 3, 7, 8, 3, 2, 11))
    me, other, dev_x, dev_y, dev_d = neighbours()
    core, x, y = lax.rem(me, 2), lax.rem(me // 2, 2), me // 4
    barrier = pltpu.get_barrier_semaphore()
    for d in range(1, NDEV):
        pl.semaphore_signal(barrier, inc=1, device_id=(lax.rem(me + d, NDEV),), device_id_type=MESH)

    tail[...] = jnp.zeros_like(tail)
    line = 0
    for n in norms:
        for layer in range(n.shape[0]):
            for j in COLUMNS:
                tail[pl.ds(line, 1), :] = n[pl.ds(layer, 1), pl.ds(j * LANES, LANES)].astype(F32)
                line += 1

    def pack(place, chip, unit):
        blocks = pack_blocks(chip, unit)

        def load(b):
            t, row, rows = blocks[b][:3]
            return pltpu.make_async_copy(grads[t].at[pl.ds(row, rows)], tiles[width_slot(WIDTHS[t])].at[b % PACK_SLOTS, pl.ds(0, rows)], in_sem.at[b % PACK_SLOTS])

        def store(b):
            t, _, rows, parity, h, to = blocks[b]
            size = rows * WIDTHS[t]
            return pltpu.make_async_copy(stage.at[b % PACK_SLOTS, pl.ds(0, size)], flat.at[place, unit, parity, h, pl.ds(to, size), 0], out_sem.at[b % PACK_SLOTS])

        for b in range(PACK_SLOTS):
            load(b).start()
        tail_copies = [pltpu.make_async_copy(tail, flat.at[place, unit, 1, 1, pl.ds(MARGIN + UNIT_ROWS - TAIL, TAIL), 0], tail_sem)
                       for _ in range(chip * unit // (3 * UNITS - 3))]
        for copy in tail_copies:
            copy.start()
        for b, block in enumerate(blocks):
            t, rows = block[0], block[2]
            w = WIDTHS[t]
            tile = tiles[width_slot(w)]
            group = row_group(rows, w)
            load(b).wait()
            if b >= PACK_SLOTS:
                store(b - PACK_SLOTS).wait()

            @pl.loop(0, rows // group)
            def _(i):
                for j in range(w):
                    values = tile[b % PACK_SLOTS, pl.ds(pl.multiple_of(i * group, 16), group), pl.ds(j * LANES, LANES)].astype(F32)
                    if w == 1:
                        stage[b % PACK_SLOTS, pl.ds(pl.multiple_of(i * group, 16), group), :] = values
                    else:
                        stage[b % PACK_SLOTS, pl.ds(i * (group * w) + j, group, stride=w), :] = values

            store(b).start()
            if b + PACK_SLOTS < len(blocks):
                load(b + PACK_SLOTS).start()
        for b in range(len(blocks) - PACK_SLOTS, len(blocks)):
            store(b).wait()
        for copy in tail_copies:
            copy.wait()

    def place_of(kind, h):
        return ((CHIP_D, CHIP_D), (CHIP_X, CHIP_Y), (CHIP_Y, CHIP_X), (CHIP_OWN, CHIP_OWN))[kind][h]

    def chunk(kind, h, i, parity):
        return flat.at[place_of(kind, h), i // 4, parity, h, pl.ds(MARGIN + RS_ROWS * lax.rem(i, 4), RS_ROWS)]

    def start_row(h, i):
        return RS_HALF_START * h + RS_ROWS * i

    def partner_copy(kind, h, i):
        return pltpu.make_async_remote_copy(
            src_ref=chunk(kind, h, i, 1 - core), dst_ref=land_p.at[kind, h, i],
            send_sem=p_send.at[kind, h, i], recv_sem=p_recv.at[kind, h, i],
            device_id=(me + other,), device_id_type=MESH)

    def link_copy(kind, h, i):
        land = (land_d, land_n, land_s)[kind]
        to = ((dev_x, dev_y), (dev_x, dev_y), (dev_y, dev_x))[kind][h]
        return pltpu.make_async_remote_copy(
            src_ref=sums.at[kind, h, i], dst_ref=land.at[h, i, pl.ds(0, RS_ROWS), 0],
            send_sem=i_send.at[kind, h, i], recv_sem=i_recv.at[kind, h, i],
            device_id=(to,), device_id_type=MESH)

    def load_mine(kind, h, i):
        return pltpu.make_async_copy(chunk(kind, h, i, core).at[:, 0], mine.at[h], load_sem.at[0, h])

    def load_part(kind, h, i):
        return pltpu.make_async_copy(land_p.at[kind, h, i, pl.ds(0, RS_ROWS), 0], part.at[h], load_sem.at[1, h])

    def load_link(land, buf, n, h, i):
        return pltpu.make_async_copy(land.at[h, i, pl.ds(0, RS_ROWS), 0], buf.at[h], load_sem.at[n, h])

    def store_g(h, i):
        return pltpu.make_async_copy(g_buf.at[h], g_out.at[pl.ds(start_row(h, i), RS_ROWS), 0], g_sem.at[h])

    def exchange(kinds, begin, end):
        @pl.loop(begin, end)
        def _(i):
            for kind in kinds:
                for h in HALVES:
                    partner_copy(kind, h, i).start()

    def send(kind, begin, end):
        @pl.loop(begin, end)
        def _(i):
            for h in HALVES:
                load_mine(kind, h, i).start()
            for h in HALVES:
                partner_copy(kind, h, i).wait_recv()
                load_part(kind, h, i).start()
                if kind == KIND_S:
                    link_copy(KIND_D, h, i).wait_recv()
                    load_link(land_d, first, 2, h, i).start()
            for h in HALVES:
                load_mine(kind, h, i).wait()
                load_part(kind, h, i).wait()
                total = mine[h] + part[h]
                if kind == KIND_S:
                    load_link(land_d, first, 2, h, i).wait()
                    total = total + first[h]
                sums[kind, h, i] = total
                link_copy(kind, h, i).start()

    @pl.loop(0, 4 * UNITS)
    def _(n):
        place, unit = n // UNITS, lax.rem(n, UNITS)
        flip_x, flip_y = 1 - place // 2, 1 - lax.rem(place, 2)
        chip = (x + flip_x * (1 - 2 * x)) + 2 * (y + flip_y * (1 - 2 * y))
        for case in range(4 * UNITS):
            @pl.when(UNITS * chip + unit == case)
            def _():
                pack(place, case // UNITS, case % UNITS)

        @pl.when(n == 0)
        def _():
            pl.semaphore_wait(barrier, NDEV - 1)

        @pl.when(n < UNITS)
        def _():
            exchange((KIND_D,), 4 * unit, 4 * unit + 4)
            send(KIND_D, 4 * unit, 4 * unit + 4)

        @pl.when(n == 3 * UNITS - 1)
        def _():
            exchange((KIND_N, KIND_S), 0, CHUNKS)
            send(KIND_N, 0, CHUNKS)

    exchange((KIND_O,), 0, CHUNKS)
    send(KIND_S, 0, CHUNKS)

    def last(i, acc):
        for h in HALVES:
            load_mine(KIND_O, h, i).start()
            partner_copy(KIND_O, h, i).wait_recv()
            load_part(KIND_O, h, i).start()
        for h in HALVES:
            link_copy(KIND_N, h, i).wait_recv()
            load_link(land_n, first, 2, h, i).start()
        for h in HALVES:
            link_copy(KIND_S, h, i).wait_recv()
            load_link(land_s, second, 3, h, i).start()
            load_mine(KIND_O, h, i).wait()
            load_part(KIND_O, h, i).wait()
            load_link(land_n, first, 2, h, i).wait()
            load_link(land_s, second, 3, h, i).wait()

            @pl.when(i > 0)
            def _():
                store_g(h, i - 1).wait()

            g = ((mine[h] + part[h]) + (first[h] + second[h])) * (1.0 / NDEV)
            g_buf[h] = g
            store_g(h, i).start()
            square = g * g
            if h == 1:
                row = lax.broadcasted_iota(jnp.int32, (RS_ROWS, LANES), 0) + RS_ROWS * i
                square = jnp.where(row >= CHUNKS * RS_ROWS - RS_HALF_START, square, 0.0)
            acc = acc + jnp.sum(square, axis=0, keepdims=True)
        return acc

    acc = lax.fori_loop(0, CHUNKS, last, jnp.zeros((1, LANES), F32))
    ss[...] = jnp.broadcast_to(acc, (8, LANES))

    @pl.loop(0, CHUNKS)
    def _(i):
        for h in HALVES:
            for kind in range(4):
                partner_copy(kind, h, i).wait_send()
            for kind in range(3):
                link_copy(kind, h, i).wait_send()

    def norm_copy(d):
        return pltpu.make_async_remote_copy(
            src_ref=ss, dst_ref=ss_all.at[d], send_sem=ss_send.at[d], recv_sem=ss_recv.at[d],
            device_id=(lax.rem(me + d, NDEV),), device_id_type=MESH)

    for d in range(1, NDEV):
        norm_copy(d).start()
    for h in HALVES:
        store_g(h, CHUNKS - 1).wait()
    ss_all[0] = ss[...]
    for d in range(1, NDEV):
        norm_copy(d).wait()
    total = jnp.zeros((8, LANES), F32)
    for dev in range(NDEV):
        total = total + ss_all[lax.rem(me - dev + NDEV, NDEV)]
    norm_out[...] = jnp.broadcast_to(jnp.sqrt(jnp.sum(total, axis=1, keepdims=True)), (8, LANES))


def reduce_grads(grads, norms):
    land = jax.ShapeDtypeStruct((2, CHUNKS, RS_ROWS, 1, LANES), F32)
    land_p = jax.ShapeDtypeStruct((4, 2, CHUNKS, RS_ROWS, 1, LANES), F32)
    flat = jax.ShapeDtypeStruct((4, UNITS, 2, 2, UNIT_ROWS + 2 * MARGIN, 1, LANES), F32)
    buf = pltpu.VMEM((2, RS_ROWS, LANES), F32)
    partner, link, pair, all_devs, slots = DMA((4, 2, CHUNKS)), DMA((3, 2, CHUNKS)), DMA((2,)), DMA((NDEV,)), DMA((PACK_SLOTS,))
    outs = pl.pallas_call(
        reduce_kernel,
        name="reduce_grads",
        out_shape=[jax.ShapeDtypeStruct((SEG, 1, LANES), F32), jax.ShapeDtypeStruct((8, LANES), F32), flat, land_p, land, land, land],
        in_specs=[ANY] * 7 + [VMEM_SPEC] * 3,
        out_specs=[ANY, VMEM_SPEC] + [ANY] * 5,
        scratch_shapes=[buf] * 4 + [pltpu.VMEM((3, 2, CHUNKS, RS_ROWS, LANES), F32), buf, pltpu.VMEM((8, LANES), F32), pltpu.VMEM((NDEV, 8, LANES), F32)]
        + tile_scratch(PACK_SLOTS, PACK_ROWS.values()) + [pltpu.VMEM((PACK_SLOTS, PACK_STAGE, LANES), F32), pltpu.VMEM((TAIL, LANES), F32)]
        + [partner, partner, link, link, DMA((4, 2)), pair, all_devs, all_devs, slots, slots, DMA],
        compiler_params=pltpu.CompilerParams(collective_id=0, has_side_effects=True, vmem_limit_bytes=VMEM_LIMIT),
        cost_estimate=COST,
    )(*grads, *norms)
    return outs[0], outs[1]


def adam_rows(g, m, v, p, norm_row, lr, decay):
    clip = jnp.minimum(1.0, MAX_NORM / (norm_row + CLIP_EPS))
    clipped = clip * g
    new_m = BETA_ONE * m + (1.0 - BETA_ONE) * clipped
    new_v = BETA_TWO * v + (1.0 - BETA_TWO) * clipped * clipped
    adam_dir = (new_m * (1.0 / BIAS_ONE)) / (jnp.sqrt(new_v * (1.0 / BIAS_TWO)) + ADAM_EPS)
    decay_term = jnp.where(decay, WEIGHT_DECAY * p, 0.0)
    return p - lr * (decay_term + adam_dir), new_m, new_v


UP_ROWS = 1824
UP_LAST = SEG - 15 * UP_ROWS
SUB = 152


def decay_rows(me, start, rows):
    return lax.broadcasted_iota(jnp.int32, (rows, LANES), 0) + (SEG * me + start) < MATRIX_ROWS


def gather_kernel(g, m, v, p, norm, lr, full, late, gb, mb, vb, pb, new_p, late_p,
                  load_sem, own_sem, late_sem, own_send, own_recv, fwd_send, fwd_recv, p_send, p_recv):
    me, other, dev_x, dev_y, dev_d = neighbours()
    partner = me + other
    barrier = pltpu.get_barrier_semaphore()
    for dev in (partner, dev_x, dev_y):
        pl.semaphore_signal(barrier, inc=1, device_id=(dev,), device_id_type=MESH)
    to = (dev_x, dev_y, partner)
    sources = (me, dev_x, dev_y, dev_d)

    def is_last(h, i):
        return h == 1 and isinstance(i, int) and i == HALF - 1

    def start_row(h, i):
        return PIECE * (PIECES - 1) if is_last(h, i) else PIECE * (HALF * h + i)

    def size(h, i):
        return PIECE_LAST if is_last(h, i) else PIECE

    def rows_of(dev, h, i):
        return full.at[pl.ds(SEG * dev + start_row(h, i), size(h, i)), 0]

    def loads(h, i):
        return loads_at(h, start_row(h, i), size(h, i))

    def loads_at(h, start, rows):
        start = pl.multiple_of(start, 8)
        copies = [pltpu.make_async_copy(g.at[pl.ds(start, rows), 0], gb.at[h, pl.ds(0, rows)], load_sem.at[0, h])]
        for n, (src, buf) in enumerate(((m, mb), (v, vb), (p, pb))):
            copies.append(pltpu.make_async_copy(src.at[pl.ds(start, rows)], buf.at[h, pl.ds(0, rows)], load_sem.at[n + 1, h]))
        return copies

    def own_copy(n, h, i):
        return pltpu.make_async_remote_copy(
            src_ref=new_p.at[h, i, pl.ds(0, size(h, i))], dst_ref=rows_of(me, h, i),
            send_sem=own_send.at[n, h, i], recv_sem=own_recv.at[n, h, i], device_id=(to[n],), device_id_type=MESH)

    def own_store(h, i):
        return pltpu.make_async_copy(new_p.at[h, i, pl.ds(0, size(h, i))], rows_of(me, h, i), own_sem.at[h, i])

    def forward(h, i):
        src = rows_of((dev_y, dev_x)[h], h, i)
        return pltpu.make_async_remote_copy(
            src_ref=src, dst_ref=src, send_sem=fwd_send.at[h, i], recv_sem=fwd_recv.at[h, i],
            device_id=((dev_x, dev_y)[h],), device_id_type=MESH)

    def arrival(n, h, i):
        src = rows_of((dev_x, dev_y, partner)[n], h, i)
        return pltpu.make_async_remote_copy(
            src_ref=src, dst_ref=src, send_sem=own_send.at[n, h, i], recv_sem=own_recv.at[n, h, i],
            device_id=(to[n],), device_id_type=MESH)

    def forward_arrival(h, i):
        src = rows_of(dev_d, h, i)
        return pltpu.make_async_remote_copy(
            src_ref=src, dst_ref=src, send_sem=fwd_send.at[h, i], recv_sem=fwd_recv.at[h, i],
            device_id=((dev_x, dev_y)[h],), device_id_type=MESH)

    def partner_copy(q, h, i):
        src = rows_of(sources[q], h, i)
        return pltpu.make_async_remote_copy(
            src_ref=src, dst_ref=src, send_sem=p_send.at[q - 1, h, i], recv_sem=p_recv.at[q - 1, h, i],
            device_id=(partner,), device_id_type=MESH)

    def partner_arrival(q, h, i):
        src = rows_of(sources[q] + other, h, i)
        return pltpu.make_async_remote_copy(
            src_ref=src, dst_ref=src, send_sem=p_send.at[q - 1, h, i], recv_sem=p_recv.at[q - 1, h, i],
            device_id=(partner,), device_id_type=MESH)

    def each(body):
        @pl.loop(0, HALF - 1)
        def _(i):
            body(i)

        body(HALF - 1)

    norm_row = norm[0:1, :]
    for h in HALVES:
        for copy in loads(h, 0):
            copy.start()
    pl.semaphore_wait(barrier, 3)

    def compute(h, out, first):
        @pl.loop(0, PIECE // SUB)
        def _(s):
            start = pl.multiple_of(s * SUB, 8)
            sub = pl.ds(start, SUB)
            out[sub] = adam_rows(gb[h, sub], mb[h, sub], vb[h, sub], pb[h, sub], norm_row, lr[0], decay_rows(me, first + start, SUB))[0]

    def update(i):
        for h in HALVES:
            for copy in loads(h, i):
                copy.wait()

            compute(h, new_p.at[h, i], start_row(h, i))
            for n in ((1, 0, 2) if h == 0 else (0, 1, 2)):
                own_copy(n, h, i).start()
            own_store(h, i).start()
            if isinstance(i, int):
                continue
            for last in (False, True):
                @pl.when((i == HALF - 2) == last)
                def _():
                    for copy in loads(h, HALF - 1 if last else i + 1):
                        copy.start()

    each(update)

    def late_store(src, to, n):
        return pltpu.make_async_copy(src, late.at[pl.ds(to, src.shape[0]), 0], late_sem.at[n])

    def late_piece(j):
        return late_store(late_p.at[j], 8 + PIECE * j, j)

    edges = [late_store(new_p.at[1, HALF - 2, pl.ds(PIECE - 8, 8)], 0, 6),
             late_store(new_p.at[1, HALF - 1, pl.ds(0, 8)], LATE_ROWS - 8, 7)]
    for copy in edges:
        copy.start()

    @pl.loop(0, LATE_END - LATE_FIRST)
    def _(j):
        first = PIECE * (LATE_FIRST + j)
        for copy in loads_at(0, first, PIECE):
            copy.start()
        for copy in loads_at(0, first, PIECE):
            copy.wait()
        compute(0, late_p.at[j], first)
        late_piece(j).start()

    def pass_on(i):
        arrival(1, 0, i).wait_recv()
        forward(0, i).start()
        partner_copy(2, 0, i).start()
        arrival(0, 1, i).wait_recv()
        forward(1, i).start()
        partner_copy(1, 1, i).start()
        arrival(0, 0, i).wait_recv()
        partner_copy(1, 0, i).start()
        arrival(1, 1, i).wait_recv()
        partner_copy(2, 1, i).start()

    each(pass_on)

    def pass_last(i):
        for h in HALVES:
            forward_arrival(h, i).wait_recv()
            partner_copy(3, h, i).start()

    each(pass_last)

    def finish(i):
        for h in HALVES:
            own_store(h, i).wait()
            arrival(2, h, i).wait_recv()
            for n in range(3):
                own_copy(n, h, i).wait_send()
            forward(h, i).wait_send()
            for q in range(1, 4):
                partner_copy(q, h, i).wait_send()
                partner_arrival(q, h, i).wait_recv()

    each(finish)
    for copy in edges:
        copy.wait()

    @pl.loop(0, LATE_END - LATE_FIRST)
    def _(j):
        late_piece(j).wait()


def gather_params(g, m, v, p, norm, lr):
    buf = pltpu.VMEM((2, PIECE, LANES), F32)
    pairs = DMA((2, HALF))
    triples = DMA((3, 2, HALF))
    return pl.pallas_call(
        gather_kernel,
        name="gather_params",
        out_shape=[jax.ShapeDtypeStruct((FLAT_ROWS, 1, LANES), F32), jax.ShapeDtypeStruct((LATE_ROWS, 1, LANES), F32)],
        in_specs=[ANY] * 4 + [VMEM_SPEC, SMEM_SPEC],
        out_specs=[ANY, ANY],
        scratch_shapes=[buf, buf, buf, buf, pltpu.VMEM((2, HALF, PIECE, LANES), F32), pltpu.VMEM((LATE_END - LATE_FIRST, PIECE, LANES), F32),
                        DMA((4, 2)), pairs, DMA((8,)), triples, triples, pairs, pairs, triples, triples],
        compiler_params=pltpu.CompilerParams(collective_id=1, has_side_effects=True, vmem_limit_bytes=VMEM_LIMIT),
        cost_estimate=COST,
    )(g, m, v, p, norm, lr)


def state_kernel(g, m, v, p, norm, lr, new_p, new_m, new_v, gb, g_sem):
    me = lax.axis_index("dp")
    i = pl.program_id(0)

    def load(j, last):
        rows = UP_LAST if last else UP_ROWS
        return pltpu.make_async_copy(g.at[pl.ds(j * UP_ROWS, rows), 0], gb.at[lax.rem(j, 2), pl.ds(0, rows)], g_sem.at[lax.rem(j, 2)])

    @pl.when(i == 0)
    def _():
        load(i, False).start()

    @pl.when(i < 14)
    def _():
        load(i + 1, False).start()

    @pl.when(i == 14)
    def _():
        load(i + 1, True).start()

    @pl.when(i < 15)
    def _():
        load(i, False).wait()

    @pl.when(i == 15)
    def _():
        load(i, True).wait()

    norm_row = norm[0:1, :]

    @pl.loop(0, UP_ROWS // SUB)
    def _(s):
        start = pl.multiple_of(s * SUB, 8)
        rows = pl.ds(start, SUB)
        new_p[rows], new_m[rows], new_v[rows] = adam_rows(
            gb[lax.rem(i, 2), rows], m[rows], v[rows], p[rows], norm_row, lr[0], decay_rows(me, i * UP_ROWS + start, SUB))


def new_state(g, m, v, p, norm, lr):
    block = pl.BlockSpec((UP_ROWS, LANES), lambda i: (i, 0))
    return pl.pallas_call(
        state_kernel,
        name="new_state",
        grid=(16,),
        out_shape=[jax.ShapeDtypeStruct((SEG, LANES), F32)] * 3,
        in_specs=[ANY, block, block, block, pl.BlockSpec((8, LANES), lambda i: (0, 0)), SMEM_SPEC],
        out_specs=[block] * 3,
        scratch_shapes=[pltpu.VMEM((2, UP_ROWS, LANES), F32), DMA((2,))],
        compiler_params=pltpu.CompilerParams(vmem_limit_bytes=VMEM_LIMIT),
        cost_estimate=COST,
    )(g, m, v, p, norm, lr)


def solution(mesh):
    def local_step(*arrays):
        grads = [a.reshape(r, w * LANES) for a, r, w in zip(arrays[:7], NAMES_ROWS, WIDTHS)]
        norms = [a.reshape(s) for a, s in zip(arrays[7:10], GAINS)]
        master, exp_avg, exp_avg_sq = [a.reshape(SEG, LANES) for a in arrays[10:13]]
        lr = arrays[13].reshape(1)
        g, norm = reduce_grads(grads, norms)
        full, late = gather_params(g, exp_avg, exp_avg_sq, master, norm, lr)
        late = lax.all_gather(late, "dp", tiled=True)
        state = new_state(g, exp_avg, exp_avg_sq, master, norm, lr)
        params = unpack_late(full, late, unpack_early(full))
        shapes = SHAPES + GAINS[:2] + [(D,)]
        return tuple([a.reshape(-1) for a in state] + [a.reshape(s) for a, s in zip(params, shapes)] + [norm[0, 0]])

    return jax.shard_map(local_step, mesh=mesh, in_specs=(P("dp"),) * 13 + (P(),), out_specs=(P("dp"),) * 3 + (P(),) * 11, check_vma=False)
```

```python
import math
import jax
import jax.numpy as jnp
from jax import lax
from jax.experimental import pallas as pl
from jax.experimental.pallas import tpu as pltpu
from jax.sharding import PartitionSpec as P

BETA_ONE = 0.9
BETA_TWO = 0.95
ADAM_EPS = 1e-8
WEIGHT_DECAY = 0.1
MAX_NORM = 1.0
CLIP_EPS = 1e-6
STEP = 4
BIAS_ONE = 1.0 - BETA_ONE ** STEP
BIAS_TWO = 1.0 - BETA_TWO ** STEP

MESH = pl.DeviceIdType.MESH
F32 = jnp.float32
BF16 = jnp.bfloat16
LANES = 128

LAYERS, D, KV, FF = 2, 896, 128, 4864
SHAPES = [(LAYERS, D, D), (LAYERS, D, KV), (LAYERS, D, KV), (LAYERS, D, D), (LAYERS, D, FF), (LAYERS, D, FF), (LAYERS, FF, D)]
GAINS = [(LAYERS, D), (LAYERS, D), (1, D)]
TAIL = 40
HALVES, TENSORS, COLUMNS = range(2), range(7), range(7)
NAMES_ROWS = [math.prod(s[:-1]) for s in SHAPES]
WIDTHS = [s[-1] // LANES for s in SHAPES]
OFFSETS = [sum(r * w for r, w in zip(NAMES_ROWS[:t], WIDTHS[:t])) for t in TENSORS]
BLOCK_ROWS = [448, 1792, 1792, 448, 128, 128, 608]
MATRIX_ROWS = 232960
FLAT_ROWS = 233000
SEG = 29125
NDEV = 8

WIDTH_ORDER = (38, 7, 1)
GROUPS = {38: (16,), 7: (16, 32, 64), 1: (16, 128, 256)}
STAGE_ROWS = max(br * WIDTHS[t] for t, br in enumerate(BLOCK_ROWS))


def split(refs, counts):
    refs = list(refs)
    return [[refs.pop(0) for _ in range(n)] for n in counts]


ANY = pl.BlockSpec(memory_space=pl.ANY)
VMEM_SPEC = pl.BlockSpec(memory_space=pltpu.VMEM)
SMEM_SPEC = pl.BlockSpec(memory_space=pltpu.SMEM)
DMA = pltpu.SemaphoreType.DMA
VMEM_LIMIT = 63 * 1024 * 1024
COST = pl.CostEstimate(flops=2 * 10 ** 8, bytes_accessed=10 ** 8, transcendentals=0)


def tile_scratch(slots, rows):
    return [pltpu.VMEM((slots, r, w * LANES), BF16) for r, w in zip(rows, WIDTH_ORDER)]


def width_slot(width):
    return WIDTH_ORDER.index(width)


def row_group(rows, width):
    return max(g for g in GROUPS[width] if rows % g == 0)


PIECE = 480
PIECES = 61
LATE_FIRST, LATE_END = 51, 60
LATE_ROWS = PIECE * (LATE_END - LATE_FIRST) + 16
PIECE_LAST = SEG - (PIECES - 1) * PIECE
HALF = (PIECES - LATE_END + LATE_FIRST) // 2
LATE_RANGES = [((SEG * s + PIECE * LATE_FIRST) // 8 * 8, -(-(SEG * s + PIECE * LATE_END) // 8) * 8) for s in range(NDEV)]


def unpack_blocks():
    early, late = [], []
    for t in TENSORS:
        w, offset, total = WIDTHS[t], OFFSETS[t], NAMES_ROWS[t]
        cuts = {0, total}
        spans = []
        for low, high in LATE_RANGES:
            first = max(0, (low - offset) // (16 * w) * 16)
            end = min(total, -(-(high - offset) // (16 * w)) * 16)
            if first < end:
                spans.append((first, end))
                cuts |= {first, end}
        cuts = sorted(cuts)
        for begin, end in zip(cuts[:-1], cuts[1:]):
            is_late = any(first <= begin and end <= last for first, last in spans)
            count = -(-(end - begin) // BLOCK_ROWS[t])
            step = -(-(end - begin) // (16 * count)) * 16
            for row in range(begin, end, step):
                rows = min(step, end - row)
                low, high = offset + row * w, offset + (row + rows) * w
                edges = sorted({low, high} | {e for r in LATE_RANGES for e in r if low < e < high})
                sources = []
                for e0, e1 in zip(edges[:-1], edges[1:]):
                    seg = [s for s, (l, h) in enumerate(LATE_RANGES) if l <= e0 and e1 <= h]
                    start = LATE_ROWS * seg[0] + e0 - SEG * seg[0] - PIECE * LATE_FIRST + 8 if seg else e0
                    sources.append((bool(seg), start, e0 - low, e1 - e0))
                (late if is_late else early).append((t, row, rows, sources))
    return early, late


EARLY_BLOCKS, LATE_BLOCKS = unpack_blocks()
LATE_TENSORS = sorted({t for t, _, _, _ in LATE_BLOCKS})
SLOTS = 4


def unpack_body(blocks, sources, outs, tiles, stage, in_sem, out_sem):
    def loads(b):
        return [pltpu.make_async_copy(sources[late].at[pl.ds(start, rows), 0], stage.at[b % SLOTS, pl.ds(to, rows)], in_sem.at[b % SLOTS, n])
                for n, (late, start, to, rows) in enumerate(blocks[b][3])]

    def store(b):
        t, row, rows, _ = blocks[b]
        return pltpu.make_async_copy(tiles[width_slot(WIDTHS[t])].at[b % SLOTS, pl.ds(0, rows)], outs[t].at[pl.ds(row, rows)], out_sem.at[b % SLOTS])

    for b in range(min(SLOTS, len(blocks))):
        for copy in loads(b):
            copy.start()
    yield
    for b, (t, row, rows, _) in enumerate(blocks):
        w = WIDTHS[t]
        tile = tiles[width_slot(w)]
        group = row_group(rows, w)
        for copy in loads(b):
            copy.wait()
        if b >= SLOTS:
            store(b - SLOTS).wait()

        @pl.loop(0, rows // group)
        def _(i):
            for j in range(w):
                if w == 1:
                    block = stage[b % SLOTS, pl.ds(pl.multiple_of(i * group, 16), group), :]
                else:
                    block = stage[b % SLOTS, pl.ds(i * (group * w) + j, group, stride=w), :]
                tile[b % SLOTS, pl.ds(pl.multiple_of(i * group, 16), group), pl.ds(j * LANES, LANES)] = block.astype(BF16)

        store(b).start()
        if b + SLOTS < len(blocks):
            for copy in loads(b + SLOTS):
                copy.start()
    for b in range(max(0, len(blocks) - SLOTS), len(blocks)):
        store(b).wait()


UNPACK_SCRATCH = tile_scratch(SLOTS, (128, 608, 1792)) + [pltpu.VMEM((SLOTS, STAGE_ROWS, LANES), F32)]
TENSOR_TYPES = [jax.ShapeDtypeStruct((r, w * LANES), BF16) for r, w in zip(NAMES_ROWS, WIDTHS)]


def unpack_early_kernel(flat, *refs):
    outs, norms = refs[:7], refs[7:10]
    tiles, stage, tail, in_sem, out_sem, tail_sem = refs[10:13], refs[13], refs[14], refs[15], refs[16], refs[17]
    tail_copy = pltpu.make_async_copy(flat.at[pl.ds(MATRIX_ROWS, TAIL), 0], tail, tail_sem)
    tail_copy.start()
    work = unpack_body(EARLY_BLOCKS, (flat, None), outs, tiles, stage, in_sem, out_sem)
    next(work)
    tail_copy.wait()
    base = 0
    for n in norms:
        for j in COLUMNS:
            lines = [tail[pl.ds(base + j + 7 * layer, 1), :] for layer in range(n.shape[0])]
            n[:, pl.ds(j * LANES, LANES)] = jnp.concatenate(lines, axis=0).astype(BF16)
        base += 7 * n.shape[0]
    for _ in work:
        pass


def unpack_early(flat):
    return pl.pallas_call(
        unpack_early_kernel,
        name="unpack_early",
        out_shape=TENSOR_TYPES + [jax.ShapeDtypeStruct(s, BF16) for s in GAINS],
        in_specs=[ANY],
        out_specs=[ANY] * 7 + [VMEM_SPEC] * 3,
        scratch_shapes=UNPACK_SCRATCH + [pltpu.VMEM((TAIL, LANES), F32), DMA((SLOTS, 3)), DMA((SLOTS,)), DMA],
        compiler_params=pltpu.CompilerParams(vmem_limit_bytes=VMEM_LIMIT),
        cost_estimate=COST,
    )(flat)


def unpack_late_kernel(flat, late, *refs):
    count = len(LATE_TENSORS)
    outs = dict(zip(LATE_TENSORS, refs[count:2 * count]))
    tiles, stage, in_sem, out_sem = refs[2 * count:2 * count + 3], refs[2 * count + 3], refs[2 * count + 4], refs[2 * count + 5]
    for _ in unpack_body(LATE_BLOCKS, (flat, late), outs, tiles, stage, in_sem, out_sem):
        pass


def unpack_late(flat, late, params):
    count = len(LATE_TENSORS)
    outs = pl.pallas_call(
        unpack_late_kernel,
        name="unpack_late",
        out_shape=[TENSOR_TYPES[t] for t in LATE_TENSORS],
        in_specs=[ANY] * (2 + count),
        out_specs=[ANY] * count,
        input_output_aliases={2 + n: n for n in range(count)},
        scratch_shapes=UNPACK_SCRATCH + [DMA((SLOTS, 3)), DMA((SLOTS,))],
        compiler_params=pltpu.CompilerParams(vmem_limit_bytes=VMEM_LIMIT),
        cost_estimate=COST,
    )(flat, late, *[params[t] for t in LATE_TENSORS])
    params = list(params)
    for t, out in zip(LATE_TENSORS, outs):
        params[t] = out
    return params


def neighbours():
    me = lax.axis_index("dp")
    core, x, y = lax.rem(me, 2), lax.rem(me // 2, 2), me // 4
    other = 1 - 2 * core
    step_x, step_y = 2 - 4 * x, 4 - 8 * y
    return me, other, me + step_x, me + step_y, me + step_x + step_y


CHUNKS = 16
RS_ROWS = 911
RS_HALF_START = SEG - CHUNKS * RS_ROWS
UNITS = CHUNKS // 4
KIND_D, KIND_N, KIND_S, KIND_O = range(4)
CHIP_D, CHIP_X, CHIP_Y, CHIP_OWN = range(4)
UNIT_ROWS = 4 * RS_ROWS
MARGIN = 16 * 38
PACK_ROWS = {38: 112, 7: 608, 1: 896}
PACK_STAGE = 112 * 38
PACK_SLOTS = 3


def pack_blocks(chip, unit):
    blocks = []
    for parity in HALVES:
        for h in HALVES:
            begin = SEG * (2 * chip + parity) + RS_HALF_START * h + UNIT_ROWS * unit
            for t in TENSORS:
                w, offset, total = WIDTHS[t], OFFSETS[t], NAMES_ROWS[t]
                low, high = max(begin, offset), min(begin + UNIT_ROWS, offset + total * w)
                if low >= high:
                    continue
                first = (low - offset) // (16 * w) * 16
                end = -(-(high - offset) // (16 * w)) * 16
                step = -(-(end - first) // (16 * -(-(end - first) // PACK_ROWS[w]))) * 16
                for row in range(first, end, step):
                    blocks.append((t, row, min(step, end - row), parity, h, offset + row * w - begin + MARGIN))
    return blocks


def reduce_kernel(*refs):
    (grads, norms, (g_out, norm_out, flat, land_p, land_d, land_n, land_s),
     (mine, part, first, second, sums, g_buf, ss, ss_all), tiles, (stage, tail),
     (p_send, p_recv, i_send, i_recv, load_sem, g_sem, ss_send, ss_recv, in_sem, out_sem, tail_sem)) = split(refs, (7, 3, 7, 8, 3, 2, 11))
    me, other, dev_x, dev_y, _ = neighbours()
    core, x, y = lax.rem(me, 2), lax.rem(me // 2, 2), me // 4
    barrier = pltpu.get_barrier_semaphore()
    for d in range(1, NDEV):
        pl.semaphore_signal(barrier, inc=1, device_id=(lax.rem(me + d, NDEV),), device_id_type=MESH)

    tail[...] = jnp.zeros_like(tail)
    line = 0
    for n in norms:
        for layer in range(n.shape[0]):
            for j in COLUMNS:
                tail[pl.ds(line, 1), :] = n[pl.ds(layer, 1), pl.ds(j * LANES, LANES)].astype(F32)
                line += 1

    def pack(place, chip, unit):
        blocks = pack_blocks(chip, unit)

        def load(b):
            t, row, rows = blocks[b][:3]
            return pltpu.make_async_copy(grads[t].at[pl.ds(row, rows)], tiles[width_slot(WIDTHS[t])].at[b % PACK_SLOTS, pl.ds(0, rows)], in_sem.at[b % PACK_SLOTS])

        def store(b):
            t, _, rows, parity, h, to = blocks[b]
            size = rows * WIDTHS[t]
            return pltpu.make_async_copy(stage.at[b % PACK_SLOTS, pl.ds(0, size)], flat.at[place, unit, parity, h, pl.ds(to, size), 0], out_sem.at[b % PACK_SLOTS])

        for b in range(PACK_SLOTS):
            load(b).start()
        tail_copies = [pltpu.make_async_copy(tail, flat.at[place, unit, 1, 1, pl.ds(MARGIN + UNIT_ROWS - TAIL, TAIL), 0], tail_sem)
                       for _ in range(chip * unit // (3 * UNITS - 3))]
        for copy in tail_copies:
            copy.start()
        for b, block in enumerate(blocks):
            t, rows = block[0], block[2]
            w = WIDTHS[t]
            tile = tiles[width_slot(w)]
            group = row_group(rows, w)
            load(b).wait()
            if b >= PACK_SLOTS:
                store(b - PACK_SLOTS).wait()

            @pl.loop(0, rows // group)
            def _(i):
                for j in range(w):
                    values = tile[b % PACK_SLOTS, pl.ds(pl.multiple_of(i * group, 16), group), pl.ds(j * LANES, LANES)].astype(F32)
                    if w == 1:
                        stage[b % PACK_SLOTS, pl.ds(pl.multiple_of(i * group, 16), group), :] = values
                    else:
                        stage[b % PACK_SLOTS, pl.ds(i * (group * w) + j, group, stride=w), :] = values

            store(b).start()
            if b + PACK_SLOTS < len(blocks):
                load(b + PACK_SLOTS).start()
        for b in range(len(blocks) - PACK_SLOTS, len(blocks)):
            store(b).wait()
        for copy in tail_copies:
            copy.wait()

    def place_of(kind, h):
        return ((CHIP_D, CHIP_D), (CHIP_X, CHIP_Y), (CHIP_Y, CHIP_X), (CHIP_OWN, CHIP_OWN))[kind][h]

    def chunk(kind, h, i, parity):
        return flat.at[place_of(kind, h), i // 4, parity, h, pl.ds(MARGIN + RS_ROWS * lax.rem(i, 4), RS_ROWS)]

    def start_row(h, i):
        return RS_HALF_START * h + RS_ROWS * i

    def partner_copy(kind, h, i):
        return pltpu.make_async_remote_copy(
            src_ref=chunk(kind, h, i, 1 - core), dst_ref=land_p.at[kind, h, i],
            send_sem=p_send.at[kind, h, i], recv_sem=p_recv.at[kind, h, i],
            device_id=(me + other,), device_id_type=MESH)

    def link_copy(kind, h, i):
        land = (land_d, land_n, land_s)[kind]
        to = ((dev_x, dev_y), (dev_x, dev_y), (dev_y, dev_x))[kind][h]
        return pltpu.make_async_remote_copy(
            src_ref=sums.at[kind, h, i], dst_ref=land.at[h, i, pl.ds(0, RS_ROWS), 0],
            send_sem=i_send.at[kind, h, i], recv_sem=i_recv.at[kind, h, i],
            device_id=(to,), device_id_type=MESH)

    def load_mine(kind, h, i):
        return pltpu.make_async_copy(chunk(kind, h, i, core).at[:, 0], mine.at[h], load_sem.at[0, h])

    def load_part(kind, h, i):
        return pltpu.make_async_copy(land_p.at[kind, h, i, pl.ds(0, RS_ROWS), 0], part.at[h], load_sem.at[1, h])

    def load_link(land, buf, n, h, i):
        return pltpu.make_async_copy(land.at[h, i, pl.ds(0, RS_ROWS), 0], buf.at[h], load_sem.at[n, h])

    def store_g(h, i):
        return pltpu.make_async_copy(g_buf.at[h], g_out.at[pl.ds(start_row(h, i), RS_ROWS), 0], g_sem.at[h])

    def exchange(kinds, begin, end):
        @pl.loop(begin, end)
        def _(i):
            for kind in kinds:
                for h in HALVES:
                    partner_copy(kind, h, i).start()

    def send(kind, begin, end):
        @pl.loop(begin, end)
        def _(i):
            for h in HALVES:
                load_mine(kind, h, i).start()
            for h in HALVES:
                partner_copy(kind, h, i).wait_recv()
                load_part(kind, h, i).start()
                if kind == KIND_S:
                    link_copy(KIND_D, h, i).wait_recv()
                    load_link(land_d, first, 2, h, i).start()
            for h in HALVES:
                load_mine(kind, h, i).wait()
                load_part(kind, h, i).wait()
                total = mine[h] + part[h]
                if kind == KIND_S:
                    load_link(land_d, first, 2, h, i).wait()
                    total = total + first[h]
                sums[kind, h, i] = total
                link_copy(kind, h, i).start()

    @pl.loop(0, 4 * UNITS)
    def _(n):
        place, unit = n // UNITS, lax.rem(n, UNITS)
        flip_x, flip_y = 1 - place // 2, 1 - lax.rem(place, 2)
        chip = (x + flip_x * (1 - 2 * x)) + 2 * (y + flip_y * (1 - 2 * y))
        for case in range(4 * UNITS):
            @pl.when(UNITS * chip + unit == case)
            def _():
                pack(place, case // UNITS, case % UNITS)

        @pl.when(n == 0)
        def _():
            pl.semaphore_wait(barrier, NDEV - 1)

        @pl.when(n < UNITS)
        def _():
            exchange((KIND_D,), 4 * unit, 4 * unit + 4)
            send(KIND_D, 4 * unit, 4 * unit + 4)

        @pl.when(n == 3 * UNITS - 1)
        def _():
            exchange((KIND_N, KIND_S), 0, CHUNKS)
            send(KIND_N, 0, CHUNKS)

    exchange((KIND_O,), 0, CHUNKS)
    send(KIND_S, 0, CHUNKS)

    def last(i, acc):
        for h in HALVES:
            load_mine(KIND_O, h, i).start()
            partner_copy(KIND_O, h, i).wait_recv()
            load_part(KIND_O, h, i).start()
        for h in HALVES:
            link_copy(KIND_N, h, i).wait_recv()
            load_link(land_n, first, 2, h, i).start()
        for h in HALVES:
            link_copy(KIND_S, h, i).wait_recv()
            load_link(land_s, second, 3, h, i).start()
            load_mine(KIND_O, h, i).wait()
            load_part(KIND_O, h, i).wait()
            load_link(land_n, first, 2, h, i).wait()
            load_link(land_s, second, 3, h, i).wait()

            @pl.when(i > 0)
            def _():
                store_g(h, i - 1).wait()

            g = ((mine[h] + part[h]) + (first[h] + second[h])) * (1.0 / NDEV)
            g_buf[h] = g
            store_g(h, i).start()
            square = g * g
            if h == 1:
                row = lax.broadcasted_iota(jnp.int32, (RS_ROWS, LANES), 0) + RS_ROWS * i
                square = jnp.where(row >= CHUNKS * RS_ROWS - RS_HALF_START, square, 0.0)
            acc = acc + jnp.sum(square, axis=0, keepdims=True)
        return acc

    acc = lax.fori_loop(0, CHUNKS, last, jnp.zeros((1, LANES), F32))
    ss[...] = jnp.broadcast_to(acc, (8, LANES))

    @pl.loop(0, CHUNKS)
    def _(i):
        for h in HALVES:
            for kind in range(4):
                partner_copy(kind, h, i).wait_send()
            for kind in range(3):
                link_copy(kind, h, i).wait_send()

    def norm_copy(d):
        return pltpu.make_async_remote_copy(
            src_ref=ss, dst_ref=ss_all.at[d], send_sem=ss_send.at[d], recv_sem=ss_recv.at[d],
            device_id=(lax.rem(me + d, NDEV),), device_id_type=MESH)

    for d in range(1, NDEV):
        norm_copy(d).start()
    for h in HALVES:
        store_g(h, CHUNKS - 1).wait()
    ss_all[0] = ss[...]
    for d in range(1, NDEV):
        norm_copy(d).wait()
    total = jnp.zeros((8, LANES), F32)
    for dev in range(NDEV):
        total = total + ss_all[lax.rem(me - dev + NDEV, NDEV)]
    norm_out[...] = jnp.broadcast_to(jnp.sqrt(jnp.sum(total, axis=1, keepdims=True)), (8, LANES))


def reduce_grads(grads, norms):
    land = jax.ShapeDtypeStruct((2, CHUNKS, RS_ROWS, 1, LANES), F32)
    land_p = jax.ShapeDtypeStruct((4, 2, CHUNKS, RS_ROWS, 1, LANES), F32)
    flat = jax.ShapeDtypeStruct((4, UNITS, 2, 2, UNIT_ROWS + 2 * MARGIN, 1, LANES), F32)
    buf = pltpu.VMEM((2, RS_ROWS, LANES), F32)
    partner, link, pair, all_devs, slots = DMA((4, 2, CHUNKS)), DMA((3, 2, CHUNKS)), DMA((2,)), DMA((NDEV,)), DMA((PACK_SLOTS,))
    outs = pl.pallas_call(
        reduce_kernel,
        name="reduce_grads",
        out_shape=[jax.ShapeDtypeStruct((SEG, 1, LANES), F32), jax.ShapeDtypeStruct((8, LANES), F32), flat, land_p, land, land, land],
        in_specs=[ANY] * 7 + [VMEM_SPEC] * 3,
        out_specs=[ANY, VMEM_SPEC] + [ANY] * 5,
        scratch_shapes=[buf] * 4 + [pltpu.VMEM((3, 2, CHUNKS, RS_ROWS, LANES), F32), buf, pltpu.VMEM((8, LANES), F32), pltpu.VMEM((NDEV, 8, LANES), F32)]
        + tile_scratch(PACK_SLOTS, PACK_ROWS.values()) + [pltpu.VMEM((PACK_SLOTS, PACK_STAGE, LANES), F32), pltpu.VMEM((TAIL, LANES), F32)]
        + [partner, partner, link, link, DMA((4, 2)), pair, all_devs, all_devs, slots, slots, DMA],
        compiler_params=pltpu.CompilerParams(collective_id=0, has_side_effects=True, vmem_limit_bytes=VMEM_LIMIT),
        cost_estimate=COST,
    )(*grads, *norms)
    return outs[0], outs[1]


def adam_rows(g, m, v, p, norm_row, lr, decay):
    clip = jnp.minimum(1.0, MAX_NORM / (norm_row + CLIP_EPS))
    clipped = clip * g
    new_m = BETA_ONE * m + (1.0 - BETA_ONE) * clipped
    new_v = BETA_TWO * v + (1.0 - BETA_TWO) * clipped * clipped
    adam_dir = (new_m * (1.0 / BIAS_ONE)) / (jnp.sqrt(new_v * (1.0 / BIAS_TWO)) + ADAM_EPS)
    decay_term = jnp.where(decay, WEIGHT_DECAY * p, 0.0)
    return p - lr * (decay_term + adam_dir), new_m, new_v


STATE_ROWS = 2 * PIECE
STATE_COUNT = SEG // STATE_ROWS
STATE_LAST = SEG - STATE_COUNT * STATE_ROWS
STATE_SLOTS = 4
SUB = 160


def decay_rows(me, start, rows):
    return lax.broadcasted_iota(jnp.int32, (rows, LANES), 0) + (SEG * me + start) < MATRIX_ROWS


def gather_kernel(g, m, v, p, norm, lr, full, late, gb, mb, vb, pb, new_p, late_p,
                  load_sem, own_sem, late_sem, own_send, own_recv, fwd_send, fwd_recv, p_send, p_recv):
    me, other, dev_x, dev_y, dev_d = neighbours()
    partner = me + other
    barrier = pltpu.get_barrier_semaphore()
    for dev in (partner, dev_x, dev_y):
        pl.semaphore_signal(barrier, inc=1, device_id=(dev,), device_id_type=MESH)
    to = (dev_x, dev_y, partner)
    sources = (me, dev_x, dev_y, dev_d)

    def is_last(h, i):
        return h == 1 and isinstance(i, int) and i == HALF - 1

    def start_row(h, i):
        return PIECE * (PIECES - 1) if is_last(h, i) else PIECE * (HALF * h + i)

    def size(h, i):
        return PIECE_LAST if is_last(h, i) else PIECE

    def rows_of(dev, h, i):
        return full.at[pl.ds(SEG * dev + start_row(h, i), size(h, i)), 0]

    def loads(h, i):
        return loads_at(h, start_row(h, i), size(h, i))

    def loads_at(h, start, rows):
        start = pl.multiple_of(start, 8)
        copies = [pltpu.make_async_copy(g.at[pl.ds(start, rows), 0], gb.at[h, pl.ds(0, rows)], load_sem.at[0, h])]
        for n, (src, buf) in enumerate(((m, mb), (v, vb), (p, pb))):
            copies.append(pltpu.make_async_copy(src.at[pl.ds(start, rows)], buf.at[h, pl.ds(0, rows)], load_sem.at[n + 1, h]))
        return copies

    def own_copy(n, h, i):
        return pltpu.make_async_remote_copy(
            src_ref=new_p.at[h, i, pl.ds(0, size(h, i))], dst_ref=rows_of(me, h, i),
            send_sem=own_send.at[n, h, i], recv_sem=own_recv.at[n, h, i], device_id=(to[n],), device_id_type=MESH)

    def own_store(h, i):
        return pltpu.make_async_copy(new_p.at[h, i, pl.ds(0, size(h, i))], rows_of(me, h, i), own_sem.at[h, i])

    def forward(h, i):
        src = rows_of((dev_y, dev_x)[h], h, i)
        return pltpu.make_async_remote_copy(
            src_ref=src, dst_ref=src, send_sem=fwd_send.at[h, i], recv_sem=fwd_recv.at[h, i],
            device_id=((dev_x, dev_y)[h],), device_id_type=MESH)

    def arrival(n, h, i):
        src = rows_of((dev_x, dev_y, partner)[n], h, i)
        return pltpu.make_async_remote_copy(
            src_ref=src, dst_ref=src, send_sem=own_send.at[n, h, i], recv_sem=own_recv.at[n, h, i],
            device_id=(to[n],), device_id_type=MESH)

    def forward_arrival(h, i):
        src = rows_of(dev_d, h, i)
        return pltpu.make_async_remote_copy(
            src_ref=src, dst_ref=src, send_sem=fwd_send.at[h, i], recv_sem=fwd_recv.at[h, i],
            device_id=((dev_x, dev_y)[h],), device_id_type=MESH)

    def partner_copy(q, h, i):
        src = rows_of(sources[q], h, i)
        return pltpu.make_async_remote_copy(
            src_ref=src, dst_ref=src, send_sem=p_send.at[q - 1, h, i], recv_sem=p_recv.at[q - 1, h, i],
            device_id=(partner,), device_id_type=MESH)

    def partner_arrival(q, h, i):
        src = rows_of(sources[q] + other, h, i)
        return pltpu.make_async_remote_copy(
            src_ref=src, dst_ref=src, send_sem=p_send.at[q - 1, h, i], recv_sem=p_recv.at[q - 1, h, i],
            device_id=(partner,), device_id_type=MESH)

    def each(body):
        @pl.loop(0, HALF - 1)
        def _(i):
            body(i)

        body(HALF - 1)

    norm_row = norm[0:1, :]
    for h in HALVES:
        for copy in loads(h, 0):
            copy.start()
    pl.semaphore_wait(barrier, 3)

    def compute(h, out, first):
        @pl.loop(0, PIECE // SUB)
        def _(s):
            start = pl.multiple_of(s * SUB, 8)
            sub = pl.ds(start, SUB)
            out[sub] = adam_rows(gb[h, sub], mb[h, sub], vb[h, sub], pb[h, sub], norm_row, lr[0], decay_rows(me, first + start, SUB))[0]

    def update(i):
        for h in HALVES:
            for copy in loads(h, i):
                copy.wait()

            compute(h, new_p.at[h, i], start_row(h, i))
            for n in ((1, 0, 2) if h == 0 else (0, 1, 2)):
                own_copy(n, h, i).start()
            own_store(h, i).start()
            if isinstance(i, int):
                continue
            for last in (False, True):
                @pl.when((i == HALF - 2) == last)
                def _():
                    for copy in loads(h, HALF - 1 if last else i + 1):
                        copy.start()

    each(update)

    def late_store(src, to, n):
        return pltpu.make_async_copy(src, late.at[pl.ds(to, src.shape[0]), 0], late_sem.at[n])

    def late_piece(j):
        return late_store(late_p.at[j], 8 + PIECE * j, j)

    edges = [late_store(new_p.at[1, HALF - 2, pl.ds(PIECE - 8, 8)], 0, LATE_END - LATE_FIRST),
             late_store(new_p.at[1, HALF - 1, pl.ds(0, 8)], LATE_ROWS - 8, LATE_END - LATE_FIRST + 1)]
    for copy in edges:
        copy.start()

    @pl.loop(0, LATE_END - LATE_FIRST)
    def _(j):
        first = PIECE * (LATE_FIRST + j)
        for copy in loads_at(0, first, PIECE):
            copy.start()
        for copy in loads_at(0, first, PIECE):
            copy.wait()
        compute(0, late_p.at[j], first)
        late_piece(j).start()

    def pass_on(i):
        arrival(1, 0, i).wait_recv()
        forward(0, i).start()
        partner_copy(2, 0, i).start()
        arrival(0, 1, i).wait_recv()
        forward(1, i).start()
        partner_copy(1, 1, i).start()
        arrival(0, 0, i).wait_recv()
        partner_copy(1, 0, i).start()
        arrival(1, 1, i).wait_recv()
        partner_copy(2, 1, i).start()

    each(pass_on)

    def pass_last(i):
        for h in HALVES:
            forward_arrival(h, i).wait_recv()
            partner_copy(3, h, i).start()

    each(pass_last)

    def finish(i):
        for h in HALVES:
            own_store(h, i).wait()
            arrival(2, h, i).wait_recv()
            for n in range(3):
                own_copy(n, h, i).wait_send()
            forward(h, i).wait_send()
            for q in range(1, 4):
                partner_copy(q, h, i).wait_send()
                partner_arrival(q, h, i).wait_recv()

    each(finish)
    for copy in edges:
        copy.wait()

    @pl.loop(0, LATE_END - LATE_FIRST)
    def _(j):
        late_piece(j).wait()


def gather_params(g, m, v, p, norm, lr):
    buf = pltpu.VMEM((2, PIECE, LANES), F32)
    pairs = DMA((2, HALF))
    triples = DMA((3, 2, HALF))
    return pl.pallas_call(
        gather_kernel,
        name="gather_params",
        out_shape=[jax.ShapeDtypeStruct((FLAT_ROWS, 1, LANES), F32), jax.ShapeDtypeStruct((LATE_ROWS, 1, LANES), F32)],
        in_specs=[ANY] * 4 + [VMEM_SPEC, SMEM_SPEC],
        out_specs=[ANY, ANY],
        scratch_shapes=[buf, buf, buf, buf, pltpu.VMEM((2, HALF, PIECE, LANES), F32), pltpu.VMEM((LATE_END - LATE_FIRST, PIECE, LANES), F32),
                        DMA((4, 2)), pairs, DMA((LATE_END - LATE_FIRST + 2,)), triples, triples, pairs, pairs, triples, triples],
        compiler_params=pltpu.CompilerParams(collective_id=1, has_side_effects=True, vmem_limit_bytes=VMEM_LIMIT),
        cost_estimate=COST,
    )(g, m, v, p, norm, lr)


def state_kernel(g, m, v, p, norm, lr, new_p, new_m, new_v, gb, mb, vb, pb, pn, mn, vn, in_sem, out_sem):
    me = lax.axis_index("dp")
    norm_row = norm[pl.ds(0, 1), :]

    def window(i):
        rows = STATE_LAST if isinstance(i, int) and i == STATE_COUNT else STATE_ROWS
        slot = lax.rem(i, STATE_SLOTS)
        return slot, pl.ds(pl.multiple_of(i * STATE_ROWS, 8), rows), pl.ds(0, rows)

    def loads(i):
        slot, rows, size = window(i)
        pairs = ((g.at[rows, 0], gb), (m.at[rows], mb), (v.at[rows], vb), (p.at[rows], pb))
        return [pltpu.make_async_copy(src, buf.at[slot, size], in_sem.at[n, slot]) for n, (src, buf) in enumerate(pairs)]

    def stores(i):
        slot, rows, size = window(i)
        pairs = ((pn, new_p), (mn, new_m), (vn, new_v))
        return [pltpu.make_async_copy(buf.at[slot, size], dst.at[rows], out_sem.at[n, slot]) for n, (buf, dst) in enumerate(pairs)]

    def run(copies, wait=False):
        for copy in copies:
            copy.wait() if wait else copy.start()

    def compute(i):
        slot = lax.rem(i, STATE_SLOTS)

        @pl.loop(0, STATE_ROWS // SUB)
        def _(s):
            start = pl.multiple_of(s * SUB, 8)
            rows = pl.ds(start, SUB)
            pn[slot, rows], mn[slot, rows], vn[slot, rows] = adam_rows(
                gb[slot, rows], mb[slot, rows], vb[slot, rows], pb[slot, rows], norm_row, lr[0],
                decay_rows(me, i * STATE_ROWS + start, SUB))

    for i in range(STATE_SLOTS):
        run(loads(i))

    @pl.loop(0, STATE_COUNT)
    def _(i):
        run(loads(i), wait=True)

        @pl.when(i >= STATE_SLOTS)
        def _():
            run(stores(i - STATE_SLOTS), wait=True)

        compute(i)
        run(stores(i))

        @pl.when(i + STATE_SLOTS < STATE_COUNT)
        def _():
            run(loads(i + STATE_SLOTS))

        @pl.when(i + STATE_SLOTS == STATE_COUNT)
        def _():
            run(loads(STATE_COUNT))

    run(loads(STATE_COUNT), wait=True)
    run(stores(STATE_COUNT - STATE_SLOTS), wait=True)
    compute(STATE_COUNT)
    run(stores(STATE_COUNT))
    for n in range(STATE_SLOTS):
        run(stores(STATE_COUNT - STATE_SLOTS + 1 + n), wait=True)


def new_state(g, m, v, p, norm, lr):
    return pl.pallas_call(
        state_kernel,
        name="new_state",
        out_shape=[jax.ShapeDtypeStruct((SEG, LANES), F32)] * 3,
        in_specs=[ANY] * 4 + [VMEM_SPEC, SMEM_SPEC],
        out_specs=[ANY] * 3,
        scratch_shapes=[pltpu.VMEM((STATE_SLOTS, STATE_ROWS, LANES), F32)] * 7 + [DMA((4, STATE_SLOTS)), DMA((3, STATE_SLOTS))],
        compiler_params=pltpu.CompilerParams(vmem_limit_bytes=VMEM_LIMIT),
        cost_estimate=COST,
    )(g, m, v, p, norm, lr)


def solution(mesh):
    def local_step(*arrays):
        grads = [a.reshape(r, w * LANES) for a, r, w in zip(arrays[:7], NAMES_ROWS, WIDTHS)]
        norms = [a.reshape(s) for a, s in zip(arrays[7:10], GAINS)]
        master, exp_avg, exp_avg_sq = [a.reshape(SEG, LANES) for a in arrays[10:13]]
        lr = arrays[13].reshape(1)
        g, norm = reduce_grads(grads, norms)
        full, late = gather_params(g, exp_avg, exp_avg_sq, master, norm, lr)
        late = lax.all_gather(late, "dp", tiled=True)
        state = new_state(g, exp_avg, exp_avg_sq, master, norm, lr)
        params = unpack_late(full, late, unpack_early(full))
        shapes = SHAPES + GAINS[:2] + [(D,)]
        return tuple([a.reshape(-1) for a in state] + [a.reshape(s) for a, s in zip(params, shapes)] + [norm[0, 0]])

    return jax.shard_map(local_step, mesh=mesh, in_specs=(P("dp"),) * 13 + (P(),), out_specs=(P("dp"),) * 3 + (P(),) * 11, check_vma=False)
```

```python
import functools
import math
import jax
import jax.numpy as jnp
from jax import lax
from jax.experimental import pallas as pl
from jax.experimental.pallas import tpu as pltpu
from jax.sharding import PartitionSpec as P

BETA_ONE = 0.9
BETA_TWO = 0.95
ADAM_EPS = 1e-8
WEIGHT_DECAY = 0.1
MAX_NORM = 1.0
CLIP_EPS = 1e-6
STEP = 4
BIAS_ONE = 1.0 - BETA_ONE ** STEP
BIAS_TWO = 1.0 - BETA_TWO ** STEP

MESH = pl.DeviceIdType.MESH
F32 = jnp.float32
BF16 = jnp.bfloat16
LANES = 128

LAYERS, D, KV, FF = 2, 896, 128, 4864
SHAPES = [(LAYERS, D, D), (LAYERS, D, KV), (LAYERS, D, KV), (LAYERS, D, D), (LAYERS, D, FF), (LAYERS, D, FF), (LAYERS, FF, D)]
GAINS = [(LAYERS, D), (LAYERS, D), (1, D)]
TAIL = 40
HALVES, TENSORS, COLUMNS = range(2), range(7), range(7)
NAMES_ROWS = [math.prod(s[:-1]) for s in SHAPES]
WIDTHS = [s[-1] // LANES for s in SHAPES]
OFFSETS = [sum(r * w for r, w in zip(NAMES_ROWS[:t], WIDTHS[:t])) for t in TENSORS]
BLOCK_ROWS = [448, 1792, 1792, 448, 128, 128, 608]
MATRIX_ROWS = 232960
FLAT_ROWS = 233000
SEG = 29125
NDEV = 8

WIDTH_ORDER = (38, 7, 1)
GROUPS = {38: (16,), 7: (16, 32, 64), 1: (16, 128, 256)}
STAGE_ROWS = max(br * WIDTHS[t] for t, br in enumerate(BLOCK_ROWS))

def split(refs, counts):
    refs = list(refs)
    return [[refs.pop(0) for _ in range(n)] for n in counts]


ANY = pl.BlockSpec(memory_space=pl.ANY)
VMEM_SPEC = pl.BlockSpec(memory_space=pltpu.VMEM)
SMEM_SPEC = pl.BlockSpec(memory_space=pltpu.SMEM)
DMA = pltpu.SemaphoreType.DMA
VMEM_LIMIT = 63 * 1024 * 1024
COST = pl.CostEstimate(flops=2 * 10 ** 8, bytes_accessed=10 ** 8, transcendentals=0)


def tile_scratch(slots, rows):
    return [pltpu.VMEM((slots, r, w * LANES), BF16) for r, w in zip(rows, WIDTH_ORDER)]


def width_slot(width):
    return WIDTH_ORDER.index(width)


def row_group(rows, width):
    return max(g for g in GROUPS[width] if rows % g == 0)


PIECE = 480
PIECES = 61
LATE_FIRST, LATE_END = 51, 60
LATE_ROWS = PIECE * (LATE_END - LATE_FIRST) + 16
PIECE_LAST = SEG - (PIECES - 1) * PIECE
HALF = (PIECES - LATE_END + LATE_FIRST) // 2
LATE_HALF = (LATE_ROWS + 16) // 2
LATE_STARTS = (0, LATE_ROWS - LATE_HALF)
LATE_RANGES = [((SEG * s + PIECE * LATE_FIRST) // 8 * 8, -(-(SEG * s + PIECE * LATE_END) // 8) * 8) for s in range(NDEV)]


def unpack_blocks():
    early, late = [], []
    for t in TENSORS:
        w, offset, total = WIDTHS[t], OFFSETS[t], NAMES_ROWS[t]
        cuts = {0, total}
        spans = []
        for low, high in LATE_RANGES:
            first = max(0, (low - offset) // (16 * w) * 16)
            end = min(total, -(-(high - offset) // (16 * w)) * 16)
            if first < end:
                spans.append((first, end))
                cuts |= {first, end}
        cuts = sorted(cuts)
        for begin, end in zip(cuts[:-1], cuts[1:]):
            is_late = any(first <= begin and end <= last for first, last in spans)
            count = -(-(end - begin) // BLOCK_ROWS[t])
            step = -(-(end - begin) // (16 * count)) * 16
            for row in range(begin, end, step):
                rows = min(step, end - row)
                low, high = offset + row * w, offset + (row + rows) * w
                middles = [l + LATE_STARTS[1] for l, _ in LATE_RANGES]
                edges = sorted({low, high} | {e for r in LATE_RANGES + [middles] for e in r if low < e < high})
                sources = []
                for e0, e1 in zip(edges[:-1], edges[1:]):
                    seg = [s for s, (l, h) in enumerate(LATE_RANGES) if l <= e0 and e1 <= h]
                    source = None
                    start = e0
                    if seg:
                        start = e0 - SEG * seg[0] - PIECE * LATE_FIRST + 8
                        half = int(e0 >= middles[seg[0]])
                        source, start = (seg[0], half), start - LATE_STARTS[half]
                    sources.append((source, start, e0 - low, e1 - e0))
                (late if is_late else early).append((t, row, rows, sources))
    return early, late


EARLY_BLOCKS, LATE_BLOCKS = unpack_blocks()
LATE_TENSORS = sorted({t for t, _, _, _ in LATE_BLOCKS})
SLOTS = 4


def unpack_body(blocks, flat, lates, outs, tiles, stage, in_sem, out_sem):
    def loads(b, start=True):
        for n, (source, row, to, rows) in enumerate(blocks[b][3]):
            def copy(ref):
                return pltpu.make_async_copy(ref.at[pl.ds(row, rows), 0], stage.at[b % SLOTS, pl.ds(to, rows)], in_sem.at[b % SLOTS, n])

            if not start:
                copy(flat).wait()
            elif source is None:
                copy(flat).start()
            else:
                for relation in range(NDEV):
                    @pl.when(lax.bitwise_xor(lax.axis_index("dp"), source[0]) == relation)
                    def _():
                        copy(lates[relation][source[1]]).start()

    def store(b):
        t, row, rows, _ = blocks[b]
        return pltpu.make_async_copy(tiles[width_slot(WIDTHS[t])].at[b % SLOTS, pl.ds(0, rows)], outs[t].at[pl.ds(row, rows)], out_sem.at[b % SLOTS])

    for b in range(min(SLOTS, len(blocks))):
        loads(b)
    yield
    for b, (t, row, rows, _) in enumerate(blocks):
        w = WIDTHS[t]
        tile = tiles[width_slot(w)]
        group = row_group(rows, w)
        loads(b, start=False)
        if b >= SLOTS:
            store(b - SLOTS).wait()

        @pl.loop(0, rows // group)
        def _(i):
            for j in range(w):
                if w == 1:
                    block = stage[b % SLOTS, pl.ds(pl.multiple_of(i * group, 16), group), :]
                else:
                    block = stage[b % SLOTS, pl.ds(i * (group * w) + j, group, stride=w), :]
                tile[b % SLOTS, pl.ds(pl.multiple_of(i * group, 16), group), pl.ds(j * LANES, LANES)] = block.astype(BF16)

        store(b).start()
        if b + SLOTS < len(blocks):
            loads(b + SLOTS)
    for b in range(max(0, len(blocks) - SLOTS), len(blocks)):
        store(b).wait()


UNPACK_SCRATCH = tile_scratch(SLOTS, (128, 608, 1792)) + [pltpu.VMEM((SLOTS, STAGE_ROWS, LANES), F32)]
TENSOR_TYPES = [jax.ShapeDtypeStruct((r, w * LANES), BF16) for r, w in zip(NAMES_ROWS, WIDTHS)]


def unpack_early_kernel(tensors, flat, *refs):
    gains = len(refs) - len(tensors) - 8
    outs, norms, tiles, (stage, tail, in_sem, out_sem, tail_sem) = split(refs, (len(tensors), gains, 3, 5))
    tail_copy = pltpu.make_async_copy(flat.at[pl.ds(MATRIX_ROWS, TAIL), 0], tail, tail_sem)
    tail_copy.start()
    work = unpack_body([b for b in EARLY_BLOCKS if b[0] in tensors], flat, None, dict(zip(tensors, outs)), tiles, stage, in_sem, out_sem)
    next(work)
    tail_copy.wait()
    base = 0
    for n in norms:
        for j in COLUMNS:
            lines = [tail[pl.ds(base + j + 7 * layer, 1), :] for layer in range(n.shape[0])]
            n[:, pl.ds(j * LANES, LANES)] = jnp.concatenate(lines, axis=0).astype(BF16)
        base += 7 * n.shape[0]
    for _ in work:
        pass


def unpack_early(flat, tensors, gains):
    return pl.pallas_call(
        functools.partial(unpack_early_kernel, tensors),
        name="unpack_early",
        out_shape=[TENSOR_TYPES[t] for t in tensors] + [jax.ShapeDtypeStruct(s, BF16) for s in gains],
        in_specs=[ANY],
        out_specs=[ANY] * len(tensors) + [VMEM_SPEC] * len(gains),
        scratch_shapes=UNPACK_SCRATCH + [pltpu.VMEM((TAIL, LANES), F32), DMA((SLOTS, 4)), DMA((SLOTS,)), DMA],
        compiler_params=pltpu.CompilerParams(vmem_limit_bytes=VMEM_LIMIT),
        cost_estimate=COST,
    )(flat)


def unpack_late_kernel(flat, *refs):
    count = len(LATE_TENSORS)
    lates, _, outs, tiles, (stage, in_sem, out_sem) = split(refs, (2 * NDEV, count, count, 3, 3))
    for _ in unpack_body(LATE_BLOCKS, flat, list(zip(lates[::2], lates[1::2])), dict(zip(LATE_TENSORS, outs)), tiles, stage, in_sem, out_sem):
        pass


def unpack_late(flat, lates, params):
    count = len(LATE_TENSORS)
    lates = [a for pair in lates for a in pair]
    outs = pl.pallas_call(
        unpack_late_kernel,
        name="unpack_late",
        out_shape=[TENSOR_TYPES[t] for t in LATE_TENSORS],
        in_specs=[ANY] * (1 + len(lates) + count),
        out_specs=[ANY] * count,
        input_output_aliases={1 + len(lates) + n: n for n in range(count)},
        scratch_shapes=UNPACK_SCRATCH + [DMA((SLOTS, 4)), DMA((SLOTS,))],
        compiler_params=pltpu.CompilerParams(vmem_limit_bytes=VMEM_LIMIT),
        cost_estimate=COST,
    )(flat, *lates, *[params[t] for t in LATE_TENSORS])
    return {**params, **dict(zip(LATE_TENSORS, outs))}


def neighbours():
    me = lax.axis_index("dp")
    core, x, y = lax.rem(me, 2), lax.rem(me // 2, 2), me // 4
    other = 1 - 2 * core
    step_x, step_y = 2 - 4 * x, 4 - 8 * y
    return me, other, me + step_x, me + step_y, me + step_x + step_y


CHUNKS = 16
RS_ROWS = 911
RS_HALF_START = SEG - CHUNKS * RS_ROWS
UNITS = CHUNKS // 4
KIND_D, KIND_N, KIND_S, KIND_O = range(4)
CHIP_D, CHIP_X, CHIP_Y, CHIP_OWN = range(4)
UNIT_ROWS = 4 * RS_ROWS
MARGIN = 16 * 38
PACK_ROWS = {38: 112, 7: 608, 1: 896}
PACK_STAGE = 112 * 38
PACK_SLOTS = 3


def pack_blocks(chip, unit):
    blocks = []
    for parity in HALVES:
        for h in HALVES:
            begin = SEG * (2 * chip + parity) + RS_HALF_START * h + UNIT_ROWS * unit
            for t in TENSORS:
                w, offset, total = WIDTHS[t], OFFSETS[t], NAMES_ROWS[t]
                low, high = max(begin, offset), min(begin + UNIT_ROWS, offset + total * w)
                if low >= high:
                    continue
                first = (low - offset) // (16 * w) * 16
                end = -(-(high - offset) // (16 * w)) * 16
                step = -(-(end - first) // (16 * -(-(end - first) // PACK_ROWS[w]))) * 16
                for row in range(first, end, step):
                    blocks.append((t, row, min(step, end - row), parity, h, offset + row * w - begin + MARGIN))
    return blocks


def reduce_kernel(*refs):
    (grads, norms, (g_out, norm_out, flat, land_p, land_d, land_n, land_s),
     (mine, part, first, second, sums, g_buf, ss, ss_all), tiles, (stage, tail),
     (p_send, p_recv, i_send, i_recv, load_sem, g_sem, ss_send, ss_recv, in_sem, out_sem, tail_sem)) = split(refs, (7, 3, 7, 8, 3, 2, 11))
    me, other, dev_x, dev_y, dev_d = neighbours()
    core, x, y = lax.rem(me, 2), lax.rem(me // 2, 2), me // 4
    barrier = pltpu.get_barrier_semaphore()
    for d in range(1, NDEV):
        pl.semaphore_signal(barrier, inc=1, device_id=(lax.rem(me + d, NDEV),), device_id_type=MESH)

    tail[...] = jnp.zeros_like(tail)
    line = 0
    for n in norms:
        for layer in range(n.shape[0]):
            for j in COLUMNS:
                tail[pl.ds(line, 1), :] = n[pl.ds(layer, 1), pl.ds(j * LANES, LANES)].astype(F32)
                line += 1

    def pack(place, chip, unit):
        blocks = pack_blocks(chip, unit)

        def load(b):
            t, row, rows = blocks[b][:3]
            return pltpu.make_async_copy(grads[t].at[pl.ds(row, rows)], tiles[width_slot(WIDTHS[t])].at[b % PACK_SLOTS, pl.ds(0, rows)], in_sem.at[b % PACK_SLOTS])

        def store(b):
            t, _, rows, parity, h, to = blocks[b]
            size = rows * WIDTHS[t]
            return pltpu.make_async_copy(stage.at[b % PACK_SLOTS, pl.ds(0, size)], flat.at[place, unit, parity, h, pl.ds(to, size), 0], out_sem.at[b % PACK_SLOTS])

        for b in range(PACK_SLOTS):
            load(b).start()
        tail_copies = [pltpu.make_async_copy(tail, flat.at[place, unit, 1, 1, pl.ds(MARGIN + UNIT_ROWS - TAIL, TAIL), 0], tail_sem)
                       for _ in range(chip * unit // (3 * UNITS - 3))]
        for copy in tail_copies:
            copy.start()
        for b, block in enumerate(blocks):
            t, rows = block[0], block[2]
            w = WIDTHS[t]
            tile = tiles[width_slot(w)]
            group = row_group(rows, w)
            load(b).wait()
            if b >= PACK_SLOTS:
                store(b - PACK_SLOTS).wait()

            @pl.loop(0, rows // group)
            def _(i):
                for j in range(w):
                    values = tile[b % PACK_SLOTS, pl.ds(pl.multiple_of(i * group, 16), group), pl.ds(j * LANES, LANES)].astype(F32)
                    if w == 1:
                        stage[b % PACK_SLOTS, pl.ds(pl.multiple_of(i * group, 16), group), :] = values
                    else:
                        stage[b % PACK_SLOTS, pl.ds(i * (group * w) + j, group, stride=w), :] = values

            store(b).start()
            if b + PACK_SLOTS < len(blocks):
                load(b + PACK_SLOTS).start()
        for b in range(len(blocks) - PACK_SLOTS, len(blocks)):
            store(b).wait()
        for copy in tail_copies:
            copy.wait()

    def place_of(kind, h):
        return ((CHIP_D, CHIP_D), (CHIP_X, CHIP_Y), (CHIP_Y, CHIP_X), (CHIP_OWN, CHIP_OWN))[kind][h]

    def chunk(kind, h, i, parity):
        return flat.at[place_of(kind, h), i // 4, parity, h, pl.ds(MARGIN + RS_ROWS * lax.rem(i, 4), RS_ROWS)]

    def start_row(h, i):
        return RS_HALF_START * h + RS_ROWS * i

    def partner_copy(kind, h, i):
        return pltpu.make_async_remote_copy(
            src_ref=chunk(kind, h, i, 1 - core), dst_ref=land_p.at[kind, h, i],
            send_sem=p_send.at[kind, h, i], recv_sem=p_recv.at[kind, h, i],
            device_id=(me + other,), device_id_type=MESH)

    def link_copy(kind, h, i):
        land = (land_d, land_n, land_s)[kind]
        to = ((dev_x, dev_y), (dev_x, dev_y), (dev_y, dev_x))[kind][h]
        return pltpu.make_async_remote_copy(
            src_ref=sums.at[kind, h, i], dst_ref=land.at[h, i, pl.ds(0, RS_ROWS), 0],
            send_sem=i_send.at[kind, h, i], recv_sem=i_recv.at[kind, h, i],
            device_id=(to,), device_id_type=MESH)

    def load_mine(kind, h, i):
        return pltpu.make_async_copy(chunk(kind, h, i, core).at[:, 0], mine.at[h], load_sem.at[0, h])

    def load_part(kind, h, i):
        return pltpu.make_async_copy(land_p.at[kind, h, i, pl.ds(0, RS_ROWS), 0], part.at[h], load_sem.at[1, h])

    def load_link(land, buf, n, h, i):
        return pltpu.make_async_copy(land.at[h, i, pl.ds(0, RS_ROWS), 0], buf.at[h], load_sem.at[n, h])

    def store_g(h, i):
        return pltpu.make_async_copy(g_buf.at[h], g_out.at[pl.ds(start_row(h, i), RS_ROWS), 0], g_sem.at[h])

    def exchange(kinds, begin, end):
        @pl.loop(begin, end)
        def _(i):
            for kind in kinds:
                for h in HALVES:
                    partner_copy(kind, h, i).start()

    def send(kind, begin, end):
        @pl.loop(begin, end)
        def _(i):
            for h in HALVES:
                load_mine(kind, h, i).start()
            for h in HALVES:
                partner_copy(kind, h, i).wait_recv()
                load_part(kind, h, i).start()
                if kind == KIND_S:
                    link_copy(KIND_D, h, i).wait_recv()
                    load_link(land_d, first, 2, h, i).start()
            for h in HALVES:
                load_mine(kind, h, i).wait()
                load_part(kind, h, i).wait()
                total = mine[h] + part[h]
                if kind == KIND_S:
                    load_link(land_d, first, 2, h, i).wait()
                    total = total + first[h]
                sums[kind, h, i] = total
                link_copy(kind, h, i).start()

    @pl.loop(0, 4 * UNITS)
    def _(n):
        place, unit = n // UNITS, lax.rem(n, UNITS)
        flip_x, flip_y = 1 - place // 2, 1 - lax.rem(place, 2)
        chip = (x + flip_x * (1 - 2 * x)) + 2 * (y + flip_y * (1 - 2 * y))
        for case in range(4 * UNITS):
            @pl.when(UNITS * chip + unit == case)
            def _():
                pack(place, case // UNITS, case % UNITS)

        @pl.when(n == 0)
        def _():
            pl.semaphore_wait(barrier, NDEV - 1)

        @pl.when(n < UNITS)
        def _():
            exchange((KIND_D,), 4 * unit, 4 * unit + 4)
            send(KIND_D, 4 * unit, 4 * unit + 4)

        @pl.when(n == 3 * UNITS - 1)
        def _():
            exchange((KIND_N, KIND_S), 0, CHUNKS)
            send(KIND_N, 0, CHUNKS)

    exchange((KIND_O,), 0, CHUNKS)
    send(KIND_S, 0, CHUNKS)

    def last(i, acc):
        for h in HALVES:
            load_mine(KIND_O, h, i).start()
            partner_copy(KIND_O, h, i).wait_recv()
            load_part(KIND_O, h, i).start()
        for h in HALVES:
            link_copy(KIND_N, h, i).wait_recv()
            load_link(land_n, first, 2, h, i).start()
        for h in HALVES:
            link_copy(KIND_S, h, i).wait_recv()
            load_link(land_s, second, 3, h, i).start()
            load_mine(KIND_O, h, i).wait()
            load_part(KIND_O, h, i).wait()
            load_link(land_n, first, 2, h, i).wait()
            load_link(land_s, second, 3, h, i).wait()

            @pl.when(i > 0)
            def _():
                store_g(h, i - 1).wait()

            g = ((mine[h] + part[h]) + (first[h] + second[h])) * (1.0 / NDEV)
            g_buf[h] = g
            store_g(h, i).start()
            square = g * g
            if h == 1:
                row = lax.broadcasted_iota(jnp.int32, (RS_ROWS, LANES), 0) + RS_ROWS * i
                square = jnp.where(row >= CHUNKS * RS_ROWS - RS_HALF_START, square, 0.0)
            acc = acc + jnp.sum(square, axis=0, keepdims=True)
        return acc

    acc = lax.fori_loop(0, CHUNKS, last, jnp.zeros((1, LANES), F32))
    ss[...] = jnp.broadcast_to(acc, (8, LANES))

    @pl.loop(0, CHUNKS)
    def _(i):
        for h in HALVES:
            for kind in range(4):
                partner_copy(kind, h, i).wait_send()
            for kind in range(3):
                link_copy(kind, h, i).wait_send()

    def norm_copy(d):
        return pltpu.make_async_remote_copy(
            src_ref=ss, dst_ref=ss_all.at[d], send_sem=ss_send.at[d], recv_sem=ss_recv.at[d],
            device_id=(lax.rem(me + d, NDEV),), device_id_type=MESH)

    for d in range(1, NDEV):
        norm_copy(d).start()
    for h in HALVES:
        store_g(h, CHUNKS - 1).wait()
    ss_all[0] = ss[...]
    for d in range(1, NDEV):
        norm_copy(d).wait()
    total = jnp.zeros((8, LANES), F32)
    for dev in range(NDEV):
        total = total + ss_all[lax.rem(me - dev + NDEV, NDEV)]
    norm_out[...] = jnp.broadcast_to(jnp.sqrt(jnp.sum(total, axis=1, keepdims=True)), (8, LANES))


def reduce_grads(grads, norms):
    land = jax.ShapeDtypeStruct((2, CHUNKS, RS_ROWS, 1, LANES), F32)
    land_p = jax.ShapeDtypeStruct((4, 2, CHUNKS, RS_ROWS, 1, LANES), F32)
    flat = jax.ShapeDtypeStruct((4, UNITS, 2, 2, UNIT_ROWS + 2 * MARGIN, 1, LANES), F32)
    buf = pltpu.VMEM((2, RS_ROWS, LANES), F32)
    partner, link, pair, all_devs, slots = DMA((4, 2, CHUNKS)), DMA((3, 2, CHUNKS)), DMA((2,)), DMA((NDEV,)), DMA((PACK_SLOTS,))
    outs = pl.pallas_call(
        reduce_kernel,
        name="reduce_grads",
        out_shape=[jax.ShapeDtypeStruct((SEG, 1, LANES), F32), jax.ShapeDtypeStruct((8, LANES), F32), flat, land_p, land, land, land],
        in_specs=[ANY] * 7 + [VMEM_SPEC] * 3,
        out_specs=[ANY, VMEM_SPEC] + [ANY] * 5,
        scratch_shapes=[buf] * 4 + [pltpu.VMEM((3, 2, CHUNKS, RS_ROWS, LANES), F32), buf, pltpu.VMEM((8, LANES), F32), pltpu.VMEM((NDEV, 8, LANES), F32)]
        + tile_scratch(PACK_SLOTS, PACK_ROWS.values()) + [pltpu.VMEM((PACK_SLOTS, PACK_STAGE, LANES), F32), pltpu.VMEM((TAIL, LANES), F32)]
        + [partner, partner, link, link, DMA((4, 2)), pair, all_devs, all_devs, slots, slots, DMA],
        compiler_params=pltpu.CompilerParams(collective_id=0, has_side_effects=True, vmem_limit_bytes=VMEM_LIMIT),
        cost_estimate=COST,
    )(*grads, *norms)
    return outs[0], outs[1]


def adam_rows(g, m, v, p, norm_row, lr, decay):
    clip = jnp.minimum(1.0, MAX_NORM / (norm_row + CLIP_EPS))
    clipped = clip * g
    new_m = BETA_ONE * m + (1.0 - BETA_ONE) * clipped
    new_v = BETA_TWO * v + (1.0 - BETA_TWO) * clipped * clipped
    adam_dir = (new_m * (1.0 / BIAS_ONE)) / (jnp.sqrt(new_v * (1.0 / BIAS_TWO)) + ADAM_EPS)
    decay_term = jnp.where(decay, WEIGHT_DECAY * p, 0.0)
    return p - lr * (decay_term + adam_dir), new_m, new_v


STATE_ROWS = 2 * PIECE
STATE_COUNT = SEG // STATE_ROWS
STATE_LAST = SEG - STATE_COUNT * STATE_ROWS
STATE_SLOTS = 4
SUB = 160


def decay_rows(me, start, rows):
    return lax.broadcasted_iota(jnp.int32, (rows, LANES), 0) + (SEG * me + start) < MATRIX_ROWS


def gather_kernel(g, m, v, p, norm, lr, full, late_a, late_b, gb, mb, vb, pb, new_p, late_p,
                  load_sem, own_sem, late_sem, own_send, own_recv, fwd_send, fwd_recv, p_send, p_recv):
    me, other, dev_x, dev_y, dev_d = neighbours()
    partner = me + other
    barrier = pltpu.get_barrier_semaphore()
    for dev in (partner, dev_x, dev_y):
        pl.semaphore_signal(barrier, inc=1, device_id=(dev,), device_id_type=MESH)
    to = (dev_x, dev_y, partner)
    sources = (me, dev_x, dev_y, dev_d)

    def is_last(h, i):
        return h == 1 and isinstance(i, int) and i == HALF - 1

    def start_row(h, i):
        return PIECE * (PIECES - 1) if is_last(h, i) else PIECE * (HALF * h + i)

    def size(h, i):
        return PIECE_LAST if is_last(h, i) else PIECE

    def rows_of(dev, h, i):
        return full.at[pl.ds(SEG * dev + start_row(h, i), size(h, i)), 0]

    def loads(h, i):
        return loads_at(h, start_row(h, i), size(h, i))

    def loads_at(h, start, rows):
        start = pl.multiple_of(start, 8)
        copies = [pltpu.make_async_copy(g.at[pl.ds(start, rows), 0], gb.at[h, pl.ds(0, rows)], load_sem.at[0, h])]
        for n, (src, buf) in enumerate(((m, mb), (v, vb), (p, pb))):
            copies.append(pltpu.make_async_copy(src.at[pl.ds(start, rows)], buf.at[h, pl.ds(0, rows)], load_sem.at[n + 1, h]))
        return copies

    def own_copy(n, h, i):
        return pltpu.make_async_remote_copy(
            src_ref=new_p.at[h, i, pl.ds(0, size(h, i))], dst_ref=rows_of(me, h, i),
            send_sem=own_send.at[n, h, i], recv_sem=own_recv.at[n, h, i], device_id=(to[n],), device_id_type=MESH)

    def own_store(h, i):
        return pltpu.make_async_copy(new_p.at[h, i, pl.ds(0, size(h, i))], rows_of(me, h, i), own_sem.at[h, i])

    def forward(h, i):
        src = rows_of((dev_y, dev_x)[h], h, i)
        return pltpu.make_async_remote_copy(
            src_ref=src, dst_ref=src, send_sem=fwd_send.at[h, i], recv_sem=fwd_recv.at[h, i],
            device_id=((dev_x, dev_y)[h],), device_id_type=MESH)

    def arrival(n, h, i):
        src = rows_of((dev_x, dev_y, partner)[n], h, i)
        return pltpu.make_async_remote_copy(
            src_ref=src, dst_ref=src, send_sem=own_send.at[n, h, i], recv_sem=own_recv.at[n, h, i],
            device_id=(to[n],), device_id_type=MESH)

    def forward_arrival(h, i):
        src = rows_of(dev_d, h, i)
        return pltpu.make_async_remote_copy(
            src_ref=src, dst_ref=src, send_sem=fwd_send.at[h, i], recv_sem=fwd_recv.at[h, i],
            device_id=((dev_x, dev_y)[h],), device_id_type=MESH)

    def partner_copy(q, h, i):
        src = rows_of(sources[q], h, i)
        return pltpu.make_async_remote_copy(
            src_ref=src, dst_ref=src, send_sem=p_send.at[q - 1, h, i], recv_sem=p_recv.at[q - 1, h, i],
            device_id=(partner,), device_id_type=MESH)

    def partner_arrival(q, h, i):
        src = rows_of(sources[q] + other, h, i)
        return pltpu.make_async_remote_copy(
            src_ref=src, dst_ref=src, send_sem=p_send.at[q - 1, h, i], recv_sem=p_recv.at[q - 1, h, i],
            device_id=(partner,), device_id_type=MESH)

    def each(body):
        @pl.loop(0, HALF - 1)
        def _(i):
            body(i)

        body(HALF - 1)

    norm_row = norm[0:1, :]
    for h in HALVES:
        for copy in loads(h, 0):
            copy.start()
    pl.semaphore_wait(barrier, 3)

    def compute(h, out, first):
        @pl.loop(0, PIECE // SUB)
        def _(s):
            start = pl.multiple_of(s * SUB, 8)
            sub = pl.ds(start, SUB)
            out[sub] = adam_rows(gb[h, sub], mb[h, sub], vb[h, sub], pb[h, sub], norm_row, lr[0], decay_rows(me, first + start, SUB))[0]

    def update(i):
        for h in HALVES:
            for copy in loads(h, i):
                copy.wait()

            compute(h, new_p.at[h, i], start_row(h, i))
            for n in ((1, 0, 2) if h == 0 else (0, 1, 2)):
                own_copy(n, h, i).start()
            own_store(h, i).start()
            if isinstance(i, int):
                continue
            for last in (False, True):
                @pl.when((i == HALF - 2) == last)
                def _():
                    for copy in loads(h, HALF - 1 if last else i + 1):
                        copy.start()

    each(update)

    late_copies = []

    def late_store(src, row, rows, to):
        for out, start in zip((late_a, late_b), LATE_STARTS):
            low, high = max(to, start), min(to + rows, start + LATE_HALF)
            if low < high:
                late_copies.append(pltpu.make_async_copy(src.at[pl.ds(row + low - to, high - low)], out.at[pl.ds(low - start, high - low), 0], late_sem.at[len(late_copies)]))
                late_copies[-1].start()

    late_store(new_p.at[1, HALF - 2], PIECE - 8, 8, 0)
    late_store(new_p.at[1, HALF - 1], 0, 8, LATE_ROWS - 8)
    for j in range(LATE_END - LATE_FIRST):
        first = PIECE * (LATE_FIRST + j)
        for copy in loads_at(j % 2, first, PIECE):
            copy.start()
        for copy in loads_at(j % 2, first, PIECE):
            copy.wait()
        compute(j % 2, late_p.at[j], first)
        late_store(late_p.at[j], 0, PIECE, 8 + PIECE * j)

    def pass_on(i):
        arrival(1, 0, i).wait_recv()
        forward(0, i).start()
        partner_copy(2, 0, i).start()
        arrival(0, 1, i).wait_recv()
        forward(1, i).start()
        partner_copy(1, 1, i).start()
        arrival(0, 0, i).wait_recv()
        partner_copy(1, 0, i).start()
        arrival(1, 1, i).wait_recv()
        partner_copy(2, 1, i).start()

    each(pass_on)

    def pass_last(i):
        for h in HALVES:
            forward_arrival(h, i).wait_recv()
            partner_copy(3, h, i).start()

    each(pass_last)

    def finish(i):
        for h in HALVES:
            own_store(h, i).wait()
            arrival(2, h, i).wait_recv()
            for n in range(3):
                own_copy(n, h, i).wait_send()
            forward(h, i).wait_send()
            for q in range(1, 4):
                partner_copy(q, h, i).wait_send()
                partner_arrival(q, h, i).wait_recv()

    each(finish)
    for copy in late_copies:
        copy.wait()


def gather_params(g, m, v, p, norm, lr):
    buf = pltpu.VMEM((2, PIECE, LANES), F32)
    pairs = DMA((2, HALF))
    triples = DMA((3, 2, HALF))
    return pl.pallas_call(
        gather_kernel,
        name="gather_params",
        out_shape=[jax.ShapeDtypeStruct((FLAT_ROWS, 1, LANES), F32), jax.ShapeDtypeStruct((LATE_HALF, 1, LANES), F32), jax.ShapeDtypeStruct((LATE_HALF, 1, LANES), F32)],
        in_specs=[ANY] * 4 + [VMEM_SPEC, SMEM_SPEC],
        out_specs=[ANY] * 3,
        scratch_shapes=[buf, buf, buf, buf, pltpu.VMEM((2, HALF, PIECE, LANES), F32), pltpu.VMEM((LATE_END - LATE_FIRST, PIECE, LANES), F32),
                        DMA((4, 2)), pairs, DMA((LATE_END - LATE_FIRST + 3,)), triples, triples, pairs, pairs, triples, triples],
        compiler_params=pltpu.CompilerParams(collective_id=1, has_side_effects=True, vmem_limit_bytes=VMEM_LIMIT),
        cost_estimate=COST,
    )(g, m, v, p, norm, lr)


def state_kernel(g, m, v, p, norm, lr, new_p, new_m, new_v, gb, mb, vb, pb, pn, mn, vn, in_sem, out_sem):
    me = lax.axis_index("dp")
    norm_row = norm[pl.ds(0, 1), :]

    def window(i):
        rows = STATE_LAST if isinstance(i, int) and i == STATE_COUNT else STATE_ROWS
        slot = lax.rem(i, STATE_SLOTS)
        return slot, pl.ds(pl.multiple_of(i * STATE_ROWS, 8), rows), pl.ds(0, rows)

    def loads(i):
        slot, rows, size = window(i)
        pairs = ((g.at[rows, 0], gb), (m.at[rows], mb), (v.at[rows], vb), (p.at[rows], pb))
        return [pltpu.make_async_copy(src, buf.at[slot, size], in_sem.at[n, slot]) for n, (src, buf) in enumerate(pairs)]

    def stores(i):
        slot, rows, size = window(i)
        pairs = ((pn, new_p), (mn, new_m), (vn, new_v))
        return [pltpu.make_async_copy(buf.at[slot, size], dst.at[rows], out_sem.at[n, slot]) for n, (buf, dst) in enumerate(pairs)]

    def run(copies, wait=False):
        for copy in copies:
            copy.wait() if wait else copy.start()

    def compute(i):
        slot = lax.rem(i, STATE_SLOTS)

        @pl.loop(0, STATE_ROWS // SUB)
        def _(s):
            start = pl.multiple_of(s * SUB, 8)
            rows = pl.ds(start, SUB)
            pn[slot, rows], mn[slot, rows], vn[slot, rows] = adam_rows(
                gb[slot, rows], mb[slot, rows], vb[slot, rows], pb[slot, rows], norm_row, lr[0],
                decay_rows(me, i * STATE_ROWS + start, SUB))

    for i in range(STATE_SLOTS):
        run(loads(i))

    @pl.loop(0, STATE_COUNT)
    def _(i):
        run(loads(i), wait=True)

        @pl.when(i >= STATE_SLOTS)
        def _():
            run(stores(i - STATE_SLOTS), wait=True)

        compute(i)
        run(stores(i))

        @pl.when(i + STATE_SLOTS < STATE_COUNT)
        def _():
            run(loads(i + STATE_SLOTS))

        @pl.when(i + STATE_SLOTS == STATE_COUNT)
        def _():
            run(loads(STATE_COUNT))

    run(loads(STATE_COUNT), wait=True)
    run(stores(STATE_COUNT - STATE_SLOTS), wait=True)
    compute(STATE_COUNT)
    run(stores(STATE_COUNT))
    for n in range(STATE_SLOTS):
        run(stores(STATE_COUNT - STATE_SLOTS + 1 + n), wait=True)


def new_state(g, m, v, p, norm, lr):
    return pl.pallas_call(
        state_kernel,
        name="new_state",
        out_shape=[jax.ShapeDtypeStruct((SEG, LANES), F32)] * 3,
        in_specs=[ANY] * 4 + [VMEM_SPEC, SMEM_SPEC],
        out_specs=[ANY] * 3,
        scratch_shapes=[pltpu.VMEM((STATE_SLOTS, STATE_ROWS, LANES), F32)] * 7 + [DMA((4, STATE_SLOTS)), DMA((3, STATE_SLOTS))],
        compiler_params=pltpu.CompilerParams(vmem_limit_bytes=VMEM_LIMIT),
        cost_estimate=COST,
    )(g, m, v, p, norm, lr)


def solution(mesh):
    def local_step(*arrays):
        grads = [a.reshape(r, w * LANES) for a, r, w in zip(arrays[:7], NAMES_ROWS, WIDTHS)]
        norms = [a.reshape(s) for a, s in zip(arrays[7:10], GAINS)]
        master, exp_avg, exp_avg_sq = [a.reshape(SEG, LANES) for a in arrays[10:13]]
        lr = arrays[13].reshape(1)
        g, norm = reduce_grads(grads, norms)
        full, *late = gather_params(g, exp_avg, exp_avg_sq, master, norm, lr)

        def permute(a, bits):
            return lax.ppermute(a, "dp", [(d, d ^ bits) for d in range(NDEV)])

        own = [permute(a, 1) for a in late]
        by_y, by_x = permute(late[0], 4), permute(late[1], 2)
        far_x, far_y = permute(late[0], 2), permute(late[1], 4)
        second = (0, 1, 2, 3, 6)
        rest = list(unpack_early(full, second, GAINS))
        by_y, by_x, full, g, rest[-1] = lax.optimization_barrier((by_y, by_x, full, g, rest[-1]))
        across = (permute(by_y, 2), permute(by_x, 4))
        from_y, from_x = permute(by_y, 1), permute(by_x, 1)
        state = list(new_state(g, exp_avg, exp_avg_sq, master, norm, lr))
        far_x, far_y, full, state[0] = lax.optimization_barrier((far_x, far_y, full, state[0]))
        far = permute(far_x, 1), permute(far_y, 1)
        gate, = unpack_early(full, (4,), [])
        *across, full, gate = lax.optimization_barrier((*across, full, gate))
        from_across = [permute(a, 1) for a in across]
        up, = unpack_early(full, (5,), [])
        params = {**dict(zip(second, rest)), 4: gate, 5: up}
        lates = [late, own, (far_x, by_x), (far[0], from_x), (by_y, far_y), (from_y, far[1]), across, from_across]
        params = unpack_late(full, lates, params)
        params = [params[t] for t in TENSORS] + rest[len(second):]
        shapes = SHAPES + GAINS[:2] + [(D,)]
        return tuple([a.reshape(-1) for a in state] + [a.reshape(s) for a, s in zip(params, shapes)] + [norm[0, 0]])

    return jax.shard_map(local_step, mesh=mesh, in_specs=(P("dp"),) * 13 + (P(),), out_specs=(P("dp"),) * 3 + (P(),) * 11, check_vma=False)
```

```python
import functools
import math
import jax
import jax.numpy as jnp
from jax import lax
from jax.experimental import pallas as pl
from jax.experimental.pallas import tpu as pltpu
from jax.sharding import PartitionSpec as P

BETA_ONE = 0.9
BETA_TWO = 0.95
ADAM_EPS = 1e-8
WEIGHT_DECAY = 0.1
MAX_NORM = 1.0
CLIP_EPS = 1e-6
STEP = 4
BIAS_ONE = 1.0 - BETA_ONE ** STEP
BIAS_TWO = 1.0 - BETA_TWO ** STEP

MESH = pl.DeviceIdType.MESH
F32 = jnp.float32
BF16 = jnp.bfloat16
LANES = 128

LAYERS, D, KV, FF = 2, 896, 128, 4864
SHAPES = [(LAYERS, D, D), (LAYERS, D, KV), (LAYERS, D, KV), (LAYERS, D, D), (LAYERS, D, FF), (LAYERS, D, FF), (LAYERS, FF, D)]
GAINS = [(LAYERS, D), (LAYERS, D), (1, D)]
TAIL = 40
HALVES, TENSORS, COLUMNS = range(2), range(7), range(7)
NAMES_ROWS = [math.prod(s[:-1]) for s in SHAPES]
WIDTHS = [s[-1] // LANES for s in SHAPES]
OFFSETS = [sum(r * w for r, w in zip(NAMES_ROWS[:t], WIDTHS[:t])) for t in TENSORS]
BLOCK_ROWS = [448, 1792, 1792, 448, 128, 128, 608]
MATRIX_ROWS = 232960
FLAT_ROWS = 233000
SEG = 29125
NDEV = 8

WIDTH_ORDER = (38, 7, 1)
GROUPS = {38: (16,), 7: (16, 32, 64), 1: (16, 128, 256)}
STAGE_ROWS = max(br * WIDTHS[t] for t, br in enumerate(BLOCK_ROWS))

def split(refs, counts):
    refs = list(refs)
    return [[refs.pop(0) for _ in range(n)] for n in counts]


ANY = pl.BlockSpec(memory_space=pl.ANY)
VMEM_SPEC = pl.BlockSpec(memory_space=pltpu.VMEM)
SMEM_SPEC = pl.BlockSpec(memory_space=pltpu.SMEM)
DMA = pltpu.SemaphoreType.DMA
VMEM_LIMIT = 63 * 1024 * 1024
COST = pl.CostEstimate(flops=2 * 10 ** 8, bytes_accessed=10 ** 8, transcendentals=0)


def tile_scratch(slots, rows):
    return [pltpu.VMEM((slots, r, w * LANES), BF16) for r, w in zip(rows, WIDTH_ORDER)]


def width_slot(width):
    return WIDTH_ORDER.index(width)


def row_group(rows, width):
    return max(g for g in GROUPS[width] if rows % g == 0)


PIECE = 912
PIECES = 32
LATE_FIRST, LATE_END = 25, 31
LATE_ROWS = PIECE * (LATE_END - LATE_FIRST) + 16
PIECE_LAST = SEG - (PIECES - 1) * PIECE
HALF = (PIECES - LATE_END + LATE_FIRST) // 2
LATE_HALF = (LATE_ROWS + 16) // 2
LATE_STARTS = (0, LATE_ROWS - LATE_HALF)
LATE_RANGES = [((SEG * s + PIECE * LATE_FIRST) // 8 * 8, -(-(SEG * s + PIECE * LATE_END) // 8) * 8) for s in range(NDEV)]


def unpack_blocks():
    early, late = [], []
    for t in TENSORS:
        w, offset, total = WIDTHS[t], OFFSETS[t], NAMES_ROWS[t]
        cuts = {0, total}
        spans = []
        for low, high in LATE_RANGES:
            first = max(0, (low - offset) // (16 * w) * 16)
            end = min(total, -(-(high - offset) // (16 * w)) * 16)
            if first < end:
                spans.append((first, end))
                cuts |= {first, end}
        cuts = sorted(cuts)
        for begin, end in zip(cuts[:-1], cuts[1:]):
            is_late = any(first <= begin and end <= last for first, last in spans)
            count = -(-(end - begin) // BLOCK_ROWS[t])
            step = -(-(end - begin) // (16 * count)) * 16
            for row in range(begin, end, step):
                rows = min(step, end - row)
                low, high = offset + row * w, offset + (row + rows) * w
                middles = [l + LATE_STARTS[1] for l, _ in LATE_RANGES]
                edges = sorted({low, high} | {e for r in LATE_RANGES + [middles] for e in r if low < e < high})
                sources = []
                for e0, e1 in zip(edges[:-1], edges[1:]):
                    seg = [s for s, (l, h) in enumerate(LATE_RANGES) if l <= e0 and e1 <= h]
                    source = None
                    start = e0
                    if seg:
                        start = e0 - SEG * seg[0] - PIECE * LATE_FIRST + 8
                        half = int(e0 >= middles[seg[0]])
                        source, start = (seg[0], half), start - LATE_STARTS[half]
                    sources.append((source, start, e0 - low, e1 - e0))
                (late if is_late else early).append((t, row, rows, sources))
    return early, late


EARLY_BLOCKS, LATE_BLOCKS = unpack_blocks()
LATE_TENSORS = sorted({t for t, _, _, _ in LATE_BLOCKS})
SLOTS = 4


def unpack_body(blocks, flat, lates, outs, tiles, stage, in_sem, out_sem):
    def loads(b, start=True):
        for n, (source, row, to, rows) in enumerate(blocks[b][3]):
            def copy(ref):
                return pltpu.make_async_copy(ref.at[pl.ds(row, rows), 0], stage.at[b % SLOTS, pl.ds(to, rows)], in_sem.at[b % SLOTS, n])

            if not start:
                copy(flat).wait()
            elif source is None:
                copy(flat).start()
            else:
                for relation in range(NDEV):
                    @pl.when(lax.bitwise_xor(lax.axis_index("dp"), source[0]) == relation)
                    def _():
                        copy(lates[relation][source[1]]).start()

    def store(b):
        t, row, rows, _ = blocks[b]
        return pltpu.make_async_copy(tiles[width_slot(WIDTHS[t])].at[b % SLOTS, pl.ds(0, rows)], outs[t].at[pl.ds(row, rows)], out_sem.at[b % SLOTS])

    for b in range(min(SLOTS, len(blocks))):
        loads(b)
    yield
    for b, (t, row, rows, _) in enumerate(blocks):
        w = WIDTHS[t]
        tile = tiles[width_slot(w)]
        group = row_group(rows, w)
        loads(b, start=False)
        if b >= SLOTS:
            store(b - SLOTS).wait()

        @pl.loop(0, rows // group)
        def _(i):
            for j in range(w):
                if w == 1:
                    block = stage[b % SLOTS, pl.ds(pl.multiple_of(i * group, 16), group), :]
                else:
                    block = stage[b % SLOTS, pl.ds(i * (group * w) + j, group, stride=w), :]
                tile[b % SLOTS, pl.ds(pl.multiple_of(i * group, 16), group), pl.ds(j * LANES, LANES)] = block.astype(BF16)

        store(b).start()
        if b + SLOTS < len(blocks):
            loads(b + SLOTS)
    for b in range(max(0, len(blocks) - SLOTS), len(blocks)):
        store(b).wait()


UNPACK_SCRATCH = tile_scratch(SLOTS, (128, 608, 1792)) + [pltpu.VMEM((SLOTS, STAGE_ROWS, LANES), F32)]
TENSOR_TYPES = [jax.ShapeDtypeStruct((r, w * LANES), BF16) for r, w in zip(NAMES_ROWS, WIDTHS)]


def unpack_early_kernel(tensors, flat, *refs):
    gains = len(refs) - len(tensors) - 8
    outs, norms, tiles, (stage, tail, in_sem, out_sem, tail_sem) = split(refs, (len(tensors), gains, 3, 5))
    tail_copy = pltpu.make_async_copy(flat.at[pl.ds(MATRIX_ROWS, TAIL), 0], tail, tail_sem)
    tail_copy.start()
    work = unpack_body([b for b in EARLY_BLOCKS if b[0] in tensors], flat, None, dict(zip(tensors, outs)), tiles, stage, in_sem, out_sem)
    next(work)
    tail_copy.wait()
    base = 0
    for n in norms:
        for j in COLUMNS:
            lines = [tail[pl.ds(base + j + 7 * layer, 1), :] for layer in range(n.shape[0])]
            n[:, pl.ds(j * LANES, LANES)] = jnp.concatenate(lines, axis=0).astype(BF16)
        base += 7 * n.shape[0]
    for _ in work:
        pass


def unpack_early(flat, tensors, gains):
    return pl.pallas_call(
        functools.partial(unpack_early_kernel, tensors),
        name="unpack_early",
        out_shape=[TENSOR_TYPES[t] for t in tensors] + [jax.ShapeDtypeStruct(s, BF16) for s in gains],
        in_specs=[ANY],
        out_specs=[ANY] * len(tensors) + [VMEM_SPEC] * len(gains),
        scratch_shapes=UNPACK_SCRATCH + [pltpu.VMEM((TAIL, LANES), F32), DMA((SLOTS, 4)), DMA((SLOTS,)), DMA],
        compiler_params=pltpu.CompilerParams(vmem_limit_bytes=VMEM_LIMIT),
        cost_estimate=COST,
    )(flat)


def unpack_late_kernel(flat, *refs):
    count = len(LATE_TENSORS)
    lates, _, outs, tiles, (stage, in_sem, out_sem) = split(refs, (2 * NDEV, count, count, 3, 3))
    for _ in unpack_body(LATE_BLOCKS, flat, list(zip(lates[::2], lates[1::2])), dict(zip(LATE_TENSORS, outs)), tiles, stage, in_sem, out_sem):
        pass


def unpack_late(flat, lates, params):
    count = len(LATE_TENSORS)
    lates = [a for pair in lates for a in pair]
    outs = pl.pallas_call(
        unpack_late_kernel,
        name="unpack_late",
        out_shape=[TENSOR_TYPES[t] for t in LATE_TENSORS],
        in_specs=[ANY] * (1 + len(lates) + count),
        out_specs=[ANY] * count,
        input_output_aliases={1 + len(lates) + n: n for n in range(count)},
        scratch_shapes=UNPACK_SCRATCH + [DMA((SLOTS, 4)), DMA((SLOTS,))],
        compiler_params=pltpu.CompilerParams(vmem_limit_bytes=VMEM_LIMIT),
        cost_estimate=COST,
    )(flat, *lates, *[params[t] for t in LATE_TENSORS])
    return {**params, **dict(zip(LATE_TENSORS, outs))}


def neighbours():
    me = lax.axis_index("dp")
    core, x, y = lax.rem(me, 2), lax.rem(me // 2, 2), me // 4
    other = 1 - 2 * core
    step_x, step_y = 2 - 4 * x, 4 - 8 * y
    return me, other, me + step_x, me + step_y, me + step_x + step_y


CHUNKS = 16
RS_ROWS = 911
RS_HALF_START = SEG - CHUNKS * RS_ROWS
UNITS = CHUNKS // 4
KIND_D, KIND_N, KIND_S, KIND_O = range(4)
CHIP_D, CHIP_X, CHIP_Y, CHIP_OWN = range(4)
UNIT_ROWS = 4 * RS_ROWS
MARGIN = 16 * 38
PACK_ROWS = {38: 112, 7: 608, 1: 896}
PACK_STAGE = 112 * 38
PACK_SLOTS = 3


def pack_blocks(chip, unit):
    blocks = []
    for parity in HALVES:
        for h in HALVES:
            begin = SEG * (2 * chip + parity) + RS_HALF_START * h + UNIT_ROWS * unit
            for t in TENSORS:
                w, offset, total = WIDTHS[t], OFFSETS[t], NAMES_ROWS[t]
                low, high = max(begin, offset), min(begin + UNIT_ROWS, offset + total * w)
                if low >= high:
                    continue
                first = (low - offset) // (16 * w) * 16
                end = -(-(high - offset) // (16 * w)) * 16
                step = -(-(end - first) // (16 * -(-(end - first) // PACK_ROWS[w]))) * 16
                for row in range(first, end, step):
                    blocks.append((t, row, min(step, end - row), parity, h, offset + row * w - begin + MARGIN))
    return blocks


def reduce_kernel(*refs):
    (grads, norms, (g_out, norm_out, flat, land_p, land_d, land_n),
     (mine, part, first, land_s, sums, g_buf, ss, ss_all), tiles, (stage, tail),
     (p_send, p_recv, i_send, i_recv, load_sem, g_sem, ss_send, ss_recv, in_sem, out_sem, tail_sem)) = split(refs, (7, 3, 6, 8, 3, 2, 11))
    me, other, dev_x, dev_y, dev_d = neighbours()
    core, x, y = lax.rem(me, 2), lax.rem(me // 2, 2), me // 4
    barrier = pltpu.get_barrier_semaphore()
    for d in range(1, NDEV):
        pl.semaphore_signal(barrier, inc=1, device_id=(lax.rem(me + d, NDEV),), device_id_type=MESH)

    tail[...] = jnp.zeros_like(tail)
    line = 0
    for n in norms:
        for layer in range(n.shape[0]):
            for j in COLUMNS:
                tail[pl.ds(line, 1), :] = n[pl.ds(layer, 1), pl.ds(j * LANES, LANES)].astype(F32)
                line += 1

    def pack(place, chip, unit):
        blocks = pack_blocks(chip, unit)

        def load(b):
            t, row, rows = blocks[b][:3]
            return pltpu.make_async_copy(grads[t].at[pl.ds(row, rows)], tiles[width_slot(WIDTHS[t])].at[b % PACK_SLOTS, pl.ds(0, rows)], in_sem.at[b % PACK_SLOTS])

        def store(b):
            t, _, rows, parity, h, to = blocks[b]
            size = rows * WIDTHS[t]
            return pltpu.make_async_copy(stage.at[b % PACK_SLOTS, pl.ds(0, size)], flat.at[place, unit, parity, h, pl.ds(to, size), 0], out_sem.at[b % PACK_SLOTS])

        for b in range(PACK_SLOTS):
            load(b).start()
        tail_copies = [pltpu.make_async_copy(tail, flat.at[place, unit, 1, 1, pl.ds(MARGIN + UNIT_ROWS - TAIL, TAIL), 0], tail_sem)
                       for _ in range(chip * unit // (3 * UNITS - 3))]
        for copy in tail_copies:
            copy.start()
        for b, block in enumerate(blocks):
            t, rows = block[0], block[2]
            w = WIDTHS[t]
            tile = tiles[width_slot(w)]
            group = row_group(rows, w)
            load(b).wait()
            if b >= PACK_SLOTS:
                store(b - PACK_SLOTS).wait()

            @pl.loop(0, rows // group)
            def _(i):
                for j in range(w):
                    values = tile[b % PACK_SLOTS, pl.ds(pl.multiple_of(i * group, 16), group), pl.ds(j * LANES, LANES)].astype(F32)
                    if w == 1:
                        stage[b % PACK_SLOTS, pl.ds(pl.multiple_of(i * group, 16), group), :] = values
                    else:
                        stage[b % PACK_SLOTS, pl.ds(i * (group * w) + j, group, stride=w), :] = values

            store(b).start()
            if b + PACK_SLOTS < len(blocks):
                load(b + PACK_SLOTS).start()
        for b in range(len(blocks) - PACK_SLOTS, len(blocks)):
            store(b).wait()
        for copy in tail_copies:
            copy.wait()

    def place_of(kind, h):
        return ((CHIP_D, CHIP_D), (CHIP_X, CHIP_Y), (CHIP_Y, CHIP_X), (CHIP_OWN, CHIP_OWN))[kind][h]

    def chunk(kind, h, i, parity):
        return flat.at[place_of(kind, h), i // 4, parity, h, pl.ds(MARGIN + RS_ROWS * lax.rem(i, 4), RS_ROWS)]

    def start_row(h, i):
        return RS_HALF_START * h + RS_ROWS * i

    def partner_copy(kind, h, i):
        return pltpu.make_async_remote_copy(
            src_ref=chunk(kind, h, i, 1 - core), dst_ref=land_p.at[kind, h, i],
            send_sem=p_send.at[kind, h, i], recv_sem=p_recv.at[kind, h, i],
            device_id=(me + other,), device_id_type=MESH)

    def link_copy(kind, h, i):
        land = land_s.at[h, i] if kind == KIND_S else (land_d, land_n)[kind].at[h, i, pl.ds(0, RS_ROWS), 0]
        to = ((dev_x, dev_y), (dev_x, dev_y), (dev_y, dev_x))[kind][h]
        return pltpu.make_async_remote_copy(
            src_ref=sums.at[kind % 2, h, i], dst_ref=land,
            send_sem=i_send.at[kind, h, i], recv_sem=i_recv.at[kind, h, i],
            device_id=(to,), device_id_type=MESH)

    def load_mine(kind, h, i):
        return pltpu.make_async_copy(chunk(kind, h, i, core).at[:, 0], mine.at[h], load_sem.at[0, h])

    def load_part(kind, h, i):
        return pltpu.make_async_copy(land_p.at[kind, h, i, pl.ds(0, RS_ROWS), 0], part.at[h], load_sem.at[1, h])

    def load_link(land, buf, n, h, i):
        return pltpu.make_async_copy(land.at[h, i, pl.ds(0, RS_ROWS), 0], buf.at[h], load_sem.at[n, h])

    def store_g(h, i):
        return pltpu.make_async_copy(g_buf.at[h], g_out.at[pl.ds(start_row(h, i), RS_ROWS), 0], g_sem.at[h])

    def exchange(kinds, begin, end):
        @pl.loop(begin, end)
        def _(i):
            for kind in kinds:
                for h in HALVES:
                    partner_copy(kind, h, i).start()

    def send(kind, begin, end):
        @pl.loop(begin, end)
        def _(i):
            for h in HALVES:
                load_mine(kind, h, i).start()
            for h in HALVES:
                partner_copy(kind, h, i).wait_recv()
                load_part(kind, h, i).start()
                if kind == KIND_S:
                    link_copy(KIND_D, h, i).wait_recv()
                    load_link(land_d, first, 2, h, i).start()
            for h in HALVES:
                load_mine(kind, h, i).wait()
                load_part(kind, h, i).wait()
                total = mine[h] + part[h]
                if kind == KIND_S:
                    load_link(land_d, first, 2, h, i).wait()
                    total = total + first[h]
                    link_copy(KIND_D, h, i).wait_send()
                sums[kind % 2, h, i] = total
                link_copy(kind, h, i).start()

    @pl.loop(0, 4 * UNITS)
    def _(n):
        place, unit = n // UNITS, lax.rem(n, UNITS)
        flip_x, flip_y = 1 - place // 2, 1 - lax.rem(place, 2)
        chip = (x + flip_x * (1 - 2 * x)) + 2 * (y + flip_y * (1 - 2 * y))
        for case in range(4 * UNITS):
            @pl.when(UNITS * chip + unit == case)
            def _():
                pack(place, case // UNITS, case % UNITS)

        @pl.when(n == 0)
        def _():
            pl.semaphore_wait(barrier, NDEV - 1)

        @pl.when(n < UNITS)
        def _():
            exchange((KIND_D,), 4 * unit, 4 * unit + 4)
            send(KIND_D, 4 * unit, 4 * unit + 4)

        @pl.when(n == 3 * UNITS - 1)
        def _():
            exchange((KIND_N, KIND_S), 0, CHUNKS)
            send(KIND_N, 0, CHUNKS)

    exchange((KIND_O,), 0, CHUNKS)
    send(KIND_S, 0, CHUNKS)

    def last(i, acc):
        for h in HALVES:
            load_mine(KIND_O, h, i).start()
            partner_copy(KIND_O, h, i).wait_recv()
            load_part(KIND_O, h, i).start()
        for h in HALVES:
            link_copy(KIND_N, h, i).wait_recv()
            load_link(land_n, first, 2, h, i).start()
        for h in HALVES:
            load_mine(KIND_O, h, i).wait()
            load_part(KIND_O, h, i).wait()
            load_link(land_n, first, 2, h, i).wait()
            link_copy(KIND_S, h, i).wait_recv()

            @pl.when(i > 0)
            def _():
                store_g(h, i - 1).wait()

            g = ((mine[h] + part[h]) + (first[h] + land_s[h, i])) * (1.0 / NDEV)
            g_buf[h] = g
            store_g(h, i).start()
            square = g * g
            if h == 1:
                row = lax.broadcasted_iota(jnp.int32, (RS_ROWS, LANES), 0) + RS_ROWS * i
                square = jnp.where(row >= CHUNKS * RS_ROWS - RS_HALF_START, square, 0.0)
            acc = acc + jnp.sum(square, axis=0, keepdims=True)
        return acc

    acc = lax.fori_loop(0, CHUNKS, last, jnp.zeros((1, LANES), F32))
    ss[...] = jnp.broadcast_to(acc, (8, LANES))

    @pl.loop(0, CHUNKS)
    def _(i):
        for h in HALVES:
            for kind in range(4):
                partner_copy(kind, h, i).wait_send()
            for kind in (KIND_N, KIND_S):
                link_copy(kind, h, i).wait_send()

    def norm_copy(d):
        return pltpu.make_async_remote_copy(
            src_ref=ss, dst_ref=ss_all.at[d], send_sem=ss_send.at[d], recv_sem=ss_recv.at[d],
            device_id=(lax.rem(me + d, NDEV),), device_id_type=MESH)

    for d in range(1, NDEV):
        norm_copy(d).start()
    for h in HALVES:
        store_g(h, CHUNKS - 1).wait()
    ss_all[0] = ss[...]
    for d in range(1, NDEV):
        norm_copy(d).wait()
    total = jnp.zeros((8, LANES), F32)
    for dev in range(NDEV):
        total = total + ss_all[lax.rem(me - dev + NDEV, NDEV)]
    norm_out[...] = jnp.broadcast_to(jnp.sqrt(jnp.sum(total, axis=1, keepdims=True)), (8, LANES))


def reduce_grads(grads, norms):
    land = jax.ShapeDtypeStruct((2, CHUNKS, RS_ROWS, 1, LANES), F32)
    land_p = jax.ShapeDtypeStruct((4, 2, CHUNKS, RS_ROWS, 1, LANES), F32)
    flat = jax.ShapeDtypeStruct((4, UNITS, 2, 2, UNIT_ROWS + 2 * MARGIN, 1, LANES), F32)
    buf = pltpu.VMEM((2, RS_ROWS, LANES), F32)
    partner, link, pair, all_devs, slots = DMA((4, 2, CHUNKS)), DMA((3, 2, CHUNKS)), DMA((2,)), DMA((NDEV,)), DMA((PACK_SLOTS,))
    outs = pl.pallas_call(
        reduce_kernel,
        name="reduce_grads",
        out_shape=[jax.ShapeDtypeStruct((SEG, 1, LANES), F32), jax.ShapeDtypeStruct((8, LANES), F32), flat, land_p, land, land],
        in_specs=[ANY] * 7 + [VMEM_SPEC] * 3,
        out_specs=[ANY, VMEM_SPEC] + [ANY] * 4,
        scratch_shapes=[buf] * 3 + [pltpu.VMEM((2, CHUNKS, RS_ROWS, LANES), F32), pltpu.VMEM((2, 2, CHUNKS, RS_ROWS, LANES), F32), buf, pltpu.VMEM((8, LANES), F32), pltpu.VMEM((NDEV, 8, LANES), F32)]
        + tile_scratch(PACK_SLOTS, PACK_ROWS.values()) + [pltpu.VMEM((PACK_SLOTS, PACK_STAGE, LANES), F32), pltpu.VMEM((TAIL, LANES), F32)]
        + [partner, partner, link, link, DMA((4, 2)), pair, all_devs, all_devs, slots, slots, DMA],
        compiler_params=pltpu.CompilerParams(collective_id=0, has_side_effects=True, vmem_limit_bytes=VMEM_LIMIT),
        cost_estimate=COST,
    )(*grads, *norms)
    return outs[0], outs[1]


def adam_rows(g, m, v, p, norm_row, lr, decay):
    clip = jnp.minimum(1.0, MAX_NORM / (norm_row + CLIP_EPS))
    clipped = clip * g
    new_m = BETA_ONE * m + (1.0 - BETA_ONE) * clipped
    new_v = BETA_TWO * v + (1.0 - BETA_TWO) * clipped * clipped
    adam_dir = (new_m * (1.0 / BIAS_ONE)) / (jnp.sqrt(new_v * (1.0 / BIAS_TWO)) + ADAM_EPS)
    decay_term = jnp.where(decay, WEIGHT_DECAY * p, 0.0)
    return p - lr * (decay_term + adam_dir), new_m, new_v


STATE_ROWS = PIECE
STATE_COUNT = SEG // STATE_ROWS
STATE_LAST = SEG - STATE_COUNT * STATE_ROWS
STATE_SLOTS = 4
SUB = 152


def decay_rows(me, start, rows):
    return lax.broadcasted_iota(jnp.int32, (rows, LANES), 0) + (SEG * me + start) < MATRIX_ROWS


def gather_kernel(g, m, v, p, norm, lr, full, late_a, late_b, gb, mb, vb, pb, new_p, late_p,
                  load_sem, own_sem, late_sem, own_send, own_recv, fwd_send, fwd_recv, p_send, p_recv):
    me, other, dev_x, dev_y, dev_d = neighbours()
    partner = me + other
    barrier = pltpu.get_barrier_semaphore()
    for dev in (partner, dev_x, dev_y):
        pl.semaphore_signal(barrier, inc=1, device_id=(dev,), device_id_type=MESH)
    to = (dev_x, dev_y, partner)
    sources = (me, dev_x, dev_y, dev_d)

    def is_last(h, i):
        return h == 1 and isinstance(i, int) and i == HALF - 1

    def start_row(h, i):
        return PIECE * (PIECES - 1) if is_last(h, i) else PIECE * (HALF * h + i)

    def size(h, i):
        return PIECE_LAST if is_last(h, i) else PIECE

    def rows_of(dev, h, i):
        return full.at[pl.ds(SEG * dev + start_row(h, i), size(h, i)), 0]

    def loads(h, i):
        return loads_at(h, start_row(h, i), size(h, i))

    def loads_at(h, start, rows):
        start = pl.multiple_of(start, 8)
        copies = [pltpu.make_async_copy(g.at[pl.ds(start, rows), 0], gb.at[h, pl.ds(0, rows)], load_sem.at[0, h])]
        for n, (src, buf) in enumerate(((m, mb), (v, vb), (p, pb))):
            copies.append(pltpu.make_async_copy(src.at[pl.ds(start, rows)], buf.at[h, pl.ds(0, rows)], load_sem.at[n + 1, h]))
        return copies

    def own_copy(n, h, i):
        return pltpu.make_async_remote_copy(
            src_ref=new_p.at[h, i, pl.ds(0, size(h, i))], dst_ref=rows_of(me, h, i),
            send_sem=own_send.at[n, h, i], recv_sem=own_recv.at[n, h, i], device_id=(to[n],), device_id_type=MESH)

    def own_store(h, i):
        return pltpu.make_async_copy(new_p.at[h, i, pl.ds(0, size(h, i))], rows_of(me, h, i), own_sem.at[h, i])

    def forward(h, i):
        src = rows_of((dev_y, dev_x)[h], h, i)
        return pltpu.make_async_remote_copy(
            src_ref=src, dst_ref=src, send_sem=fwd_send.at[h, i], recv_sem=fwd_recv.at[h, i],
            device_id=((dev_x, dev_y)[h],), device_id_type=MESH)

    def arrival(n, h, i):
        src = rows_of((dev_x, dev_y, partner)[n], h, i)
        return pltpu.make_async_remote_copy(
            src_ref=src, dst_ref=src, send_sem=own_send.at[n, h, i], recv_sem=own_recv.at[n, h, i],
            device_id=(to[n],), device_id_type=MESH)

    def forward_arrival(h, i):
        src = rows_of(dev_d, h, i)
        return pltpu.make_async_remote_copy(
            src_ref=src, dst_ref=src, send_sem=fwd_send.at[h, i], recv_sem=fwd_recv.at[h, i],
            device_id=((dev_x, dev_y)[h],), device_id_type=MESH)

    def partner_copy(q, h, i):
        src = rows_of(sources[q], h, i)
        return pltpu.make_async_remote_copy(
            src_ref=src, dst_ref=src, send_sem=p_send.at[q - 1, h, i], recv_sem=p_recv.at[q - 1, h, i],
            device_id=(partner,), device_id_type=MESH)

    def partner_arrival(q, h, i):
        src = rows_of(sources[q] + other, h, i)
        return pltpu.make_async_remote_copy(
            src_ref=src, dst_ref=src, send_sem=p_send.at[q - 1, h, i], recv_sem=p_recv.at[q - 1, h, i],
            device_id=(partner,), device_id_type=MESH)

    def each(body):
        @pl.loop(0, HALF - 1)
        def _(i):
            body(i)

        body(HALF - 1)

    norm_row = norm[0:1, :]
    for h in HALVES:
        for copy in loads(h, 0):
            copy.start()
    pl.semaphore_wait(barrier, 3)

    def compute(h, out, first):
        @pl.loop(0, PIECE // SUB)
        def _(s):
            start = pl.multiple_of(s * SUB, 8)
            sub = pl.ds(start, SUB)
            out[sub] = adam_rows(gb[h, sub], mb[h, sub], vb[h, sub], pb[h, sub], norm_row, lr[0], decay_rows(me, first + start, SUB))[0]

    def update(i):
        for h in HALVES:
            for copy in loads(h, i):
                copy.wait()

            compute(h, new_p.at[h, i], start_row(h, i))
            for n in ((1, 0, 2) if h == 0 else (0, 1, 2)):
                own_copy(n, h, i).start()
            own_store(h, i).start()
            if isinstance(i, int):
                continue
            for last in (False, True):
                @pl.when((i == HALF - 2) == last)
                def _():
                    for copy in loads(h, HALF - 1 if last else i + 1):
                        copy.start()

    each(update)

    late_copies = []

    def late_store(src, row, rows, to):
        for out, start in zip((late_a, late_b), LATE_STARTS):
            low, high = max(to, start), min(to + rows, start + LATE_HALF)
            if low < high:
                late_copies.append(pltpu.make_async_copy(src.at[pl.ds(row + low - to, high - low)], out.at[pl.ds(low - start, high - low), 0], late_sem.at[len(late_copies)]))
                late_copies[-1].start()

    late_store(new_p.at[1, HALF - 2], PIECE - 8, 8, 0)
    late_store(new_p.at[1, HALF - 1], 0, 8, LATE_ROWS - 8)
    for j in range(LATE_END - LATE_FIRST):
        first = PIECE * (LATE_FIRST + j)
        for copy in loads_at(j % 2, first, PIECE):
            copy.start()
        for copy in loads_at(j % 2, first, PIECE):
            copy.wait()
        compute(j % 2, late_p.at[j], first)
        late_store(late_p.at[j], 0, PIECE, 8 + PIECE * j)

    def pass_on(i):
        arrival(1, 0, i).wait_recv()
        forward(0, i).start()
        partner_copy(2, 0, i).start()
        arrival(0, 1, i).wait_recv()
        forward(1, i).start()
        partner_copy(1, 1, i).start()
        arrival(0, 0, i).wait_recv()
        partner_copy(1, 0, i).start()
        arrival(1, 1, i).wait_recv()
        partner_copy(2, 1, i).start()

    each(pass_on)

    def pass_last(i):
        for h in HALVES:
            forward_arrival(h, i).wait_recv()
            partner_copy(3, h, i).start()

    each(pass_last)

    def finish(i):
        for h in HALVES:
            own_store(h, i).wait()
            arrival(2, h, i).wait_recv()
            for n in range(3):
                own_copy(n, h, i).wait_send()
            forward(h, i).wait_send()
            for q in range(1, 4):
                partner_copy(q, h, i).wait_send()
                partner_arrival(q, h, i).wait_recv()

    each(finish)
    for copy in late_copies:
        copy.wait()


def gather_params(g, m, v, p, norm, lr):
    buf = pltpu.VMEM((2, PIECE, LANES), F32)
    pairs = DMA((2, HALF))
    triples = DMA((3, 2, HALF))
    return pl.pallas_call(
        gather_kernel,
        name="gather_params",
        out_shape=[jax.ShapeDtypeStruct((FLAT_ROWS, 1, LANES), F32), jax.ShapeDtypeStruct((LATE_HALF, 1, LANES), F32), jax.ShapeDtypeStruct((LATE_HALF, 1, LANES), F32)],
        in_specs=[ANY] * 4 + [VMEM_SPEC, SMEM_SPEC],
        out_specs=[ANY] * 3,
        scratch_shapes=[buf, buf, buf, buf, pltpu.VMEM((2, HALF, PIECE, LANES), F32), pltpu.VMEM((LATE_END - LATE_FIRST, PIECE, LANES), F32),
                        DMA((4, 2)), pairs, DMA((LATE_END - LATE_FIRST + 4,)), triples, triples, pairs, pairs, triples, triples],
        compiler_params=pltpu.CompilerParams(collective_id=1, has_side_effects=True, vmem_limit_bytes=VMEM_LIMIT),
        cost_estimate=COST,
    )(g, m, v, p, norm, lr)


def state_kernel(g, m, v, p, norm, lr, new_p, new_m, new_v, gb, mb, vb, pb, pn, mn, vn, in_sem, out_sem):
    me = lax.axis_index("dp")
    norm_row = norm[pl.ds(0, 1), :]

    def window(i):
        rows = STATE_LAST if isinstance(i, int) and i == STATE_COUNT else STATE_ROWS
        slot = lax.rem(i, STATE_SLOTS)
        return slot, pl.ds(pl.multiple_of(i * STATE_ROWS, 8), rows), pl.ds(0, rows)

    def loads(i):
        slot, rows, size = window(i)
        pairs = ((g.at[rows, 0], gb), (m.at[rows], mb), (v.at[rows], vb), (p.at[rows], pb))
        return [pltpu.make_async_copy(src, buf.at[slot, size], in_sem.at[n, slot]) for n, (src, buf) in enumerate(pairs)]

    def stores(i):
        slot, rows, size = window(i)
        pairs = ((pn, new_p), (mn, new_m), (vn, new_v))
        return [pltpu.make_async_copy(buf.at[slot, size], dst.at[rows], out_sem.at[n, slot]) for n, (buf, dst) in enumerate(pairs)]

    def run(copies, wait=False):
        for copy in copies:
            copy.wait() if wait else copy.start()

    def compute(i):
        slot = lax.rem(i, STATE_SLOTS)

        @pl.loop(0, STATE_ROWS // SUB)
        def _(s):
            start = pl.multiple_of(s * SUB, 8)
            rows = pl.ds(start, SUB)
            pn[slot, rows], mn[slot, rows], vn[slot, rows] = adam_rows(
                gb[slot, rows], mb[slot, rows], vb[slot, rows], pb[slot, rows], norm_row, lr[0],
                decay_rows(me, i * STATE_ROWS + start, SUB))

    for i in range(STATE_SLOTS):
        run(loads(i))

    @pl.loop(0, STATE_COUNT)
    def _(i):
        run(loads(i), wait=True)

        @pl.when(i >= STATE_SLOTS)
        def _():
            run(stores(i - STATE_SLOTS), wait=True)

        compute(i)
        run(stores(i))

        @pl.when(i + STATE_SLOTS < STATE_COUNT)
        def _():
            run(loads(i + STATE_SLOTS))

        @pl.when(i + STATE_SLOTS == STATE_COUNT)
        def _():
            run(loads(STATE_COUNT))

    run(loads(STATE_COUNT), wait=True)
    run(stores(STATE_COUNT - STATE_SLOTS), wait=True)
    compute(STATE_COUNT)
    run(stores(STATE_COUNT))
    for n in range(STATE_SLOTS):
        run(stores(STATE_COUNT - STATE_SLOTS + 1 + n), wait=True)


def new_state(g, m, v, p, norm, lr):
    return pl.pallas_call(
        state_kernel,
        name="new_state",
        out_shape=[jax.ShapeDtypeStruct((SEG, LANES), F32)] * 3,
        in_specs=[ANY] * 4 + [VMEM_SPEC, SMEM_SPEC],
        out_specs=[ANY] * 3,
        scratch_shapes=[pltpu.VMEM((STATE_SLOTS, STATE_ROWS, LANES), F32)] * 7 + [DMA((4, STATE_SLOTS)), DMA((3, STATE_SLOTS))],
        compiler_params=pltpu.CompilerParams(vmem_limit_bytes=VMEM_LIMIT),
        cost_estimate=COST,
    )(g, m, v, p, norm, lr)


def solution(mesh):
    def local_step(*arrays):
        grads = [a.reshape(r, w * LANES) for a, r, w in zip(arrays[:7], NAMES_ROWS, WIDTHS)]
        norms = [a.reshape(s) for a, s in zip(arrays[7:10], GAINS)]
        master, exp_avg, exp_avg_sq = [a.reshape(SEG, LANES) for a in arrays[10:13]]
        lr = arrays[13].reshape(1)
        g, norm = reduce_grads(grads, norms)
        full, *late = gather_params(g, exp_avg, exp_avg_sq, master, norm, lr)

        def permute(a, bits):
            return lax.ppermute(a, "dp", [(d, d ^ bits) for d in range(NDEV)])

        by_y, by_x = permute(late[0], 4), permute(late[1], 2)
        far_x, far_y = permute(late[0], 2), permute(late[1], 4)
        own = [permute(a, 1) for a in late]
        state = list(new_state(g, exp_avg, exp_avg_sq, master, norm, lr))
        by_y, by_x, full, state[0] = lax.optimization_barrier((by_y, by_x, full, state[0]))
        across = (permute(by_y, 2), permute(by_x, 4))
        from_y, from_x = permute(by_y, 1), permute(by_x, 1)
        wide, down, small = (4, 5), (6,), (0, 1, 2, 3)
        params = dict(zip(wide, unpack_early(full, wide, [])))
        far_x, far_y, full, params[4] = lax.optimization_barrier((far_x, far_y, full, params[4]))
        far = permute(far_x, 1), permute(far_y, 1)
        params[6], = unpack_early(full, down, [])
        *across, full, params[6] = lax.optimization_barrier((*across, full, params[6]))
        from_across = [permute(a, 1) for a in across]
        rest = list(unpack_early(full, small, GAINS))
        params |= dict(zip(small, rest))
        lates = [late, own, (far_x, by_x), (far[0], from_x), (by_y, far_y), (from_y, far[1]), across, from_across]
        params = unpack_late(full, lates, params)
        params = [params[t] for t in TENSORS] + rest[len(small):]
        shapes = SHAPES + GAINS[:2] + [(D,)]
        return tuple([a.reshape(-1) for a in state] + [a.reshape(s) for a, s in zip(params, shapes)] + [norm[0, 0]])

    return jax.shard_map(local_step, mesh=mesh, in_specs=(P("dp"),) * 13 + (P(),), out_specs=(P("dp"),) * 3 + (P(),) * 11, check_vma=False)
```

```python
import functools
import math
import jax
import jax.numpy as jnp
from jax import lax
from jax.experimental import pallas as pl
from jax.experimental.pallas import tpu as pltpu
from jax.sharding import PartitionSpec as P

BETA_ONE = 0.9
BETA_TWO = 0.95
ADAM_EPS = 1e-8
WEIGHT_DECAY = 0.1
MAX_NORM = 1.0
CLIP_EPS = 1e-6
STEP = 4
BIAS_ONE = 1.0 - BETA_ONE ** STEP
BIAS_TWO = 1.0 - BETA_TWO ** STEP

MESH = pl.DeviceIdType.MESH
F32 = jnp.float32
BF16 = jnp.bfloat16
LANES = 128

LAYERS, D, KV, FF = 2, 896, 128, 4864
SHAPES = [(LAYERS, D, D), (LAYERS, D, KV), (LAYERS, D, KV), (LAYERS, D, D), (LAYERS, D, FF), (LAYERS, D, FF), (LAYERS, FF, D)]
GAINS = [(LAYERS, D), (LAYERS, D), (1, D)]
TAIL = 40
HALVES, TENSORS, COLUMNS = range(2), range(7), range(7)
NAMES_ROWS = [math.prod(s[:-1]) for s in SHAPES]
WIDTHS = [s[-1] // LANES for s in SHAPES]
OFFSETS = [sum(r * w for r, w in zip(NAMES_ROWS[:t], WIDTHS[:t])) for t in TENSORS]
BLOCK_ROWS = [448, 1792, 1792, 448, 128, 128, 608]
MATRIX_ROWS = 232960
FLAT_ROWS = 233000
SEG = 29125
NDEV = 8

WIDTH_ORDER = (38, 7, 1)
GROUPS = {38: (16,), 7: (16, 32, 64), 1: (16, 128, 256)}
STAGE_ROWS = max(br * WIDTHS[t] for t, br in enumerate(BLOCK_ROWS))

def split(refs, counts):
    refs = list(refs)
    return [[refs.pop(0) for _ in range(n)] for n in counts]


ANY = pl.BlockSpec(memory_space=pl.ANY)
VMEM_SPEC = pl.BlockSpec(memory_space=pltpu.VMEM)
SMEM_SPEC = pl.BlockSpec(memory_space=pltpu.SMEM)
DMA = pltpu.SemaphoreType.DMA
VMEM_LIMIT = 63 * 1024 * 1024
COST = pl.CostEstimate(flops=2 * 10 ** 8, bytes_accessed=10 ** 8, transcendentals=0)


def tile_scratch(slots, rows):
    return [pltpu.VMEM((slots, r, w * LANES), BF16) for r, w in zip(rows, WIDTH_ORDER)]


def width_slot(width):
    return WIDTH_ORDER.index(width)


def row_group(rows, width):
    return max(g for g in GROUPS[width] if rows % g == 0)


PIECE = 912
PIECES = 32
LATE_FIRST, LATE_END = 25, 31
LATE_ROWS = PIECE * (LATE_END - LATE_FIRST) + 16
PIECE_LAST = SEG - (PIECES - 1) * PIECE
HALF = (PIECES - LATE_END + LATE_FIRST) // 2
LATE_HALF = (LATE_ROWS + 16) // 2
LATE_STARTS = (0, LATE_ROWS - LATE_HALF)
LATE_RANGES = [((SEG * s + PIECE * LATE_FIRST) // 8 * 8, -(-(SEG * s + PIECE * LATE_END) // 8) * 8) for s in range(NDEV)]


def unpack_blocks():
    early, late = [], []
    for t in TENSORS:
        w, offset, total = WIDTHS[t], OFFSETS[t], NAMES_ROWS[t]
        cuts = {0, total}
        spans = []
        for low, high in LATE_RANGES:
            first = max(0, (low - offset) // (16 * w) * 16)
            end = min(total, -(-(high - offset) // (16 * w)) * 16)
            if first < end:
                spans.append((first, end))
                cuts |= {first, end}
        cuts = sorted(cuts)
        for begin, end in zip(cuts[:-1], cuts[1:]):
            is_late = any(first <= begin and end <= last for first, last in spans)
            count = -(-(end - begin) // BLOCK_ROWS[t])
            step = -(-(end - begin) // (16 * count)) * 16
            for row in range(begin, end, step):
                rows = min(step, end - row)
                low, high = offset + row * w, offset + (row + rows) * w
                middles = [l + LATE_STARTS[1] for l, _ in LATE_RANGES]
                edges = sorted({low, high} | {e for r in LATE_RANGES + [middles] for e in r if low < e < high})
                sources = []
                for e0, e1 in zip(edges[:-1], edges[1:]):
                    seg = [s for s, (l, h) in enumerate(LATE_RANGES) if l <= e0 and e1 <= h]
                    source = None
                    start = e0
                    if seg:
                        start = e0 - SEG * seg[0] - PIECE * LATE_FIRST + 8
                        half = int(e0 >= middles[seg[0]])
                        source, start = (seg[0], half), start - LATE_STARTS[half]
                    sources.append((source, start, e0 - low, e1 - e0))
                (late if is_late else early).append((t, row, rows, sources))
    return early, late


EARLY_BLOCKS, LATE_BLOCKS = unpack_blocks()
LATE_TENSORS = sorted({t for t, _, _, _ in LATE_BLOCKS})
SLOTS = 4


def unpack_body(blocks, flat, lates, outs, tiles, stage, in_sem, out_sem, wanted=None):
    def when(b):
        return pl.when(wanted(b)) if wanted else lambda f: f()

    def loads(b, start=True):
        for n, (source, row, to, rows) in enumerate(blocks[b][3]):
            def copy(ref):
                return pltpu.make_async_copy(ref.at[pl.ds(row, rows), 0], stage.at[b % SLOTS, pl.ds(to, rows)], in_sem.at[b % SLOTS, n])

            if not start:
                copy(flat).wait()
            elif source is None:
                copy(flat).start()
            else:
                for relation, halves in lates.items():
                    @pl.when(lax.bitwise_xor(lax.axis_index("dp"), source[0]) == relation)
                    def _():
                        copy(halves[source[1]]).start()

    def store(b):
        t, row, rows, _ = blocks[b]
        return pltpu.make_async_copy(tiles[width_slot(WIDTHS[t])].at[b % SLOTS, pl.ds(0, rows)], outs[t].at[pl.ds(row, rows)], out_sem.at[b % SLOTS])

    for b in range(min(SLOTS, len(blocks))):
        when(b)(lambda: loads(b))
    yield
    for b, (t, row, rows, _) in enumerate(blocks):
        w = WIDTHS[t]
        tile = tiles[width_slot(w)]
        group = row_group(rows, w)
        if b >= SLOTS:
            when(b - SLOTS)(lambda: store(b - SLOTS).wait())

        @when(b)
        def _():
            loads(b, start=False)

            @pl.loop(0, rows // group)
            def _(i):
                for j in range(w):
                    if w == 1:
                        block = stage[b % SLOTS, pl.ds(pl.multiple_of(i * group, 16), group), :]
                    else:
                        block = stage[b % SLOTS, pl.ds(i * (group * w) + j, group, stride=w), :]
                    tile[b % SLOTS, pl.ds(pl.multiple_of(i * group, 16), group), pl.ds(j * LANES, LANES)] = block.astype(BF16)

            store(b).start()

        if b + SLOTS < len(blocks):
            when(b + SLOTS)(lambda: loads(b + SLOTS))
    for b in range(max(0, len(blocks) - SLOTS), len(blocks)):
        when(b)(lambda: store(b).wait())


UNPACK_SCRATCH = tile_scratch(SLOTS, (128, 608, 1792)) + [pltpu.VMEM((SLOTS, STAGE_ROWS, LANES), F32)]
TENSOR_TYPES = [jax.ShapeDtypeStruct((r, w * LANES), BF16) for r, w in zip(NAMES_ROWS, WIDTHS)]


def unpack_early_kernel(tensors, flat, *refs):
    gains = len(refs) - len(tensors) - 8
    outs, norms, tiles, (stage, tail, in_sem, out_sem, tail_sem) = split(refs, (len(tensors), gains, 3, 5))
    tail_copy = pltpu.make_async_copy(flat.at[pl.ds(MATRIX_ROWS, TAIL), 0], tail, tail_sem)
    tail_copy.start()
    work = unpack_body([b for b in EARLY_BLOCKS if b[0] in tensors], flat, None, dict(zip(tensors, outs)), tiles, stage, in_sem, out_sem)
    next(work)
    tail_copy.wait()
    base = 0
    for n in norms:
        for j in COLUMNS:
            lines = [tail[pl.ds(base + j + 7 * layer, 1), :] for layer in range(n.shape[0])]
            n[:, pl.ds(j * LANES, LANES)] = jnp.concatenate(lines, axis=0).astype(BF16)
        base += 7 * n.shape[0]
    for _ in work:
        pass


def unpack_early(flat, tensors, gains):
    return pl.pallas_call(
        functools.partial(unpack_early_kernel, tensors),
        name="unpack_early",
        out_shape=[TENSOR_TYPES[t] for t in tensors] + [jax.ShapeDtypeStruct(s, BF16) for s in gains],
        in_specs=[ANY],
        out_specs=[ANY] * len(tensors) + [VMEM_SPEC] * len(gains),
        scratch_shapes=UNPACK_SCRATCH + [pltpu.VMEM((TAIL, LANES), F32), DMA((SLOTS, 4)), DMA((SLOTS,)), DMA],
        compiler_params=pltpu.CompilerParams(vmem_limit_bytes=VMEM_LIMIT),
        cost_estimate=COST,
    )(flat)


def unpack_late_kernel(relations, flat, *refs):
    count = len(LATE_TENSORS)
    lates, _, outs, tiles, (stage, in_sem, out_sem) = split(refs, (2 * len(relations), count, count, 3, 3))
    lates = dict(zip(relations, zip(lates[::2], lates[1::2])))

    def wanted(b):
        seg = [source[0] for source, _, _, _ in LATE_BLOCKS[b][3] if source][0]
        relation = lax.bitwise_xor(lax.axis_index("dp"), seg)
        return jnp.logical_and(relation >= relations[0], relation <= relations[-1])

    for _ in unpack_body(LATE_BLOCKS, flat, lates, dict(zip(LATE_TENSORS, outs)), tiles, stage, in_sem, out_sem, wanted):
        pass


def unpack_late(flat, lates, params):
    count = len(LATE_TENSORS)
    relations = sorted(lates)
    lates = [a for r in relations for a in lates[r]]
    outs = pl.pallas_call(
        functools.partial(unpack_late_kernel, relations),
        name="unpack_late",
        out_shape=[TENSOR_TYPES[t] for t in LATE_TENSORS],
        in_specs=[ANY] * (1 + len(lates) + count),
        out_specs=[ANY] * count,
        input_output_aliases={1 + len(lates) + n: n for n in range(count)},
        scratch_shapes=UNPACK_SCRATCH + [DMA((SLOTS, 4)), DMA((SLOTS,))],
        compiler_params=pltpu.CompilerParams(vmem_limit_bytes=VMEM_LIMIT),
        cost_estimate=COST,
    )(flat, *lates, *[params[t] for t in LATE_TENSORS])
    return {**params, **dict(zip(LATE_TENSORS, outs))}


def neighbours():
    me = lax.axis_index("dp")
    core, x, y = lax.rem(me, 2), lax.rem(me // 2, 2), me // 4
    other = 1 - 2 * core
    step_x, step_y = 2 - 4 * x, 4 - 8 * y
    return me, other, me + step_x, me + step_y, me + step_x + step_y


CHUNKS = 16
RS_ROWS = 911
RS_HALF_START = SEG - CHUNKS * RS_ROWS
UNITS = CHUNKS // 4
KIND_D, KIND_N, KIND_S, KIND_O = range(4)
CHIP_D, CHIP_X, CHIP_Y, CHIP_OWN = range(4)
UNIT_ROWS = 4 * RS_ROWS
MARGIN = 16 * 38
PACK_ROWS = {38: 112, 7: 608, 1: 896}
PACK_STAGE = 112 * 38
PACK_SLOTS = 3


def pack_blocks(chip, unit):
    blocks = []
    for parity in HALVES:
        for h in HALVES:
            begin = SEG * (2 * chip + parity) + RS_HALF_START * h + UNIT_ROWS * unit
            for t in TENSORS:
                w, offset, total = WIDTHS[t], OFFSETS[t], NAMES_ROWS[t]
                low, high = max(begin, offset), min(begin + UNIT_ROWS, offset + total * w)
                if low >= high:
                    continue
                first = (low - offset) // (16 * w) * 16
                end = -(-(high - offset) // (16 * w)) * 16
                step = -(-(end - first) // (16 * -(-(end - first) // PACK_ROWS[w]))) * 16
                for row in range(first, end, step):
                    blocks.append((t, row, min(step, end - row), parity, h, offset + row * w - begin + MARGIN))
    return blocks


def reduce_kernel(*refs):
    (grads, norms, (g_out, norm_out, flat, land_p, land_d, land_n),
     (mine, part, first, land_s, sums, g_buf, ss, ss_all), tiles, (stage, tail),
     (p_send, p_recv, i_send, i_recv, load_sem, g_sem, ss_send, ss_recv, in_sem, out_sem, tail_sem)) = split(refs, (7, 3, 6, 8, 3, 2, 11))
    me, other, dev_x, dev_y, dev_d = neighbours()
    core, x, y = lax.rem(me, 2), lax.rem(me // 2, 2), me // 4
    barrier = pltpu.get_barrier_semaphore()
    for d in range(1, NDEV):
        pl.semaphore_signal(barrier, inc=1, device_id=(lax.rem(me + d, NDEV),), device_id_type=MESH)

    tail[...] = jnp.zeros_like(tail)
    line = 0
    for n in norms:
        for layer in range(n.shape[0]):
            for j in COLUMNS:
                tail[pl.ds(line, 1), :] = n[pl.ds(layer, 1), pl.ds(j * LANES, LANES)].astype(F32)
                line += 1

    def pack(place, chip, unit):
        blocks = pack_blocks(chip, unit)

        def load(b):
            t, row, rows = blocks[b][:3]
            return pltpu.make_async_copy(grads[t].at[pl.ds(row, rows)], tiles[width_slot(WIDTHS[t])].at[b % PACK_SLOTS, pl.ds(0, rows)], in_sem.at[b % PACK_SLOTS])

        def store(b):
            t, _, rows, parity, h, to = blocks[b]
            size = rows * WIDTHS[t]
            return pltpu.make_async_copy(stage.at[b % PACK_SLOTS, pl.ds(0, size)], flat.at[place, unit, parity, h, pl.ds(to, size), 0], out_sem.at[b % PACK_SLOTS])

        for b in range(PACK_SLOTS):
            load(b).start()
        tail_copies = [pltpu.make_async_copy(tail, flat.at[place, unit, 1, 1, pl.ds(MARGIN + UNIT_ROWS - TAIL, TAIL), 0], tail_sem)
                       for _ in range(chip * unit // (3 * UNITS - 3))]
        for copy in tail_copies:
            copy.start()
        for b, block in enumerate(blocks):
            t, rows = block[0], block[2]
            w = WIDTHS[t]
            tile = tiles[width_slot(w)]
            group = row_group(rows, w)
            load(b).wait()
            if b >= PACK_SLOTS:
                store(b - PACK_SLOTS).wait()

            @pl.loop(0, rows // group)
            def _(i):
                for j in range(w):
                    values = tile[b % PACK_SLOTS, pl.ds(pl.multiple_of(i * group, 16), group), pl.ds(j * LANES, LANES)].astype(F32)
                    if w == 1:
                        stage[b % PACK_SLOTS, pl.ds(pl.multiple_of(i * group, 16), group), :] = values
                    else:
                        stage[b % PACK_SLOTS, pl.ds(i * (group * w) + j, group, stride=w), :] = values

            store(b).start()
            if b + PACK_SLOTS < len(blocks):
                load(b + PACK_SLOTS).start()
        for b in range(len(blocks) - PACK_SLOTS, len(blocks)):
            store(b).wait()
        for copy in tail_copies:
            copy.wait()

    def place_of(kind, h):
        return ((CHIP_D, CHIP_D), (CHIP_X, CHIP_Y), (CHIP_Y, CHIP_X), (CHIP_OWN, CHIP_OWN))[kind][h]

    def chunk(kind, h, i, parity):
        return flat.at[place_of(kind, h), i // 4, parity, h, pl.ds(MARGIN + RS_ROWS * lax.rem(i, 4), RS_ROWS)]

    def start_row(h, i):
        return RS_HALF_START * h + RS_ROWS * i

    def partner_copy(kind, h, i):
        return pltpu.make_async_remote_copy(
            src_ref=chunk(kind, h, i, 1 - core), dst_ref=land_p.at[kind, h, i],
            send_sem=p_send.at[kind, h, i], recv_sem=p_recv.at[kind, h, i],
            device_id=(me + other,), device_id_type=MESH)

    def link_copy(kind, h, i):
        land = land_s.at[h, i] if kind == KIND_S else (land_d, land_n)[kind].at[h, i, pl.ds(0, RS_ROWS), 0]
        to = ((dev_x, dev_y), (dev_x, dev_y), (dev_y, dev_x))[kind][h]
        return pltpu.make_async_remote_copy(
            src_ref=sums.at[kind % 2, h, i], dst_ref=land,
            send_sem=i_send.at[kind, h, i], recv_sem=i_recv.at[kind, h, i],
            device_id=(to,), device_id_type=MESH)

    def load_mine(kind, h, i):
        return pltpu.make_async_copy(chunk(kind, h, i, core).at[:, 0], mine.at[h], load_sem.at[0, h])

    def load_part(kind, h, i):
        return pltpu.make_async_copy(land_p.at[kind, h, i, pl.ds(0, RS_ROWS), 0], part.at[h], load_sem.at[1, h])

    def load_link(land, buf, n, h, i):
        return pltpu.make_async_copy(land.at[h, i, pl.ds(0, RS_ROWS), 0], buf.at[h], load_sem.at[n, h])

    def store_g(h, i):
        return pltpu.make_async_copy(g_buf.at[h], g_out.at[pl.ds(start_row(h, i), RS_ROWS), 0], g_sem.at[h])

    def exchange(kinds, begin, end):
        @pl.loop(begin, end)
        def _(i):
            for kind in kinds:
                for h in HALVES:
                    partner_copy(kind, h, i).start()

    def send(kind, begin, end):
        @pl.loop(begin, end)
        def _(i):
            for h in HALVES:
                load_mine(kind, h, i).start()
            for h in HALVES:
                partner_copy(kind, h, i).wait_recv()
                load_part(kind, h, i).start()
                if kind == KIND_S:
                    link_copy(KIND_D, h, i).wait_recv()
                    load_link(land_d, first, 2, h, i).start()
            for h in HALVES:
                load_mine(kind, h, i).wait()
                load_part(kind, h, i).wait()
                total = mine[h] + part[h]
                if kind == KIND_S:
                    load_link(land_d, first, 2, h, i).wait()
                    total = total + first[h]
                    link_copy(KIND_D, h, i).wait_send()
                sums[kind % 2, h, i] = total
                link_copy(kind, h, i).start()

    @pl.loop(0, 4 * UNITS)
    def _(n):
        place, unit = n // UNITS, lax.rem(n, UNITS)
        flip_x, flip_y = 1 - place // 2, 1 - lax.rem(place, 2)
        chip = (x + flip_x * (1 - 2 * x)) + 2 * (y + flip_y * (1 - 2 * y))
        for case in range(4 * UNITS):
            @pl.when(UNITS * chip + unit == case)
            def _():
                pack(place, case // UNITS, case % UNITS)

        @pl.when(n == 0)
        def _():
            pl.semaphore_wait(barrier, NDEV - 1)

        @pl.when(n < UNITS)
        def _():
            exchange((KIND_D,), 4 * unit, 4 * unit + 4)
            send(KIND_D, 4 * unit, 4 * unit + 4)

        @pl.when(n == 3 * UNITS - 1)
        def _():
            exchange((KIND_N, KIND_S), 0, CHUNKS)
            send(KIND_N, 0, CHUNKS)

    exchange((KIND_O,), 0, CHUNKS)
    send(KIND_S, 0, CHUNKS)

    def last(i, acc):
        for h in HALVES:
            for kind in (KIND_D, KIND_N, KIND_S):
                partner_copy(kind, h, i).wait_send()
            link_copy(KIND_N, h, i).wait_send()

            @pl.when(i > 0)
            def _():
                partner_copy(KIND_O, h, i - 1).wait_send()
                link_copy(KIND_S, h, i - 1).wait_send()

        for h in HALVES:
            load_mine(KIND_O, h, i).start()
            partner_copy(KIND_O, h, i).wait_recv()
            load_part(KIND_O, h, i).start()
        for h in HALVES:
            link_copy(KIND_N, h, i).wait_recv()
            load_link(land_n, first, 2, h, i).start()
        for h in HALVES:
            load_mine(KIND_O, h, i).wait()
            load_part(KIND_O, h, i).wait()
            load_link(land_n, first, 2, h, i).wait()
            link_copy(KIND_S, h, i).wait_recv()

            @pl.when(i > 0)
            def _():
                store_g(h, i - 1).wait()

            g = ((mine[h] + part[h]) + (first[h] + land_s[h, i])) * (1.0 / NDEV)
            g_buf[h] = g
            store_g(h, i).start()
            square = g * g
            if h == 1:
                row = lax.broadcasted_iota(jnp.int32, (RS_ROWS, LANES), 0) + RS_ROWS * i
                square = jnp.where(row >= CHUNKS * RS_ROWS - RS_HALF_START, square, 0.0)
            acc = acc + jnp.sum(square, axis=0, keepdims=True)
        return acc

    acc = lax.fori_loop(0, CHUNKS, last, jnp.zeros((1, LANES), F32))
    ss[...] = jnp.broadcast_to(acc, (8, LANES))

    for h in HALVES:
        partner_copy(KIND_O, h, CHUNKS - 1).wait_send()
        link_copy(KIND_S, h, CHUNKS - 1).wait_send()
    store_g(0, CHUNKS - 1).wait()

    def norm_copy(d):
        return pltpu.make_async_remote_copy(
            src_ref=ss, dst_ref=ss_all.at[d], send_sem=ss_send.at[d], recv_sem=ss_recv.at[d],
            device_id=(lax.rem(me + d, NDEV),), device_id_type=MESH)

    for d in range(1, NDEV):
        norm_copy(d).start()
    store_g(1, CHUNKS - 1).wait()
    ss_all[0] = ss[...]
    for d in range(1, NDEV):
        norm_copy(d).wait()
    total = jnp.zeros((8, LANES), F32)
    for dev in range(NDEV):
        total = total + ss_all[lax.rem(me - dev + NDEV, NDEV)]
    norm_out[...] = jnp.broadcast_to(jnp.sqrt(jnp.sum(total, axis=1, keepdims=True)), (8, LANES))


def reduce_grads(grads, norms):
    land = jax.ShapeDtypeStruct((2, CHUNKS, RS_ROWS, 1, LANES), F32)
    land_p = jax.ShapeDtypeStruct((4, 2, CHUNKS, RS_ROWS, 1, LANES), F32)
    flat = jax.ShapeDtypeStruct((4, UNITS, 2, 2, UNIT_ROWS + 2 * MARGIN, 1, LANES), F32)
    buf = pltpu.VMEM((2, RS_ROWS, LANES), F32)
    partner, link, pair, all_devs, slots = DMA((4, 2, CHUNKS)), DMA((3, 2, CHUNKS)), DMA((2,)), DMA((NDEV,)), DMA((PACK_SLOTS,))
    outs = pl.pallas_call(
        reduce_kernel,
        name="reduce_grads",
        out_shape=[jax.ShapeDtypeStruct((SEG, 1, LANES), F32), jax.ShapeDtypeStruct((8, LANES), F32), flat, land_p, land, land],
        in_specs=[ANY] * 7 + [VMEM_SPEC] * 3,
        out_specs=[ANY, VMEM_SPEC] + [ANY] * 4,
        scratch_shapes=[buf] * 3 + [pltpu.VMEM((2, CHUNKS, RS_ROWS, LANES), F32), pltpu.VMEM((2, 2, CHUNKS, RS_ROWS, LANES), F32), buf, pltpu.VMEM((8, LANES), F32), pltpu.VMEM((NDEV, 8, LANES), F32)]
        + tile_scratch(PACK_SLOTS, PACK_ROWS.values()) + [pltpu.VMEM((PACK_SLOTS, PACK_STAGE, LANES), F32), pltpu.VMEM((TAIL, LANES), F32)]
        + [partner, partner, link, link, DMA((4, 2)), pair, all_devs, all_devs, slots, slots, DMA],
        compiler_params=pltpu.CompilerParams(collective_id=0, has_side_effects=True, vmem_limit_bytes=VMEM_LIMIT),
        cost_estimate=COST,
    )(*grads, *norms)
    return outs[0], outs[1]


def adam_rows(g, m, v, p, norm_row, lr, decay):
    clip = jnp.minimum(1.0, MAX_NORM / (norm_row + CLIP_EPS))
    clipped = clip * g
    new_m = BETA_ONE * m + (1.0 - BETA_ONE) * clipped
    new_v = BETA_TWO * v + (1.0 - BETA_TWO) * clipped * clipped
    adam_dir = (new_m * (1.0 / BIAS_ONE)) / (jnp.sqrt(new_v * (1.0 / BIAS_TWO)) + ADAM_EPS)
    decay_term = jnp.where(decay, WEIGHT_DECAY * p, 0.0)
    return p - lr * (decay_term + adam_dir), new_m, new_v


STATE_ROWS = PIECE
STATE_COUNT = SEG // STATE_ROWS
STATE_LAST = SEG - STATE_COUNT * STATE_ROWS
STATE_SLOTS = 4
SUB = 152


def decay_rows(me, start, rows):
    return lax.broadcasted_iota(jnp.int32, (rows, LANES), 0) + (SEG * me + start) < MATRIX_ROWS


def gather_kernel(g, m, v, p, norm, lr, full, late_a, late_b, gb, mb, vb, pb, new_p, late_p,
                  load_sem, own_sem, late_sem, own_send, own_recv, fwd_send, fwd_recv, p_send, p_recv):
    me, other, dev_x, dev_y, dev_d = neighbours()
    partner = me + other
    barrier = pltpu.get_barrier_semaphore()
    for dev in (partner, dev_x, dev_y):
        pl.semaphore_signal(barrier, inc=1, device_id=(dev,), device_id_type=MESH)
    to = (dev_x, dev_y, partner)
    sources = (me, dev_x, dev_y, dev_d)

    def is_last(h, i):
        return h == 1 and isinstance(i, int) and i == HALF - 1

    def start_row(h, i):
        return PIECE * (PIECES - 1) if is_last(h, i) else PIECE * (HALF * h + i)

    def size(h, i):
        return PIECE_LAST if is_last(h, i) else PIECE

    def rows_of(dev, h, i):
        return full.at[pl.ds(SEG * dev + start_row(h, i), size(h, i)), 0]

    def loads(h, i):
        return loads_at(h, start_row(h, i), size(h, i))

    def loads_at(h, start, rows):
        start = pl.multiple_of(start, 8)
        copies = [pltpu.make_async_copy(g.at[pl.ds(start, rows), 0], gb.at[h, pl.ds(0, rows)], load_sem.at[0, h])]
        for n, (src, buf) in enumerate(((m, mb), (v, vb), (p, pb))):
            copies.append(pltpu.make_async_copy(src.at[pl.ds(start, rows)], buf.at[h, pl.ds(0, rows)], load_sem.at[n + 1, h]))
        return copies

    def own_copy(n, h, i):
        return pltpu.make_async_remote_copy(
            src_ref=new_p.at[h, i, pl.ds(0, size(h, i))], dst_ref=rows_of(me, h, i),
            send_sem=own_send.at[n, h, i], recv_sem=own_recv.at[n, h, i], device_id=(to[n],), device_id_type=MESH)

    def own_store(h, i):
        return pltpu.make_async_copy(new_p.at[h, i, pl.ds(0, size(h, i))], rows_of(me, h, i), own_sem.at[h, i])

    def forward(h, i):
        src = rows_of((dev_y, dev_x)[h], h, i)
        return pltpu.make_async_remote_copy(
            src_ref=src, dst_ref=src, send_sem=fwd_send.at[h, i], recv_sem=fwd_recv.at[h, i],
            device_id=((dev_x, dev_y)[h],), device_id_type=MESH)

    def arrival(n, h, i):
        src = rows_of((dev_x, dev_y, partner)[n], h, i)
        return pltpu.make_async_remote_copy(
            src_ref=src, dst_ref=src, send_sem=own_send.at[n, h, i], recv_sem=own_recv.at[n, h, i],
            device_id=(to[n],), device_id_type=MESH)

    def forward_arrival(h, i):
        src = rows_of(dev_d, h, i)
        return pltpu.make_async_remote_copy(
            src_ref=src, dst_ref=src, send_sem=fwd_send.at[h, i], recv_sem=fwd_recv.at[h, i],
            device_id=((dev_x, dev_y)[h],), device_id_type=MESH)

    def partner_copy(q, h, i):
        src = rows_of(sources[q], h, i)
        return pltpu.make_async_remote_copy(
            src_ref=src, dst_ref=src, send_sem=p_send.at[q - 1, h, i], recv_sem=p_recv.at[q - 1, h, i],
            device_id=(partner,), device_id_type=MESH)

    def partner_arrival(q, h, i):
        src = rows_of(sources[q] + other, h, i)
        return pltpu.make_async_remote_copy(
            src_ref=src, dst_ref=src, send_sem=p_send.at[q - 1, h, i], recv_sem=p_recv.at[q - 1, h, i],
            device_id=(partner,), device_id_type=MESH)

    def each(body):
        @pl.loop(0, HALF - 1)
        def _(i):
            body(i)

        body(HALF - 1)

    norm_row = norm[0:1, :]
    for h in HALVES:
        for copy in loads(h, 0):
            copy.start()
    pl.semaphore_wait(barrier, 3)

    def compute(h, out, first):
        @pl.loop(0, PIECE // SUB)
        def _(s):
            start = pl.multiple_of(s * SUB, 8)
            sub = pl.ds(start, SUB)
            out[sub] = adam_rows(gb[h, sub], mb[h, sub], vb[h, sub], pb[h, sub], norm_row, lr[0], decay_rows(me, first + start, SUB))[0]

    def update(i):
        for h in HALVES:
            for copy in loads(h, i):
                copy.wait()

            compute(h, new_p.at[h, i], start_row(h, i))
            for n in ((1, 0, 2) if h == 0 else (0, 1, 2)):
                own_copy(n, h, i).start()
            own_store(h, i).start()
            if isinstance(i, int):
                continue
            for last in (False, True):
                @pl.when((i == HALF - 2) == last)
                def _():
                    for copy in loads(h, HALF - 1 if last else i + 1):
                        copy.start()

    each(update)

    late_copies = []

    def late_store(src, row, rows, to):
        for out, start in zip((late_a, late_b), LATE_STARTS):
            low, high = max(to, start), min(to + rows, start + LATE_HALF)
            if low < high:
                late_copies.append(pltpu.make_async_copy(src.at[pl.ds(row + low - to, high - low)], out.at[pl.ds(low - start, high - low), 0], late_sem.at[len(late_copies)]))
                late_copies[-1].start()

    late_store(new_p.at[1, HALF - 2], PIECE - 8, 8, 0)
    late_store(new_p.at[1, HALF - 1], 0, 8, LATE_ROWS - 8)
    for j in range(LATE_END - LATE_FIRST):
        first = PIECE * (LATE_FIRST + j)
        for copy in loads_at(j % 2, first, PIECE):
            copy.start()
        for copy in loads_at(j % 2, first, PIECE):
            copy.wait()
        compute(j % 2, late_p.at[j], first)
        late_store(late_p.at[j], 0, PIECE, 8 + PIECE * j)

    def pass_on(i):
        arrival(1, 0, i).wait_recv()
        forward(0, i).start()
        partner_copy(2, 0, i).start()
        arrival(0, 1, i).wait_recv()
        forward(1, i).start()
        partner_copy(1, 1, i).start()
        arrival(0, 0, i).wait_recv()
        partner_copy(1, 0, i).start()
        arrival(1, 1, i).wait_recv()
        partner_copy(2, 1, i).start()

    each(pass_on)

    for copy in late_copies:
        copy.wait()

    def finish_own(i):
        for h in HALVES:
            own_store(h, i).wait()
            arrival(2, h, i).wait_recv()
            for n in range(3):
                own_copy(n, h, i).wait_send()

    each(finish_own)

    def finish(i):
        for h in HALVES:
            forward(h, i).wait_send()
            partner_copy(3, h, i).wait_send()
            partner_arrival(3, h, i).wait_recv()

    def pass_last(i):
        for h in HALVES:
            forward_arrival(h, i).wait_recv()
            partner_copy(3, h, i).start()
            for q in (1, 2):
                partner_copy(q, h, i).wait_send()
                partner_arrival(q, h, i).wait_recv()
        if isinstance(i, int):
            finish(i - 1)
        else:
            pl.when(i > 0)(lambda: finish(i - 1))

    each(pass_last)
    finish(HALF - 1)


def gather_params(g, m, v, p, norm, lr):
    buf = pltpu.VMEM((2, PIECE, LANES), F32)
    pairs = DMA((2, HALF))
    triples = DMA((3, 2, HALF))
    return pl.pallas_call(
        gather_kernel,
        name="gather_params",
        out_shape=[jax.ShapeDtypeStruct((FLAT_ROWS, 1, LANES), F32), jax.ShapeDtypeStruct((LATE_HALF, 1, LANES), F32), jax.ShapeDtypeStruct((LATE_HALF, 1, LANES), F32)],
        in_specs=[ANY] * 4 + [VMEM_SPEC, SMEM_SPEC],
        out_specs=[ANY] * 3,
        scratch_shapes=[buf, buf, buf, buf, pltpu.VMEM((2, HALF, PIECE, LANES), F32), pltpu.VMEM((LATE_END - LATE_FIRST, PIECE, LANES), F32),
                        DMA((4, 2)), pairs, DMA((LATE_END - LATE_FIRST + 4,)), triples, triples, pairs, pairs, triples, triples],
        compiler_params=pltpu.CompilerParams(collective_id=1, has_side_effects=True, vmem_limit_bytes=VMEM_LIMIT),
        cost_estimate=COST,
    )(g, m, v, p, norm, lr)


def state_kernel(g, m, v, p, norm, lr, new_p, new_m, new_v, gb, mb, vb, pb, pn, mn, vn, in_sem, out_sem):
    me = lax.axis_index("dp")
    norm_row = norm[pl.ds(0, 1), :]

    def window(i):
        rows = STATE_LAST if isinstance(i, int) and i == STATE_COUNT else STATE_ROWS
        slot = lax.rem(i, STATE_SLOTS)
        return slot, pl.ds(pl.multiple_of(i * STATE_ROWS, 8), rows), pl.ds(0, rows)

    def loads(i):
        slot, rows, size = window(i)
        pairs = ((g.at[rows, 0], gb), (m.at[rows], mb), (v.at[rows], vb), (p.at[rows], pb))
        return [pltpu.make_async_copy(src, buf.at[slot, size], in_sem.at[n, slot]) for n, (src, buf) in enumerate(pairs)]

    def stores(i):
        slot, rows, size = window(i)
        pairs = ((pn, new_p), (mn, new_m), (vn, new_v))
        return [pltpu.make_async_copy(buf.at[slot, size], dst.at[rows], out_sem.at[n, slot]) for n, (buf, dst) in enumerate(pairs)]

    def run(copies, wait=False):
        for copy in copies:
            copy.wait() if wait else copy.start()

    def compute(i):
        slot = lax.rem(i, STATE_SLOTS)

        @pl.loop(0, STATE_ROWS // SUB)
        def _(s):
            start = pl.multiple_of(s * SUB, 8)
            rows = pl.ds(start, SUB)
            pn[slot, rows], mn[slot, rows], vn[slot, rows] = adam_rows(
                gb[slot, rows], mb[slot, rows], vb[slot, rows], pb[slot, rows], norm_row, lr[0],
                decay_rows(me, i * STATE_ROWS + start, SUB))

    for i in range(STATE_SLOTS):
        run(loads(i))

    @pl.loop(0, STATE_COUNT)
    def _(i):
        run(loads(i), wait=True)

        @pl.when(i >= STATE_SLOTS)
        def _():
            run(stores(i - STATE_SLOTS), wait=True)

        compute(i)
        run(stores(i))

        @pl.when(i + STATE_SLOTS < STATE_COUNT)
        def _():
            run(loads(i + STATE_SLOTS))

        @pl.when(i + STATE_SLOTS == STATE_COUNT)
        def _():
            run(loads(STATE_COUNT))

    run(loads(STATE_COUNT), wait=True)
    run(stores(STATE_COUNT - STATE_SLOTS), wait=True)
    compute(STATE_COUNT)
    run(stores(STATE_COUNT))
    for n in range(STATE_SLOTS):
        run(stores(STATE_COUNT - STATE_SLOTS + 1 + n), wait=True)


def new_state(g, m, v, p, norm, lr):
    return pl.pallas_call(
        state_kernel,
        name="new_state",
        out_shape=[jax.ShapeDtypeStruct((SEG, LANES), F32)] * 3,
        in_specs=[ANY] * 4 + [VMEM_SPEC, SMEM_SPEC],
        out_specs=[ANY] * 3,
        scratch_shapes=[pltpu.VMEM((STATE_SLOTS, STATE_ROWS, LANES), F32)] * 7 + [DMA((4, STATE_SLOTS)), DMA((3, STATE_SLOTS))],
        compiler_params=pltpu.CompilerParams(vmem_limit_bytes=VMEM_LIMIT),
        cost_estimate=COST,
    )(g, m, v, p, norm, lr)


def solution(mesh):
    def local_step(*arrays):
        grads = [a.reshape(r, w * LANES) for a, r, w in zip(arrays[:7], NAMES_ROWS, WIDTHS)]
        norms = [a.reshape(s) for a, s in zip(arrays[7:10], GAINS)]
        master, exp_avg, exp_avg_sq = [a.reshape(SEG, LANES) for a in arrays[10:13]]
        lr = arrays[13].reshape(1)
        g, norm = reduce_grads(grads, norms)
        full, *late = gather_params(g, exp_avg, exp_avg_sq, master, norm, lr)

        def permute(a, bits):
            return lax.ppermute(a, "dp", [(d, d ^ bits) for d in range(NDEV)])

        by_y, by_x = permute(late[0], 4), permute(late[1], 2)
        far_x, far_y = permute(late[0], 2), permute(late[1], 4)
        own = [permute(a, 1) for a in late]
        state = list(new_state(g, exp_avg, exp_avg_sq, master, norm, lr))
        by_y, by_x, full, state[0] = lax.optimization_barrier((by_y, by_x, full, state[0]))
        across = (permute(by_y, 2), permute(by_x, 4))
        from_y, from_x = permute(by_y, 1), permute(by_x, 1)
        wide, down, small = (4, 5), (3, 6), (0, 1, 2)
        params = dict(zip(wide, unpack_early(full, wide, [])))
        far_x, far_y, full, params[4] = lax.optimization_barrier((far_x, far_y, full, params[4]))
        far = permute(far_x, 1), permute(far_y, 1)
        params |= dict(zip(down, unpack_early(full, down, [])))
        full, params[6] = lax.optimization_barrier((full, params[6]))
        rest = list(unpack_early(full, small, GAINS))
        params |= dict(zip(small, rest))
        *across, full, rest[-1] = lax.optimization_barrier((*across, full, rest[-1]))
        from_across = [permute(a, 1) for a in across]
        lates = dict(enumerate([late, own, (far_x, by_x), (far[0], from_x), (by_y, far_y), (from_y, far[1])]))
        params = unpack_late(full, lates, params)
        params = unpack_late(full, {6: across, 7: from_across}, params)
        params = [params[t] for t in TENSORS] + rest[len(small):]
        shapes = SHAPES + GAINS[:2] + [(D,)]
        return tuple([a.reshape(-1) for a in state] + [a.reshape(s) for a, s in zip(params, shapes)] + [norm[0, 0]])

    return jax.shard_map(local_step, mesh=mesh, in_specs=(P("dp"),) * 13 + (P(),), out_specs=(P("dp"),) * 3 + (P(),) * 11, check_vma=False)
```

```python
import functools
import math
import jax
import jax.numpy as jnp
from jax import lax
from jax.experimental import pallas as pl
from jax.experimental.pallas import tpu as pltpu
from jax.sharding import PartitionSpec as P

BETA_ONE = 0.9
BETA_TWO = 0.95
ADAM_EPS = 1e-8
WEIGHT_DECAY = 0.1
MAX_NORM = 1.0
CLIP_EPS = 1e-6
STEP = 4
BIAS_ONE = 1.0 - BETA_ONE ** STEP
BIAS_TWO = 1.0 - BETA_TWO ** STEP

MESH = pl.DeviceIdType.MESH
F32 = jnp.float32
BF16 = jnp.bfloat16
LANES = 128

LAYERS, D, KV, FF = 2, 896, 128, 4864
SHAPES = [(LAYERS, D, D), (LAYERS, D, KV), (LAYERS, D, KV), (LAYERS, D, D), (LAYERS, D, FF), (LAYERS, D, FF), (LAYERS, FF, D)]
GAINS = [(LAYERS, D), (LAYERS, D), (1, D)]
TAIL = 40
HALVES, TENSORS, COLUMNS = range(2), range(7), range(7)
NAMES_ROWS = [math.prod(s[:-1]) for s in SHAPES]
WIDTHS = [s[-1] // LANES for s in SHAPES]
OFFSETS = [sum(r * w for r, w in zip(NAMES_ROWS[:t], WIDTHS[:t])) for t in TENSORS]
BLOCK_ROWS = [448, 1792, 1792, 448, 128, 128, 608]
MATRIX_ROWS = 232960
FLAT_ROWS = 233000
SEG = 29125
NDEV = 8

WIDTH_ORDER = (38, 7, 1)
GROUPS = {38: (16,), 7: (16, 32, 64), 1: (16, 128, 256)}
STAGE_ROWS = max(br * WIDTHS[t] for t, br in enumerate(BLOCK_ROWS))


def split(refs, counts):
    refs = list(refs)
    return [[refs.pop(0) for _ in range(n)] for n in counts]


ANY = pl.BlockSpec(memory_space=pl.ANY)
VMEM_SPEC = pl.BlockSpec(memory_space=pltpu.VMEM)
SMEM_SPEC = pl.BlockSpec(memory_space=pltpu.SMEM)
DMA = pltpu.SemaphoreType.DMA
VMEM_LIMIT = 63 * 1024 * 1024
COST = pl.CostEstimate(flops=2 * 10 ** 8, bytes_accessed=10 ** 8, transcendentals=0)


def tile_scratch(slots, rows):
    return [pltpu.VMEM((slots, r, w * LANES), BF16) for r, w in zip(rows, WIDTH_ORDER)]


def width_slot(width):
    return WIDTH_ORDER.index(width)


def row_group(rows, width):
    return max(g for g in GROUPS[width] if rows % g == 0)


PIECE = 912
PIECES = 32
LATE_FIRST, LATE_END = 25, 31
LATE_ROWS = PIECE * (LATE_END - LATE_FIRST) + 16
PIECE_LAST = SEG - (PIECES - 1) * PIECE
HALF = (PIECES - LATE_END + LATE_FIRST) // 2
LATE_HALF = (LATE_ROWS + 16) // 2
LATE_STARTS = (0, LATE_ROWS - LATE_HALF)
LATE_RANGES = [((SEG * s + PIECE * LATE_FIRST) // 8 * 8, -(-(SEG * s + PIECE * LATE_END) // 8) * 8) for s in range(NDEV)]


def unpack_blocks():
    early, late = [], []
    for t in TENSORS:
        w, offset, total = WIDTHS[t], OFFSETS[t], NAMES_ROWS[t]
        cuts = {0, total}
        spans = []
        for low, high in LATE_RANGES:
            first = max(0, (low - offset) // (16 * w) * 16)
            end = min(total, -(-(high - offset) // (16 * w)) * 16)
            if first < end:
                spans.append((first, end))
                cuts |= {first, end}
        cuts = sorted(cuts)
        for begin, end in zip(cuts[:-1], cuts[1:]):
            is_late = any(first <= begin and end <= last for first, last in spans)
            count = -(-(end - begin) // BLOCK_ROWS[t])
            step = -(-(end - begin) // (16 * count)) * 16
            for row in range(begin, end, step):
                rows = min(step, end - row)
                low, high = offset + row * w, offset + (row + rows) * w
                middles = [l + LATE_STARTS[1] for l, _ in LATE_RANGES]
                edges = sorted({low, high} | {e for r in LATE_RANGES + [middles] for e in r if low < e < high})
                sources = []
                for e0, e1 in zip(edges[:-1], edges[1:]):
                    seg = [s for s, (l, h) in enumerate(LATE_RANGES) if l <= e0 and e1 <= h]
                    source = None
                    start = e0
                    if seg:
                        start = e0 - SEG * seg[0] - PIECE * LATE_FIRST + 8
                        half = int(e0 >= middles[seg[0]])
                        source, start = (seg[0], half), start - LATE_STARTS[half]
                    sources.append((source, start, e0 - low, e1 - e0))
                (late if is_late else early).append((t, row, rows, sources))
    return early, late


EARLY_BLOCKS, LATE_BLOCKS = unpack_blocks()
LATE_TENSORS = sorted({t for t, _, _, _ in LATE_BLOCKS})
SLOTS = 4


def unpack_body(blocks, flat, lates, outs, tiles, stage, in_sem, out_sem, wanted=None):
    def when(b):
        return pl.when(wanted(b)) if wanted else lambda f: f()

    def loads(b, start=True):
        for n, (source, row, to, rows) in enumerate(blocks[b][3]):
            def copy(ref):
                return pltpu.make_async_copy(ref.at[pl.ds(row, rows), 0], stage.at[b % SLOTS, pl.ds(to, rows)], in_sem.at[b % SLOTS, n])

            if not start:
                copy(flat).wait()
            elif source is None:
                copy(flat).start()
            else:
                for relation, halves in lates.items():
                    @pl.when(lax.bitwise_xor(lax.axis_index("dp"), source[0]) == relation)
                    def _():
                        copy(halves[source[1]]).start()

    def store(b):
        t, row, rows, _ = blocks[b]
        return pltpu.make_async_copy(tiles[width_slot(WIDTHS[t])].at[b % SLOTS, pl.ds(0, rows)], outs[t].at[pl.ds(row, rows)], out_sem.at[b % SLOTS])

    for b in range(min(SLOTS, len(blocks))):
        when(b)(lambda: loads(b))
    yield
    for b, (t, row, rows, _) in enumerate(blocks):
        w = WIDTHS[t]
        tile = tiles[width_slot(w)]
        group = row_group(rows, w)
        if b >= SLOTS:
            when(b - SLOTS)(lambda: store(b - SLOTS).wait())

        @when(b)
        def _():
            loads(b, start=False)

            @pl.loop(0, rows // group)
            def _(i):
                for j in range(w):
                    if w == 1:
                        block = stage[b % SLOTS, pl.ds(pl.multiple_of(i * group, 16), group), :]
                    else:
                        block = stage[b % SLOTS, pl.ds(i * (group * w) + j, group, stride=w), :]
                    tile[b % SLOTS, pl.ds(pl.multiple_of(i * group, 16), group), pl.ds(j * LANES, LANES)] = block.astype(BF16)

            store(b).start()

        if b + SLOTS < len(blocks):
            when(b + SLOTS)(lambda: loads(b + SLOTS))
    for b in range(max(0, len(blocks) - SLOTS), len(blocks)):
        when(b)(lambda: store(b).wait())


UNPACK_SCRATCH = tile_scratch(SLOTS, (128, 608, 1792)) + [pltpu.VMEM((SLOTS, STAGE_ROWS, LANES), F32)]
TENSOR_TYPES = [jax.ShapeDtypeStruct((r, w * LANES), BF16) for r, w in zip(NAMES_ROWS, WIDTHS)]


def unpack_early_kernel(tensors, flat, *refs):
    gains = len(refs) - len(tensors) - 8
    outs, norms, tiles, (stage, tail, in_sem, out_sem, tail_sem) = split(refs, (len(tensors), gains, 3, 5))
    tail_copy = pltpu.make_async_copy(flat.at[pl.ds(MATRIX_ROWS, TAIL), 0], tail, tail_sem)
    tail_copy.start()
    work = unpack_body([b for b in EARLY_BLOCKS if b[0] in tensors], flat, None, dict(zip(tensors, outs)), tiles, stage, in_sem, out_sem)
    next(work)
    tail_copy.wait()
    base = 0
    for n in norms:
        if n.ndim == 1:
            n[...] = jnp.concatenate([tail[base + j, :] for j in COLUMNS]).astype(BF16)
            continue
        for j in COLUMNS:
            lines = [tail[pl.ds(base + j + 7 * layer, 1), :] for layer in range(n.shape[0])]
            n[:, pl.ds(j * LANES, LANES)] = jnp.concatenate(lines, axis=0).astype(BF16)
        base += 7 * n.shape[0]
    for _ in work:
        pass


def unpack_early(flat, tensors, gains):
    return pl.pallas_call(
        functools.partial(unpack_early_kernel, tensors),
        name="unpack_early",
        out_shape=[TENSOR_TYPES[t] for t in tensors] + [jax.ShapeDtypeStruct(s, BF16) for s in gains],
        in_specs=[ANY],
        out_specs=[ANY] * len(tensors) + [VMEM_SPEC] * len(gains),
        scratch_shapes=UNPACK_SCRATCH + [pltpu.VMEM((TAIL, LANES), F32), DMA((SLOTS, 4)), DMA((SLOTS,)), DMA],
        compiler_params=pltpu.CompilerParams(vmem_limit_bytes=VMEM_LIMIT),
        cost_estimate=COST,
    )(flat)


def unpack_late_kernel(relations, flat, *refs):
    count = len(LATE_TENSORS)
    lates, _, outs, tiles, (stage, in_sem, out_sem) = split(refs, (2 * len(relations), count, count, 3, 3))
    lates = dict(zip(relations, zip(lates[::2], lates[1::2])))

    def wanted(b):
        seg = [source[0] for source, _, _, _ in LATE_BLOCKS[b][3] if source][0]
        relation = lax.bitwise_xor(lax.axis_index("dp"), seg)
        return jnp.logical_and(relation >= relations[0], relation <= relations[-1])

    for _ in unpack_body(LATE_BLOCKS, flat, lates, dict(zip(LATE_TENSORS, outs)), tiles, stage, in_sem, out_sem, wanted):
        pass


def unpack_late(flat, lates, params):
    count = len(LATE_TENSORS)
    relations = sorted(lates)
    lates = [a for r in relations for a in lates[r]]
    outs = pl.pallas_call(
        functools.partial(unpack_late_kernel, relations),
        name="unpack_late",
        out_shape=[TENSOR_TYPES[t] for t in LATE_TENSORS],
        in_specs=[ANY] * (1 + len(lates) + count),
        out_specs=[ANY] * count,
        input_output_aliases={1 + len(lates) + n: n for n in range(count)},
        scratch_shapes=UNPACK_SCRATCH + [DMA((SLOTS, 4)), DMA((SLOTS,))],
        compiler_params=pltpu.CompilerParams(vmem_limit_bytes=VMEM_LIMIT),
        cost_estimate=COST,
    )(flat, *lates, *[params[t] for t in LATE_TENSORS])
    return {**params, **dict(zip(LATE_TENSORS, outs))}


def neighbours():
    me = lax.axis_index("dp")
    core, x, y = lax.rem(me, 2), lax.rem(me // 2, 2), me // 4
    other = 1 - 2 * core
    step_x, step_y = 2 - 4 * x, 4 - 8 * y
    return me, other, me + step_x, me + step_y, me + step_x + step_y


CHUNKS = 16
RS_ROWS = 911
RS_HALF_START = SEG - CHUNKS * RS_ROWS
UNITS = 4
UNIT_CHUNKS = CHUNKS // UNITS
KIND_D, KIND_N, KIND_S, KIND_O = range(4)
CHIP_D, CHIP_X, CHIP_Y, CHIP_OWN = range(4)
UNIT_ROWS = UNIT_CHUNKS * RS_ROWS
MARGIN = 16 * 38
PACK_ROWS = {38: 112, 7: 608, 1: 896}
PACK_STAGE = 112 * 38
PACK_SLOTS = 3


def pack_blocks(chip, unit):
    blocks = []
    for parity in HALVES:
        for h in HALVES:
            begin = SEG * (2 * chip + parity) + RS_HALF_START * h + UNIT_ROWS * unit
            for t in TENSORS:
                w, offset, total = WIDTHS[t], OFFSETS[t], NAMES_ROWS[t]
                low, high = max(begin, offset), min(begin + UNIT_ROWS, offset + total * w)
                if low >= high:
                    continue
                first = (low - offset) // (16 * w) * 16
                end = -(-(high - offset) // (16 * w)) * 16
                step = -(-(end - first) // (16 * -(-(end - first) // PACK_ROWS[w]))) * 16
                for row in range(first, end, step):
                    blocks.append((t, row, min(step, end - row), parity, h, offset + row * w - begin + MARGIN))
    return blocks


def reduce_kernel(*refs):
    (grads, norms, (g_out, norm_out, flat, land_p, land_d, land_n),
     (mine, part, first, land_s, sums, g_buf, ss, ss_all), tiles, (stage, tail),
     (p_send, p_recv, i_send, i_recv, load_sem, g_sem, ss_send, ss_recv, in_sem, out_sem, tail_sem)) = split(refs, (7, 3, 6, 8, 3, 2, 11))
    me, other, dev_x, dev_y, _ = neighbours()
    core, x, y = lax.rem(me, 2), lax.rem(me // 2, 2), me // 4
    barrier = pltpu.get_barrier_semaphore()
    for d in range(1, NDEV):
        pl.semaphore_signal(barrier, inc=1, device_id=(lax.rem(me + d, NDEV),), device_id_type=MESH)

    tail[...] = jnp.zeros_like(tail)
    line = 0
    for n in norms:
        for layer in range(n.shape[0]):
            for j in COLUMNS:
                tail[pl.ds(line, 1), :] = n[pl.ds(layer, 1), pl.ds(j * LANES, LANES)].astype(F32)
                line += 1

    def pack(place, chip, unit):
        blocks = pack_blocks(chip, unit)

        def load(b):
            t, row, rows = blocks[b][:3]
            return pltpu.make_async_copy(grads[t].at[pl.ds(row, rows)], tiles[width_slot(WIDTHS[t])].at[b % PACK_SLOTS, pl.ds(0, rows)], in_sem.at[b % PACK_SLOTS])

        def store(b):
            t, _, rows, parity, h, to = blocks[b]
            size = rows * WIDTHS[t]
            return pltpu.make_async_copy(stage.at[b % PACK_SLOTS, pl.ds(0, size)], flat.at[place, unit, parity, h, pl.ds(to, size), 0], out_sem.at[b % PACK_SLOTS])

        for b in range(PACK_SLOTS):
            load(b).start()
        tail_copies = [pltpu.make_async_copy(tail, flat.at[place, unit, 1, 1, pl.ds(MARGIN + UNIT_ROWS - TAIL, TAIL), 0], tail_sem)
                       for _ in range(chip * unit // (3 * UNITS - 3))]
        for copy in tail_copies:
            copy.start()
        for b, block in enumerate(blocks):
            t, rows = block[0], block[2]
            w = WIDTHS[t]
            tile = tiles[width_slot(w)]
            group = row_group(rows, w)
            load(b).wait()
            if b >= PACK_SLOTS:
                store(b - PACK_SLOTS).wait()

            @pl.loop(0, rows // group)
            def _(i):
                for j in range(w):
                    values = tile[b % PACK_SLOTS, pl.ds(pl.multiple_of(i * group, 16), group), pl.ds(j * LANES, LANES)].astype(F32)
                    if w == 1:
                        stage[b % PACK_SLOTS, pl.ds(pl.multiple_of(i * group, 16), group), :] = values
                    else:
                        stage[b % PACK_SLOTS, pl.ds(i * (group * w) + j, group, stride=w), :] = values

            store(b).start()
            if b + PACK_SLOTS < len(blocks):
                load(b + PACK_SLOTS).start()
        for b in range(len(blocks) - PACK_SLOTS, len(blocks)):
            store(b).wait()
        for copy in tail_copies:
            copy.wait()

    def place_of(kind, h):
        return ((CHIP_D, CHIP_D), (CHIP_X, CHIP_Y), (CHIP_Y, CHIP_X), (CHIP_OWN, CHIP_OWN))[kind][h]

    def chunk(kind, h, i, parity):
        return flat.at[place_of(kind, h), i // UNIT_CHUNKS, parity, h, pl.ds(MARGIN + RS_ROWS * lax.rem(i, UNIT_CHUNKS), RS_ROWS)]

    def start_row(h, i):
        return RS_HALF_START * h + RS_ROWS * i

    def partner_copy(kind, h, i):
        return pltpu.make_async_remote_copy(
            src_ref=chunk(kind, h, i, 1 - core), dst_ref=land_p.at[kind, h, i],
            send_sem=p_send.at[kind, h, i], recv_sem=p_recv.at[kind, h, i],
            device_id=(me + other,), device_id_type=MESH)

    def link_copy(kind, h, i):
        land = land_s.at[h, i] if kind == KIND_S else (land_d, land_n)[kind].at[h, i, pl.ds(0, RS_ROWS), 0]
        to = ((dev_x, dev_y), (dev_x, dev_y), (dev_y, dev_x))[kind][h]
        return pltpu.make_async_remote_copy(
            src_ref=sums.at[kind % 2, h, i], dst_ref=land,
            send_sem=i_send.at[kind, h, i], recv_sem=i_recv.at[kind, h, i],
            device_id=(to,), device_id_type=MESH)

    def load_mine(kind, h, i):
        return pltpu.make_async_copy(chunk(kind, h, i, core).at[:, 0], mine.at[h], load_sem.at[0, h])

    def load_part(kind, h, i):
        return pltpu.make_async_copy(land_p.at[kind, h, i, pl.ds(0, RS_ROWS), 0], part.at[h], load_sem.at[1, h])

    def load_link(land, buf, n, h, i):
        return pltpu.make_async_copy(land.at[h, i, pl.ds(0, RS_ROWS), 0], buf.at[h], load_sem.at[n, h])

    def store_g(h, i):
        return pltpu.make_async_copy(g_buf.at[h], g_out.at[pl.ds(start_row(h, i), RS_ROWS), 0], g_sem.at[h])

    def exchange(kinds, begin, end):
        @pl.loop(begin, end)
        def _(i):
            for kind in kinds:
                for h in HALVES:
                    partner_copy(kind, h, i).start()

    def send(kind, begin, end):
        @pl.loop(begin, end)
        def _(i):
            for h in HALVES:
                load_mine(kind, h, i).start()
            for h in HALVES:
                partner_copy(kind, h, i).wait_recv()
                load_part(kind, h, i).start()
                if kind == KIND_S:
                    link_copy(KIND_D, h, i).wait_recv()
                    load_link(land_d, first, 2, h, i).start()
            for h in HALVES:
                load_mine(kind, h, i).wait()
                load_part(kind, h, i).wait()
                total = mine[h] + part[h]
                if kind == KIND_S:
                    load_link(land_d, first, 2, h, i).wait()
                    total = total + first[h]
                    link_copy(KIND_D, h, i).wait_send()
                sums[kind % 2, h, i] = total
                link_copy(kind, h, i).start()

    @pl.loop(0, 4 * UNITS)
    def _(n):
        place, unit = n // UNITS, lax.rem(n, UNITS)
        flip_x, flip_y = 1 - place // 2, 1 - lax.rem(place, 2)
        chip = (x + flip_x * (1 - 2 * x)) + 2 * (y + flip_y * (1 - 2 * y))
        for case in range(4 * UNITS):
            @pl.when(UNITS * chip + unit == case)
            def _():
                pack(place, case // UNITS, case % UNITS)

        @pl.when(n == 0)
        def _():
            pl.semaphore_wait(barrier, NDEV - 1)

        @pl.when(n < UNITS)
        def _():
            exchange((KIND_D,), UNIT_CHUNKS * unit, UNIT_CHUNKS * unit + UNIT_CHUNKS)
            send(KIND_D, UNIT_CHUNKS * unit, UNIT_CHUNKS * unit + UNIT_CHUNKS)

        @pl.when(n == 3 * UNITS - 1)
        def _():
            exchange((KIND_N, KIND_S), 0, CHUNKS)
            send(KIND_N, 0, CHUNKS)

    exchange((KIND_O,), 0, CHUNKS)
    send(KIND_S, 0, CHUNKS)

    def last(i, acc):
        for h in HALVES:
            for kind in (KIND_D, KIND_N, KIND_S):
                partner_copy(kind, h, i).wait_send()
            link_copy(KIND_N, h, i).wait_send()

            @pl.when(i > 0)
            def _():
                partner_copy(KIND_O, h, i - 1).wait_send()
                link_copy(KIND_S, h, i - 1).wait_send()

        for h in HALVES:
            load_mine(KIND_O, h, i).start()
            partner_copy(KIND_O, h, i).wait_recv()
            load_part(KIND_O, h, i).start()
        for h in HALVES:
            link_copy(KIND_N, h, i).wait_recv()
            load_link(land_n, first, 2, h, i).start()
        for h in HALVES:
            load_mine(KIND_O, h, i).wait()
            load_part(KIND_O, h, i).wait()
            load_link(land_n, first, 2, h, i).wait()
            link_copy(KIND_S, h, i).wait_recv()

            @pl.when(i > 0)
            def _():
                store_g(h, i - 1).wait()

            g = ((mine[h] + part[h]) + (first[h] + land_s[h, i])) * (1.0 / NDEV)
            g_buf[h] = g
            store_g(h, i).start()
            square = g * g
            if h == 1:
                row = lax.broadcasted_iota(jnp.int32, (RS_ROWS, LANES), 0) + RS_ROWS * i
                square = jnp.where(row >= CHUNKS * RS_ROWS - RS_HALF_START, square, 0.0)
            acc = acc + jnp.sum(square, axis=0, keepdims=True)
        return acc

    acc = lax.fori_loop(0, CHUNKS, last, jnp.zeros((1, LANES), F32))
    ss[...] = jnp.broadcast_to(acc, (8, LANES))

    for h in HALVES:
        partner_copy(KIND_O, h, CHUNKS - 1).wait_send()
        link_copy(KIND_S, h, CHUNKS - 1).wait_send()
    store_g(0, CHUNKS - 1).wait()

    def norm_copy(d):
        return pltpu.make_async_remote_copy(
            src_ref=ss, dst_ref=ss_all.at[d], send_sem=ss_send.at[d], recv_sem=ss_recv.at[d],
            device_id=(lax.rem(me + d, NDEV),), device_id_type=MESH)

    for d in range(1, NDEV):
        norm_copy(d).start()
    store_g(1, CHUNKS - 1).wait()
    ss_all[0] = ss[...]
    for d in range(1, NDEV):
        norm_copy(d).wait()
    total = jnp.zeros((8, LANES), F32)
    for dev in range(NDEV):
        total = total + ss_all[lax.rem(me - dev + NDEV, NDEV)]
    norm_out[...] = jnp.broadcast_to(jnp.sqrt(jnp.sum(total, axis=1, keepdims=True)), (8, LANES))


def reduce_grads(grads, norms):
    land = jax.ShapeDtypeStruct((2, CHUNKS, RS_ROWS, 1, LANES), F32)
    land_p = jax.ShapeDtypeStruct((4, 2, CHUNKS, RS_ROWS, 1, LANES), F32)
    flat = jax.ShapeDtypeStruct((4, UNITS, 2, 2, UNIT_ROWS + 2 * MARGIN, 1, LANES), F32)
    buf = pltpu.VMEM((2, RS_ROWS, LANES), F32)
    partner, link, pair, all_devs, slots = DMA((4, 2, CHUNKS)), DMA((3, 2, CHUNKS)), DMA((2,)), DMA((NDEV,)), DMA((PACK_SLOTS,))
    outs = pl.pallas_call(
        reduce_kernel,
        name="reduce_grads",
        out_shape=[jax.ShapeDtypeStruct((SEG, 1, LANES), F32), jax.ShapeDtypeStruct((8, LANES), F32), flat, land_p, land, land],
        in_specs=[ANY] * 7 + [VMEM_SPEC] * 3,
        out_specs=[ANY, VMEM_SPEC] + [ANY] * 4,
        scratch_shapes=[buf] * 3 + [pltpu.VMEM((2, CHUNKS, RS_ROWS, LANES), F32), pltpu.VMEM((2, 2, CHUNKS, RS_ROWS, LANES), F32), buf, pltpu.VMEM((8, LANES), F32), pltpu.VMEM((NDEV, 8, LANES), F32)]
        + tile_scratch(PACK_SLOTS, PACK_ROWS.values()) + [pltpu.VMEM((PACK_SLOTS, PACK_STAGE, LANES), F32), pltpu.VMEM((TAIL, LANES), F32)]
        + [partner, partner, link, link, DMA((4, 2)), pair, all_devs, all_devs, slots, slots, DMA],
        compiler_params=pltpu.CompilerParams(collective_id=0, has_side_effects=True, vmem_limit_bytes=VMEM_LIMIT),
        cost_estimate=COST,
    )(*grads, *norms)
    return outs[0], outs[1]


def adam_rows(g, m, v, p, norm_row, lr, decay):
    clip = jnp.minimum(1.0, MAX_NORM / (norm_row + CLIP_EPS))
    clipped = clip * g
    new_m = BETA_ONE * m + (1.0 - BETA_ONE) * clipped
    new_v = BETA_TWO * v + (1.0 - BETA_TWO) * clipped * clipped
    adam_dir = (new_m * (1.0 / BIAS_ONE)) / (jnp.sqrt(new_v * (1.0 / BIAS_TWO)) + ADAM_EPS)
    decay_term = jnp.where(decay, WEIGHT_DECAY * p, 0.0)
    return p - lr * (decay_term + adam_dir), new_m, new_v


STATE_ROWS = PIECE
STATE_COUNT = SEG // STATE_ROWS
STATE_LAST = SEG - STATE_COUNT * STATE_ROWS
STATE_SLOTS = 4
SUB = 152


def decay_rows(me, start, rows):
    return lax.broadcasted_iota(jnp.int32, (rows, LANES), 0) + (SEG * me + start) < MATRIX_ROWS


def gather_kernel(g, m, v, p, norm, lr, full, late_a, late_b, gb, mb, vb, pb, new_p, late_p,
                  load_sem, own_sem, late_sem, own_send, own_recv, fwd_send, fwd_recv, p_send, p_recv):
    me, other, dev_x, dev_y, dev_d = neighbours()
    partner = me + other
    barrier = pltpu.get_barrier_semaphore()
    for dev in (partner, dev_x, dev_y):
        pl.semaphore_signal(barrier, inc=1, device_id=(dev,), device_id_type=MESH)
    to = (dev_x, dev_y, partner)
    sources = (me, dev_x, dev_y, dev_d)

    def is_last(h, i):
        return h == 1 and isinstance(i, int) and i == HALF - 1

    def start_row(h, i):
        return PIECE * (PIECES - 1) if is_last(h, i) else PIECE * (HALF * h + i)

    def size(h, i):
        return PIECE_LAST if is_last(h, i) else PIECE

    def rows_of(dev, h, i):
        return full.at[pl.ds(SEG * dev + start_row(h, i), size(h, i)), 0]

    def loads(h, i):
        return loads_at(h, start_row(h, i), size(h, i))

    def loads_at(h, start, rows):
        start = pl.multiple_of(start, 8)
        copies = [pltpu.make_async_copy(g.at[pl.ds(start, rows), 0], gb.at[h, pl.ds(0, rows)], load_sem.at[0, h])]
        for n, (src, buf) in enumerate(((m, mb), (v, vb), (p, pb))):
            copies.append(pltpu.make_async_copy(src.at[pl.ds(start, rows)], buf.at[h, pl.ds(0, rows)], load_sem.at[n + 1, h]))
        return copies

    def own_copy(n, h, i):
        return pltpu.make_async_remote_copy(
            src_ref=new_p.at[h, i, pl.ds(0, size(h, i))], dst_ref=rows_of(me, h, i),
            send_sem=own_send.at[n, h, i], recv_sem=own_recv.at[n, h, i], device_id=(to[n],), device_id_type=MESH)

    def own_store(h, i):
        return pltpu.make_async_copy(new_p.at[h, i, pl.ds(0, size(h, i))], rows_of(me, h, i), own_sem.at[h, i])

    def forward(h, i):
        src = rows_of((dev_y, dev_x)[h], h, i)
        return pltpu.make_async_remote_copy(
            src_ref=src, dst_ref=src, send_sem=fwd_send.at[h, i], recv_sem=fwd_recv.at[h, i],
            device_id=((dev_x, dev_y)[h],), device_id_type=MESH)

    def arrival(n, h, i):
        src = rows_of((dev_x, dev_y, partner)[n], h, i)
        return pltpu.make_async_remote_copy(
            src_ref=src, dst_ref=src, send_sem=own_send.at[n, h, i], recv_sem=own_recv.at[n, h, i],
            device_id=(to[n],), device_id_type=MESH)

    def forward_arrival(h, i):
        src = rows_of(dev_d, h, i)
        return pltpu.make_async_remote_copy(
            src_ref=src, dst_ref=src, send_sem=fwd_send.at[h, i], recv_sem=fwd_recv.at[h, i],
            device_id=((dev_x, dev_y)[h],), device_id_type=MESH)

    def partner_copy(q, h, i):
        src = rows_of(sources[q], h, i)
        return pltpu.make_async_remote_copy(
            src_ref=src, dst_ref=src, send_sem=p_send.at[q - 1, h, i], recv_sem=p_recv.at[q - 1, h, i],
            device_id=(partner,), device_id_type=MESH)

    def partner_arrival(q, h, i):
        src = rows_of(sources[q] + other, h, i)
        return pltpu.make_async_remote_copy(
            src_ref=src, dst_ref=src, send_sem=p_send.at[q - 1, h, i], recv_sem=p_recv.at[q - 1, h, i],
            device_id=(partner,), device_id_type=MESH)

    def each(body):
        @pl.loop(0, HALF - 1)
        def _(i):
            body(i)

        body(HALF - 1)

    norm_row = norm[0:1, :]
    for h in HALVES:
        for copy in loads(h, 0):
            copy.start()
    pl.semaphore_wait(barrier, 3)

    def compute(h, out, first):
        @pl.loop(0, PIECE // SUB)
        def _(s):
            start = pl.multiple_of(s * SUB, 8)
            sub = pl.ds(start, SUB)
            out[sub] = adam_rows(gb[h, sub], mb[h, sub], vb[h, sub], pb[h, sub], norm_row, lr[0], decay_rows(me, first + start, SUB))[0]

    def update(i):
        for h in HALVES:
            for copy in loads(h, i):
                copy.wait()

            compute(h, new_p.at[h, i], start_row(h, i))
            for n in ((1, 0, 2) if h == 0 else (0, 1, 2)):
                own_copy(n, h, i).start()
            own_store(h, i).start()
            if isinstance(i, int):
                continue
            for last in (False, True):
                @pl.when((i == HALF - 2) == last)
                def _():
                    for copy in loads(h, HALF - 1 if last else i + 1):
                        copy.start()

    each(update)

    late_copies = []

    def late_store(src, row, rows, to):
        for out, start in zip((late_a, late_b), LATE_STARTS):
            low, high = max(to, start), min(to + rows, start + LATE_HALF)
            if low < high:
                late_copies.append(pltpu.make_async_copy(src.at[pl.ds(row + low - to, high - low)], out.at[pl.ds(low - start, high - low), 0], late_sem.at[len(late_copies)]))
                late_copies[-1].start()

    late_store(new_p.at[1, HALF - 2], PIECE - 8, 8, 0)
    late_store(new_p.at[1, HALF - 1], 0, 8, LATE_ROWS - 8)
    for j in range(LATE_END - LATE_FIRST):
        first = PIECE * (LATE_FIRST + j)
        for copy in loads_at(j % 2, first, PIECE):
            copy.start()
        for copy in loads_at(j % 2, first, PIECE):
            copy.wait()
        compute(j % 2, late_p.at[j], first)
        late_store(late_p.at[j], 0, PIECE, 8 + PIECE * j)

    def pass_on(i):
        arrival(1, 0, i).wait_recv()
        forward(0, i).start()
        partner_copy(2, 0, i).start()
        arrival(0, 1, i).wait_recv()
        forward(1, i).start()
        partner_copy(1, 1, i).start()
        arrival(0, 0, i).wait_recv()
        partner_copy(1, 0, i).start()
        arrival(1, 1, i).wait_recv()
        partner_copy(2, 1, i).start()

    each(pass_on)

    for copy in late_copies:
        copy.wait()

    def finish_own(i):
        for h in HALVES:
            own_store(h, i).wait()
            arrival(2, h, i).wait_recv()
            for n in range(3):
                own_copy(n, h, i).wait_send()

    each(finish_own)

    def finish(i):
        for h in HALVES:
            forward(h, i).wait_send()
            partner_copy(3, h, i).wait_send()
            partner_arrival(3, h, i).wait_recv()

    def pass_last(i):
        for h in HALVES:
            forward_arrival(h, i).wait_recv()
            partner_copy(3, h, i).start()
            for q in (1, 2):
                partner_copy(q, h, i).wait_send()
                partner_arrival(q, h, i).wait_recv()
        if isinstance(i, int):
            finish(i - 1)
        else:
            pl.when(i > 0)(lambda: finish(i - 1))

    each(pass_last)
    finish(HALF - 1)


def gather_params(g, m, v, p, norm, lr):
    buf = pltpu.VMEM((2, PIECE, LANES), F32)
    pairs = DMA((2, HALF))
    triples = DMA((3, 2, HALF))
    return pl.pallas_call(
        gather_kernel,
        name="gather_params",
        out_shape=[jax.ShapeDtypeStruct((FLAT_ROWS, 1, LANES), F32), jax.ShapeDtypeStruct((LATE_HALF, 1, LANES), F32), jax.ShapeDtypeStruct((LATE_HALF, 1, LANES), F32)],
        in_specs=[ANY] * 4 + [VMEM_SPEC, SMEM_SPEC],
        out_specs=[ANY] * 3,
        scratch_shapes=[buf, buf, buf, buf, pltpu.VMEM((2, HALF, PIECE, LANES), F32), pltpu.VMEM((LATE_END - LATE_FIRST, PIECE, LANES), F32),
                        DMA((4, 2)), pairs, DMA((LATE_END - LATE_FIRST + 4,)), triples, triples, pairs, pairs, triples, triples],
        compiler_params=pltpu.CompilerParams(collective_id=1, has_side_effects=True, vmem_limit_bytes=VMEM_LIMIT),
        cost_estimate=COST,
    )(g, m, v, p, norm, lr)


def state_kernel(g, m, v, p, norm, lr, new_p, new_m, new_v, norm_out, gb, mb, vb, pb, pn, mn, vn, in_sem, out_sem):
    me = lax.axis_index("dp")
    norm_row = norm[pl.ds(0, 1), :]
    norm_out[0] = jnp.max(norm[...])

    def window(i):
        rows = STATE_LAST if isinstance(i, int) and i == STATE_COUNT else STATE_ROWS
        slot = lax.rem(i, STATE_SLOTS)
        return slot, pl.ds(pl.multiple_of(i * STATE_ROWS, 8), rows), pl.ds(0, rows)

    def loads(i):
        slot, rows, size = window(i)
        pairs = ((g.at[rows, 0], gb), (m.at[rows], mb), (v.at[rows], vb), (p.at[rows], pb))
        return [pltpu.make_async_copy(src, buf.at[slot, size], in_sem.at[n, slot]) for n, (src, buf) in enumerate(pairs)]

    def stores(i):
        slot, rows, size = window(i)
        pairs = ((pn, new_p), (mn, new_m), (vn, new_v))
        return [pltpu.make_async_copy(buf.at[slot, size], dst.at[rows], out_sem.at[n, slot]) for n, (buf, dst) in enumerate(pairs)]

    def run(copies, wait=False):
        for copy in copies:
            copy.wait() if wait else copy.start()

    def compute(i):
        slot = lax.rem(i, STATE_SLOTS)

        @pl.loop(0, STATE_ROWS // SUB)
        def _(s):
            start = pl.multiple_of(s * SUB, 8)
            rows = pl.ds(start, SUB)
            pn[slot, rows], mn[slot, rows], vn[slot, rows] = adam_rows(
                gb[slot, rows], mb[slot, rows], vb[slot, rows], pb[slot, rows], norm_row, lr[0],
                decay_rows(me, i * STATE_ROWS + start, SUB))

    for i in range(STATE_SLOTS):
        run(loads(i))

    @pl.loop(0, STATE_COUNT)
    def _(i):
        run(loads(i), wait=True)

        @pl.when(i >= STATE_SLOTS)
        def _():
            run(stores(i - STATE_SLOTS), wait=True)

        compute(i)
        run(stores(i))

        @pl.when(i + STATE_SLOTS < STATE_COUNT)
        def _():
            run(loads(i + STATE_SLOTS))

        @pl.when(i + STATE_SLOTS == STATE_COUNT)
        def _():
            run(loads(STATE_COUNT))

    run(loads(STATE_COUNT), wait=True)
    run(stores(STATE_COUNT - STATE_SLOTS), wait=True)
    compute(STATE_COUNT)
    run(stores(STATE_COUNT))
    for n in range(STATE_SLOTS):
        run(stores(STATE_COUNT - STATE_SLOTS + 1 + n), wait=True)


def new_state(g, m, v, p, norm, lr):
    return pl.pallas_call(
        state_kernel,
        name="new_state",
        out_shape=[jax.ShapeDtypeStruct((SEG, LANES), F32)] * 3 + [jax.ShapeDtypeStruct((1,), F32)],
        in_specs=[ANY] * 4 + [VMEM_SPEC, SMEM_SPEC],
        out_specs=[ANY] * 3 + [SMEM_SPEC],
        scratch_shapes=[pltpu.VMEM((STATE_SLOTS, STATE_ROWS, LANES), F32)] * 7 + [DMA((4, STATE_SLOTS)), DMA((3, STATE_SLOTS))],
        compiler_params=pltpu.CompilerParams(vmem_limit_bytes=VMEM_LIMIT),
        cost_estimate=COST,
    )(g, m, v, p, norm, lr)


def solution(mesh):
    def local_step(*arrays):
        grads = [a.reshape(r, w * LANES) for a, r, w in zip(arrays[:7], NAMES_ROWS, WIDTHS)]
        norms = [a.reshape(s) for a, s in zip(arrays[7:10], GAINS)]
        master, exp_avg, exp_avg_sq = [a.reshape(SEG, LANES) for a in arrays[10:13]]
        lr = arrays[13].reshape(1)
        g, norm = reduce_grads(grads, norms)
        full, *late = gather_params(g, exp_avg, exp_avg_sq, master, norm, lr)

        def permute(a, bits):
            return lax.ppermute(a, "dp", [(d, d ^ bits) for d in range(NDEV)])

        by_y, by_x = permute(late[0], 4), permute(late[1], 2)
        far_x, far_y = permute(late[0], 2), permute(late[1], 4)
        own = [permute(a, 1) for a in late]
        state = list(new_state(g, exp_avg, exp_avg_sq, master, norm, lr))
        by_y, by_x, full, state[0] = lax.optimization_barrier((by_y, by_x, full, state[0]))
        across_y = permute(by_y, 2)
        across_x = permute(by_x, 4)
        across = across_y, across_x
        from_y, from_x = permute(by_y, 1), permute(by_x, 1)
        wide, down, small = (4, 5), (3, 6), (0, 1, 2)
        params = dict(zip(wide, unpack_early(full, wide, [])))
        far_x, far_y, full, params[4] = lax.optimization_barrier((far_x, far_y, full, params[4]))
        far = permute(far_x, 1), permute(far_y, 1)
        params |= dict(zip(down, unpack_early(full, down, [])))
        lates = dict(enumerate([late, own, (far_x, by_x), (far[0], from_x), (by_y, far_y), (from_y, far[1])]))
        params = unpack_late(full, lates, params)
        *across, full, params[6] = lax.optimization_barrier((*across, full, params[6]))
        from_across = [permute(a, 1) for a in across]
        rest = list(unpack_early(full, small, GAINS[:2] + [(D,)]))
        params |= dict(zip(small, rest))
        params = unpack_late(full, {6: across, 7: from_across}, params)
        params = [params[t] for t in TENSORS] + rest[len(small):]
        shapes = SHAPES + GAINS[:2] + [(D,)]
        return tuple([a.reshape(-1) for a in state[:3]] + [a.reshape(s) for a, s in zip(params, shapes)] + [state[3].reshape(())])

    return jax.shard_map(local_step, mesh=mesh, in_specs=(P("dp"),) * 13 + (P(),), out_specs=(P("dp"),) * 3 + (P(),) * 11, check_vma=False)
```

```python
import functools
import math
import jax
import jax.numpy as jnp
from jax import lax
from jax.experimental import pallas as pl
from jax.experimental.pallas import tpu as pltpu
from jax.sharding import PartitionSpec as P

BETA_ONE = 0.9
BETA_TWO = 0.95
ADAM_EPS = 1e-8
WEIGHT_DECAY = 0.1
MAX_NORM = 1.0
CLIP_EPS = 1e-6
STEP = 4
BIAS_ONE = 1.0 - BETA_ONE ** STEP
BIAS_TWO = 1.0 - BETA_TWO ** STEP

MESH = pl.DeviceIdType.MESH
F32 = jnp.float32
BF16 = jnp.bfloat16
LANES = 128

LAYERS, D, KV, FF = 2, 896, 128, 4864
SHAPES = [(LAYERS, D, D), (LAYERS, D, KV), (LAYERS, D, KV), (LAYERS, D, D), (LAYERS, D, FF), (LAYERS, D, FF), (LAYERS, FF, D)]
GAINS = [(LAYERS, D), (LAYERS, D), (1, D)]
TAIL = 40
HALVES, TENSORS, COLUMNS = range(2), range(7), range(7)
NAMES_ROWS = [math.prod(s[:-1]) for s in SHAPES]
WIDTHS = [s[-1] // LANES for s in SHAPES]
OFFSETS = [sum(r * w for r, w in zip(NAMES_ROWS[:t], WIDTHS[:t])) for t in TENSORS]
BLOCK_ROWS = [448, 1792, 1792, 448, 128, 128, 608]
MATRIX_ROWS = 232960
FLAT_ROWS = 233000
SEG = 29125
NDEV = 8

WIDTH_ORDER = (38, 7, 1)
GROUPS = {38: (16,), 7: (16, 32, 64), 1: (16, 128, 256)}
STAGE_ROWS = max(br * WIDTHS[t] for t, br in enumerate(BLOCK_ROWS))


def split(refs, counts):
    refs = list(refs)
    return [[refs.pop(0) for _ in range(n)] for n in counts]


ANY = pl.BlockSpec(memory_space=pl.ANY)
VMEM_SPEC = pl.BlockSpec(memory_space=pltpu.VMEM)
SMEM_SPEC = pl.BlockSpec(memory_space=pltpu.SMEM)
DMA = pltpu.SemaphoreType.DMA
VMEM_LIMIT = 63 * 1024 * 1024
COST = pl.CostEstimate(flops=2 * 10 ** 8, bytes_accessed=10 ** 8, transcendentals=0)


def tile_scratch(slots, rows):
    return [pltpu.VMEM((slots, r, w * LANES), BF16) for r, w in zip(rows, WIDTH_ORDER)]


def width_slot(width):
    return WIDTH_ORDER.index(width)


def row_group(rows, width):
    return max(g for g in GROUPS[width] if rows % g == 0)


PIECE = 608
PIECES = 48
LATE_FIRST, LATE_END = 37, 47
LATE_ROWS = PIECE * (LATE_END - LATE_FIRST) + 16
PIECE_LAST = SEG - (PIECES - 1) * PIECE
HALF = (PIECES - LATE_END + LATE_FIRST) // 2
LATE_HALF = (LATE_ROWS + 16) // 2
LATE_STARTS = (0, LATE_ROWS - LATE_HALF)
LATE_RANGES = [((SEG * s + PIECE * LATE_FIRST) // 8 * 8, -(-(SEG * s + PIECE * LATE_END) // 8) * 8) for s in range(NDEV)]


def unpack_blocks():
    early, late = [], []
    for t in TENSORS:
        w, offset, total = WIDTHS[t], OFFSETS[t], NAMES_ROWS[t]
        cuts = {0, total}
        spans = []
        for low, high in LATE_RANGES:
            first = max(0, (low - offset) // (16 * w) * 16)
            end = min(total, -(-(high - offset) // (16 * w)) * 16)
            if first < end:
                spans.append((first, end))
                cuts |= {first, end}
        cuts = sorted(cuts)
        for begin, end in zip(cuts[:-1], cuts[1:]):
            is_late = any(first <= begin and end <= last for first, last in spans)
            count = -(-(end - begin) // BLOCK_ROWS[t])
            step = -(-(end - begin) // (16 * count)) * 16
            for row in range(begin, end, step):
                rows = min(step, end - row)
                low, high = offset + row * w, offset + (row + rows) * w
                middles = [l + LATE_STARTS[1] for l, _ in LATE_RANGES]
                edges = sorted({low, high} | {e for r in LATE_RANGES + [middles] for e in r if low < e < high})
                sources = []
                for e0, e1 in zip(edges[:-1], edges[1:]):
                    seg = [s for s, (l, h) in enumerate(LATE_RANGES) if l <= e0 and e1 <= h]
                    source = None
                    start = e0
                    if seg:
                        start = e0 - SEG * seg[0] - PIECE * LATE_FIRST + 8
                        half = int(e0 >= middles[seg[0]])
                        source, start = (seg[0], half), start - LATE_STARTS[half]
                    sources.append((source, start, e0 - low, e1 - e0))
                (late if is_late else early).append((t, row, rows, sources))
    return early, late


EARLY_BLOCKS, LATE_BLOCKS = unpack_blocks()
LATE_TENSORS = sorted({t for t, _, _, _ in LATE_BLOCKS})
SLOTS = 4


def unpack_body(blocks, flat, lates, outs, tiles, stage, in_sem, out_sem, wanted=None):
    def when(b):
        return pl.when(wanted(b)) if wanted else lambda f: f()

    def loads(b, start=True):
        for n, (source, row, to, rows) in enumerate(blocks[b][3]):
            def copy(ref):
                return pltpu.make_async_copy(ref.at[pl.ds(row, rows), 0], stage.at[b % SLOTS, pl.ds(to, rows)], in_sem.at[b % SLOTS, n])

            if not start:
                copy(flat).wait()
            elif source is None:
                copy(flat).start()
            else:
                for relation, halves in lates.items():
                    @pl.when(lax.bitwise_xor(lax.axis_index("dp"), source[0]) == relation)
                    def _():
                        copy(halves[source[1]]).start()

    def store(b):
        t, row, rows, _ = blocks[b]
        return pltpu.make_async_copy(tiles[width_slot(WIDTHS[t])].at[b % SLOTS, pl.ds(0, rows)], outs[t].at[pl.ds(row, rows)], out_sem.at[b % SLOTS])

    for b in range(min(SLOTS, len(blocks))):
        when(b)(lambda: loads(b))
    yield
    for b, (t, row, rows, _) in enumerate(blocks):
        w = WIDTHS[t]
        tile = tiles[width_slot(w)]
        group = row_group(rows, w)
        if b >= SLOTS:
            when(b - SLOTS)(lambda: store(b - SLOTS).wait())

        @when(b)
        def _():
            loads(b, start=False)

            @pl.loop(0, rows // group)
            def _(i):
                for j in range(w):
                    if w == 1:
                        block = stage[b % SLOTS, pl.ds(pl.multiple_of(i * group, 16), group), :]
                    else:
                        block = stage[b % SLOTS, pl.ds(i * (group * w) + j, group, stride=w), :]
                    tile[b % SLOTS, pl.ds(pl.multiple_of(i * group, 16), group), pl.ds(j * LANES, LANES)] = block.astype(BF16)

            store(b).start()

        if b + SLOTS < len(blocks):
            when(b + SLOTS)(lambda: loads(b + SLOTS))
    for b in range(max(0, len(blocks) - SLOTS), len(blocks)):
        when(b)(lambda: store(b).wait())


UNPACK_SCRATCH = tile_scratch(SLOTS, (128, 608, 1792)) + [pltpu.VMEM((SLOTS, STAGE_ROWS, LANES), F32)]
TENSOR_TYPES = [jax.ShapeDtypeStruct((r, w * LANES), BF16) for r, w in zip(NAMES_ROWS, WIDTHS)]


def unpack_early_kernel(tensors, flat, *refs):
    gains = len(refs) - len(tensors) - 8
    outs, norms, tiles, (stage, tail, in_sem, out_sem, tail_sem) = split(refs, (len(tensors), gains, 3, 5))
    tail_copy = pltpu.make_async_copy(flat.at[pl.ds(MATRIX_ROWS, TAIL), 0], tail, tail_sem)
    tail_copy.start()
    work = unpack_body([b for b in EARLY_BLOCKS if b[0] in tensors], flat, None, dict(zip(tensors, outs)), tiles, stage, in_sem, out_sem)
    next(work)
    tail_copy.wait()
    base = 0
    for n in norms:
        if n.ndim == 1:
            n[...] = jnp.concatenate([tail[base + j, :] for j in COLUMNS]).astype(BF16)
            continue
        for j in COLUMNS:
            lines = [tail[pl.ds(base + j + 7 * layer, 1), :] for layer in range(n.shape[0])]
            n[:, pl.ds(j * LANES, LANES)] = jnp.concatenate(lines, axis=0).astype(BF16)
        base += 7 * n.shape[0]
    for _ in work:
        pass


def unpack_early(flat, tensors, gains):
    return pl.pallas_call(
        functools.partial(unpack_early_kernel, tensors),
        name="unpack_early",
        out_shape=[TENSOR_TYPES[t] for t in tensors] + [jax.ShapeDtypeStruct(s, BF16) for s in gains],
        in_specs=[ANY],
        out_specs=[ANY] * len(tensors) + [VMEM_SPEC] * len(gains),
        scratch_shapes=UNPACK_SCRATCH + [pltpu.VMEM((TAIL, LANES), F32), DMA((SLOTS, 4)), DMA((SLOTS,)), DMA],
        compiler_params=pltpu.CompilerParams(vmem_limit_bytes=VMEM_LIMIT),
        cost_estimate=COST,
    )(flat)


def unpack_late_kernel(relations, flat, *refs):
    count = len(LATE_TENSORS)
    lates, _, outs, tiles, (stage, in_sem, out_sem) = split(refs, (2 * len(relations), count, count, 3, 3))
    lates = dict(zip(relations, zip(lates[::2], lates[1::2])))

    def wanted(b):
        seg = [source[0] for source, _, _, _ in LATE_BLOCKS[b][3] if source][0]
        relation = lax.bitwise_xor(lax.axis_index("dp"), seg)
        return jnp.logical_and(relation >= relations[0], relation <= relations[-1])

    for _ in unpack_body(LATE_BLOCKS, flat, lates, dict(zip(LATE_TENSORS, outs)), tiles, stage, in_sem, out_sem, wanted):
        pass


def unpack_late(flat, lates, params):
    count = len(LATE_TENSORS)
    relations = sorted(lates)
    lates = [a for r in relations for a in lates[r]]
    outs = pl.pallas_call(
        functools.partial(unpack_late_kernel, relations),
        name="unpack_late",
        out_shape=[TENSOR_TYPES[t] for t in LATE_TENSORS],
        in_specs=[ANY] * (1 + len(lates) + count),
        out_specs=[ANY] * count,
        input_output_aliases={1 + len(lates) + n: n for n in range(count)},
        scratch_shapes=UNPACK_SCRATCH + [DMA((SLOTS, 4)), DMA((SLOTS,))],
        compiler_params=pltpu.CompilerParams(vmem_limit_bytes=VMEM_LIMIT),
        cost_estimate=COST,
    )(flat, *lates, *[params[t] for t in LATE_TENSORS])
    return {**params, **dict(zip(LATE_TENSORS, outs))}


def neighbours():
    me = lax.axis_index("dp")
    core, x, y = lax.rem(me, 2), lax.rem(me // 2, 2), me // 4
    other = 1 - 2 * core
    step_x, step_y = 2 - 4 * x, 4 - 8 * y
    return me, other, me + step_x, me + step_y, me + step_x + step_y


CHUNKS = 16
RS_ROWS = 911
RS_HALF_START = SEG - CHUNKS * RS_ROWS
UNITS = 4
UNIT_CHUNKS = CHUNKS // UNITS
KIND_D, KIND_N, KIND_S, KIND_O = range(4)
CHIP_D, CHIP_X, CHIP_Y, CHIP_OWN = range(4)
UNIT_ROWS = UNIT_CHUNKS * RS_ROWS
MARGIN = 16 * 38
PACK_ROWS = {38: 112, 7: 608, 1: 896}
PACK_STAGE = 112 * 38
PACK_SLOTS = 3


def pack_blocks(chip, unit):
    blocks = []
    for parity in HALVES:
        for h in HALVES:
            begin = SEG * (2 * chip + parity) + RS_HALF_START * h + UNIT_ROWS * unit
            for t in TENSORS:
                w, offset, total = WIDTHS[t], OFFSETS[t], NAMES_ROWS[t]
                low, high = max(begin, offset), min(begin + UNIT_ROWS, offset + total * w)
                if low >= high:
                    continue
                first = (low - offset) // (16 * w) * 16
                end = -(-(high - offset) // (16 * w)) * 16
                step = -(-(end - first) // (16 * -(-(end - first) // PACK_ROWS[w]))) * 16
                for row in range(first, end, step):
                    blocks.append((t, row, min(step, end - row), parity, h, offset + row * w - begin + MARGIN))
    return blocks


def reduce_kernel(*refs):
    (grads, norms, (g_out, norm_out, flat, land_p, land_d, land_n),
     (mine, part, first, land_s, sums, g_buf, ss, ss_all), tiles, (stage, tail),
     (p_send, p_recv, i_send, i_recv, load_sem, g_sem, ss_send, ss_recv, in_sem, out_sem, tail_sem)) = split(refs, (7, 3, 6, 8, 3, 2, 11))
    me, other, dev_x, dev_y, _ = neighbours()
    core, x, y = lax.rem(me, 2), lax.rem(me // 2, 2), me // 4
    barrier = pltpu.get_barrier_semaphore()
    for d in range(1, NDEV):
        pl.semaphore_signal(barrier, inc=1, device_id=(lax.rem(me + d, NDEV),), device_id_type=MESH)

    tail[...] = jnp.zeros_like(tail)
    line = 0
    for n in norms:
        for layer in range(n.shape[0]):
            for j in COLUMNS:
                tail[pl.ds(line, 1), :] = n[pl.ds(layer, 1), pl.ds(j * LANES, LANES)].astype(F32)
                line += 1

    def pack(place, chip, unit):
        blocks = pack_blocks(chip, unit)

        def load(b):
            t, row, rows = blocks[b][:3]
            return pltpu.make_async_copy(grads[t].at[pl.ds(row, rows)], tiles[width_slot(WIDTHS[t])].at[b % PACK_SLOTS, pl.ds(0, rows)], in_sem.at[b % PACK_SLOTS])

        def store(b):
            t, _, rows, parity, h, to = blocks[b]
            size = rows * WIDTHS[t]
            return pltpu.make_async_copy(stage.at[b % PACK_SLOTS, pl.ds(0, size)], flat.at[place, unit, parity, h, pl.ds(to, size), 0], out_sem.at[b % PACK_SLOTS])

        for b in range(PACK_SLOTS):
            load(b).start()
        tail_copies = [pltpu.make_async_copy(tail, flat.at[place, unit, 1, 1, pl.ds(MARGIN + UNIT_ROWS - TAIL, TAIL), 0], tail_sem)
                       for _ in range(chip * unit // (3 * UNITS - 3))]
        for copy in tail_copies:
            copy.start()
        for b, block in enumerate(blocks):
            t, rows = block[0], block[2]
            w = WIDTHS[t]
            tile = tiles[width_slot(w)]
            group = row_group(rows, w)
            load(b).wait()
            if b >= PACK_SLOTS:
                store(b - PACK_SLOTS).wait()

            @pl.loop(0, rows // group)
            def _(i):
                for j in range(w):
                    values = tile[b % PACK_SLOTS, pl.ds(pl.multiple_of(i * group, 16), group), pl.ds(j * LANES, LANES)].astype(F32)
                    if w == 1:
                        stage[b % PACK_SLOTS, pl.ds(pl.multiple_of(i * group, 16), group), :] = values
                    else:
                        stage[b % PACK_SLOTS, pl.ds(i * (group * w) + j, group, stride=w), :] = values

            store(b).start()
            if b + PACK_SLOTS < len(blocks):
                load(b + PACK_SLOTS).start()
        for b in range(len(blocks) - PACK_SLOTS, len(blocks)):
            store(b).wait()
        for copy in tail_copies:
            copy.wait()

    def place_of(kind, h):
        return ((CHIP_D, CHIP_D), (CHIP_X, CHIP_Y), (CHIP_Y, CHIP_X), (CHIP_OWN, CHIP_OWN))[kind][h]

    def chunk(kind, h, i, parity):
        return flat.at[place_of(kind, h), i // UNIT_CHUNKS, parity, h, pl.ds(MARGIN + RS_ROWS * lax.rem(i, UNIT_CHUNKS), RS_ROWS)]

    def start_row(h, i):
        return RS_HALF_START * h + RS_ROWS * i

    def partner_copy(kind, h, i):
        return pltpu.make_async_remote_copy(
            src_ref=chunk(kind, h, i, 1 - core), dst_ref=land_p.at[kind, h, i],
            send_sem=p_send.at[kind, h, i], recv_sem=p_recv.at[kind, h, i],
            device_id=(me + other,), device_id_type=MESH)

    def link_copy(kind, h, i):
        land = land_s.at[h, i] if kind == KIND_S else (land_d, land_n)[kind].at[h, i, pl.ds(0, RS_ROWS), 0]
        to = ((dev_x, dev_y), (dev_x, dev_y), (dev_y, dev_x))[kind][h]
        return pltpu.make_async_remote_copy(
            src_ref=sums.at[kind % 2, h, i], dst_ref=land,
            send_sem=i_send.at[kind, h, i], recv_sem=i_recv.at[kind, h, i],
            device_id=(to,), device_id_type=MESH)

    def load_mine(kind, h, i):
        return pltpu.make_async_copy(chunk(kind, h, i, core).at[:, 0], mine.at[h], load_sem.at[0, h])

    def load_part(kind, h, i):
        return pltpu.make_async_copy(land_p.at[kind, h, i, pl.ds(0, RS_ROWS), 0], part.at[h], load_sem.at[1, h])

    def load_link(land, buf, n, h, i):
        return pltpu.make_async_copy(land.at[h, i, pl.ds(0, RS_ROWS), 0], buf.at[h], load_sem.at[n, h])

    def store_g(h, i):
        return pltpu.make_async_copy(g_buf.at[h], g_out.at[pl.ds(start_row(h, i), RS_ROWS), 0], g_sem.at[h])

    def exchange(kinds, begin, end):
        @pl.loop(begin, end)
        def _(i):
            for kind in kinds:
                for h in HALVES:
                    partner_copy(kind, h, i).start()

    def send(kind, begin, end):
        @pl.loop(begin, end)
        def _(i):
            for h in HALVES:
                load_mine(kind, h, i).start()
            for h in HALVES:
                partner_copy(kind, h, i).wait_recv()
                load_part(kind, h, i).start()
                if kind == KIND_S:
                    link_copy(KIND_D, h, i).wait_recv()
                    load_link(land_d, first, 2, h, i).start()
            for h in HALVES:
                load_mine(kind, h, i).wait()
                load_part(kind, h, i).wait()
                total = mine[h] + part[h]
                if kind == KIND_S:
                    load_link(land_d, first, 2, h, i).wait()
                    total = total + first[h]
                    link_copy(KIND_D, h, i).wait_send()
                sums[kind % 2, h, i] = total
                link_copy(kind, h, i).start()

    @pl.loop(0, 4 * UNITS)
    def _(n):
        place, unit = n // UNITS, lax.rem(n, UNITS)
        flip_x, flip_y = 1 - place // 2, 1 - lax.rem(place, 2)
        chip = (x + flip_x * (1 - 2 * x)) + 2 * (y + flip_y * (1 - 2 * y))
        for case in range(4 * UNITS):
            @pl.when(UNITS * chip + unit == case)
            def _():
                pack(place, case // UNITS, case % UNITS)

        @pl.when(n == 0)
        def _():
            pl.semaphore_wait(barrier, NDEV - 1)

        @pl.when(n < UNITS)
        def _():
            exchange((KIND_D,), UNIT_CHUNKS * unit, UNIT_CHUNKS * unit + UNIT_CHUNKS)
            send(KIND_D, UNIT_CHUNKS * unit, UNIT_CHUNKS * unit + UNIT_CHUNKS)

        @pl.when(n == 3 * UNITS - 1)
        def _():
            exchange((KIND_N, KIND_S), 0, CHUNKS)
            send(KIND_N, 0, CHUNKS)

    exchange((KIND_O,), 0, CHUNKS)
    send(KIND_S, 0, CHUNKS)

    def last(i, acc):
        for h in HALVES:
            for kind in (KIND_D, KIND_N, KIND_S):
                partner_copy(kind, h, i).wait_send()
            link_copy(KIND_N, h, i).wait_send()

            @pl.when(i > 0)
            def _():
                partner_copy(KIND_O, h, i - 1).wait_send()
                link_copy(KIND_S, h, i - 1).wait_send()

        for h in HALVES:
            load_mine(KIND_O, h, i).start()
            partner_copy(KIND_O, h, i).wait_recv()
            load_part(KIND_O, h, i).start()
        for h in HALVES:
            link_copy(KIND_N, h, i).wait_recv()
            load_link(land_n, first, 2, h, i).start()
        for h in HALVES:
            load_mine(KIND_O, h, i).wait()
            load_part(KIND_O, h, i).wait()
            load_link(land_n, first, 2, h, i).wait()
            link_copy(KIND_S, h, i).wait_recv()

            @pl.when(i > 0)
            def _():
                store_g(h, i - 1).wait()

            g = ((mine[h] + part[h]) + (first[h] + land_s[h, i])) * (1.0 / NDEV)
            g_buf[h] = g
            store_g(h, i).start()
            square = g * g
            if h == 1:
                row = lax.broadcasted_iota(jnp.int32, (RS_ROWS, LANES), 0) + RS_ROWS * i
                square = jnp.where(row >= CHUNKS * RS_ROWS - RS_HALF_START, square, 0.0)
            acc = acc + jnp.sum(square, axis=0, keepdims=True)
        return acc

    acc = lax.fori_loop(0, CHUNKS, last, jnp.zeros((1, LANES), F32))
    ss[...] = jnp.broadcast_to(acc, (8, LANES))

    for h in HALVES:
        partner_copy(KIND_O, h, CHUNKS - 1).wait_send()
        link_copy(KIND_S, h, CHUNKS - 1).wait_send()
    store_g(0, CHUNKS - 1).wait()

    def norm_copy(d):
        return pltpu.make_async_remote_copy(
            src_ref=ss, dst_ref=ss_all.at[d], send_sem=ss_send.at[d], recv_sem=ss_recv.at[d],
            device_id=(lax.rem(me + d, NDEV),), device_id_type=MESH)

    for d in range(1, NDEV):
        norm_copy(d).start()
    store_g(1, CHUNKS - 1).wait()
    ss_all[0] = ss[...]
    for d in range(1, NDEV):
        norm_copy(d).wait()
    total = jnp.zeros((8, LANES), F32)
    for dev in range(NDEV):
        total = total + ss_all[lax.rem(me - dev + NDEV, NDEV)]
    norm_out[...] = jnp.broadcast_to(jnp.sqrt(jnp.sum(total, axis=1, keepdims=True)), (8, LANES))


def reduce_grads(grads, norms):
    land = jax.ShapeDtypeStruct((2, CHUNKS, RS_ROWS, 1, LANES), F32)
    land_p = jax.ShapeDtypeStruct((4, 2, CHUNKS, RS_ROWS, 1, LANES), F32)
    flat = jax.ShapeDtypeStruct((4, UNITS, 2, 2, UNIT_ROWS + 2 * MARGIN, 1, LANES), F32)
    buf = pltpu.VMEM((2, RS_ROWS, LANES), F32)
    partner, link, pair, all_devs, slots = DMA((4, 2, CHUNKS)), DMA((3, 2, CHUNKS)), DMA((2,)), DMA((NDEV,)), DMA((PACK_SLOTS,))
    outs = pl.pallas_call(
        reduce_kernel,
        name="reduce_grads",
        out_shape=[jax.ShapeDtypeStruct((SEG, 1, LANES), F32), jax.ShapeDtypeStruct((8, LANES), F32), flat, land_p, land, land],
        in_specs=[ANY] * 7 + [VMEM_SPEC] * 3,
        out_specs=[ANY, VMEM_SPEC] + [ANY] * 4,
        scratch_shapes=[buf] * 3 + [pltpu.VMEM((2, CHUNKS, RS_ROWS, LANES), F32), pltpu.VMEM((2, 2, CHUNKS, RS_ROWS, LANES), F32), buf, pltpu.VMEM((8, LANES), F32), pltpu.VMEM((NDEV, 8, LANES), F32)]
        + tile_scratch(PACK_SLOTS, PACK_ROWS.values()) + [pltpu.VMEM((PACK_SLOTS, PACK_STAGE, LANES), F32), pltpu.VMEM((TAIL, LANES), F32)]
        + [partner, partner, link, link, DMA((4, 2)), pair, all_devs, all_devs, slots, slots, DMA],
        compiler_params=pltpu.CompilerParams(collective_id=0, has_side_effects=True, vmem_limit_bytes=VMEM_LIMIT),
        cost_estimate=COST,
    )(*grads, *norms)
    return outs[0], outs[1]


def adam_rows(g, m, v, p, norm_row, lr, decay):
    clip = jnp.minimum(1.0, MAX_NORM / (norm_row + CLIP_EPS))
    clipped = clip * g
    new_m = BETA_ONE * m + (1.0 - BETA_ONE) * clipped
    new_v = BETA_TWO * v + (1.0 - BETA_TWO) * clipped * clipped
    adam_dir = (new_m * (1.0 / BIAS_ONE)) / (jnp.sqrt(new_v * (1.0 / BIAS_TWO)) + ADAM_EPS)
    decay_term = jnp.where(decay, WEIGHT_DECAY * p, 0.0)
    return p - lr * (decay_term + adam_dir), new_m, new_v


STATE_ROWS = 912
STATE_COUNT = SEG // STATE_ROWS
STATE_LAST = SEG - STATE_COUNT * STATE_ROWS
STATE_SLOTS = 4
SUB = 152


def decay_rows(me, start, rows):
    return lax.broadcasted_iota(jnp.int32, (rows, LANES), 0) + (SEG * me + start) < MATRIX_ROWS


def gather_kernel(g, m, v, p, norm, lr, full, late_a, late_b, gb, mb, vb, pb, new_p, late_p,
                  load_sem, own_sem, late_sem, own_send, own_recv, fwd_send, fwd_recv, p_send, p_recv):
    me, other, dev_x, dev_y, dev_d = neighbours()
    partner = me + other
    barrier = pltpu.get_barrier_semaphore()
    for dev in (partner, dev_x, dev_y):
        pl.semaphore_signal(barrier, inc=1, device_id=(dev,), device_id_type=MESH)
    to = (dev_x, dev_y, partner)
    sources = (me, dev_x, dev_y, dev_d)

    def is_last(h, i):
        return h == 1 and isinstance(i, int) and i == HALF - 1

    def start_row(h, i):
        return PIECE * (PIECES - 1) if is_last(h, i) else PIECE * (HALF * h + i)

    def size(h, i):
        return PIECE_LAST if is_last(h, i) else PIECE

    def rows_of(dev, h, i):
        return full.at[pl.ds(SEG * dev + start_row(h, i), size(h, i)), 0]

    def loads(h, i):
        return loads_at(h, start_row(h, i), size(h, i))

    def loads_at(h, start, rows):
        start = pl.multiple_of(start, 8)
        copies = [pltpu.make_async_copy(g.at[pl.ds(start, rows), 0], gb.at[h, pl.ds(0, rows)], load_sem.at[0, h])]
        for n, (src, buf) in enumerate(((m, mb), (v, vb), (p, pb))):
            copies.append(pltpu.make_async_copy(src.at[pl.ds(start, rows)], buf.at[h, pl.ds(0, rows)], load_sem.at[n + 1, h]))
        return copies

    def own_copy(n, h, i):
        return pltpu.make_async_remote_copy(
            src_ref=new_p.at[h, i, pl.ds(0, size(h, i))], dst_ref=rows_of(me, h, i),
            send_sem=own_send.at[n, h, i], recv_sem=own_recv.at[n, h, i], device_id=(to[n],), device_id_type=MESH)

    def own_store(h, i):
        return pltpu.make_async_copy(new_p.at[h, i, pl.ds(0, size(h, i))], rows_of(me, h, i), own_sem.at[h, i])

    def forward(h, i):
        src = rows_of((dev_y, dev_x)[h], h, i)
        return pltpu.make_async_remote_copy(
            src_ref=src, dst_ref=src, send_sem=fwd_send.at[h, i], recv_sem=fwd_recv.at[h, i],
            device_id=((dev_x, dev_y)[h],), device_id_type=MESH)

    def arrival(n, h, i):
        src = rows_of((dev_x, dev_y, partner)[n], h, i)
        return pltpu.make_async_remote_copy(
            src_ref=src, dst_ref=src, send_sem=own_send.at[n, h, i], recv_sem=own_recv.at[n, h, i],
            device_id=(to[n],), device_id_type=MESH)

    def forward_arrival(h, i):
        src = rows_of(dev_d, h, i)
        return pltpu.make_async_remote_copy(
            src_ref=src, dst_ref=src, send_sem=fwd_send.at[h, i], recv_sem=fwd_recv.at[h, i],
            device_id=((dev_x, dev_y)[h],), device_id_type=MESH)

    def partner_copy(q, h, i):
        src = rows_of(sources[q], h, i)
        return pltpu.make_async_remote_copy(
            src_ref=src, dst_ref=src, send_sem=p_send.at[q - 1, h, i], recv_sem=p_recv.at[q - 1, h, i],
            device_id=(partner,), device_id_type=MESH)

    def partner_arrival(q, h, i):
        src = rows_of(sources[q] + other, h, i)
        return pltpu.make_async_remote_copy(
            src_ref=src, dst_ref=src, send_sem=p_send.at[q - 1, h, i], recv_sem=p_recv.at[q - 1, h, i],
            device_id=(partner,), device_id_type=MESH)

    def each(body):
        @pl.loop(0, HALF - 1)
        def _(i):
            body(i)

        body(HALF - 1)

    norm_row = norm[0:1, :]
    for h in HALVES:
        for copy in loads(h, 0):
            copy.start()
    pl.semaphore_wait(barrier, 3)

    def compute(h, out, first):
        @pl.loop(0, PIECE // SUB)
        def _(s):
            start = pl.multiple_of(s * SUB, 8)
            sub = pl.ds(start, SUB)
            out[sub] = adam_rows(gb[h, sub], mb[h, sub], vb[h, sub], pb[h, sub], norm_row, lr[0], decay_rows(me, first + start, SUB))[0]

    def update(i):
        for h in HALVES:
            for copy in loads(h, i):
                copy.wait()

            compute(h, new_p.at[h, i], start_row(h, i))
            for n in ((1, 0, 2) if h == 0 else (0, 1, 2)):
                own_copy(n, h, i).start()
            own_store(h, i).start()
            if isinstance(i, int):
                continue
            for last in (False, True):
                @pl.when((i == HALF - 2) == last)
                def _():
                    for copy in loads(h, HALF - 1 if last else i + 1):
                        copy.start()

    each(update)

    late_copies = []

    def late_store(src, row, rows, to):
        for out, start in zip((late_a, late_b), LATE_STARTS):
            low, high = max(to, start), min(to + rows, start + LATE_HALF)
            if low < high:
                late_copies.append(pltpu.make_async_copy(src.at[pl.ds(row + low - to, high - low)], out.at[pl.ds(low - start, high - low), 0], late_sem.at[len(late_copies)]))
                late_copies[-1].start()

    late_store(new_p.at[1, HALF - 2], PIECE - 8, 8, 0)
    late_store(new_p.at[1, HALF - 1], 0, 8, LATE_ROWS - 8)
    for j in range(LATE_END - LATE_FIRST):
        first = PIECE * (LATE_FIRST + j)
        for copy in loads_at(j % 2, first, PIECE):
            copy.start()
        for copy in loads_at(j % 2, first, PIECE):
            copy.wait()
        compute(j % 2, late_p.at[j], first)
        late_store(late_p.at[j], 0, PIECE, 8 + PIECE * j)

    def pass_on(i):
        arrival(1, 0, i).wait_recv()
        forward(0, i).start()
        partner_copy(2, 0, i).start()
        arrival(0, 1, i).wait_recv()
        forward(1, i).start()
        partner_copy(1, 1, i).start()
        arrival(0, 0, i).wait_recv()
        partner_copy(1, 0, i).start()
        arrival(1, 1, i).wait_recv()
        partner_copy(2, 1, i).start()

    each(pass_on)

    for copy in late_copies:
        copy.wait()

    def finish_own(i):
        for h in HALVES:
            own_store(h, i).wait()
            arrival(2, h, i).wait_recv()
            for n in range(3):
                own_copy(n, h, i).wait_send()

    each(finish_own)

    def finish(i):
        for h in HALVES:
            forward(h, i).wait_send()
            partner_copy(3, h, i).wait_send()
            partner_arrival(3, h, i).wait_recv()

    def pass_last(i):
        for h in HALVES:
            forward_arrival(h, i).wait_recv()
            partner_copy(3, h, i).start()
            for q in (1, 2):
                partner_copy(q, h, i).wait_send()
                partner_arrival(q, h, i).wait_recv()
        if isinstance(i, int):
            finish(i - 1)
        else:
            pl.when(i > 0)(lambda: finish(i - 1))

    each(pass_last)
    finish(HALF - 1)


def gather_params(g, m, v, p, norm, lr):
    buf = pltpu.VMEM((2, PIECE, LANES), F32)
    pairs = DMA((2, HALF))
    triples = DMA((3, 2, HALF))
    return pl.pallas_call(
        gather_kernel,
        name="gather_params",
        out_shape=[jax.ShapeDtypeStruct((FLAT_ROWS, 1, LANES), F32), jax.ShapeDtypeStruct((LATE_HALF, 1, LANES), F32), jax.ShapeDtypeStruct((LATE_HALF, 1, LANES), F32)],
        in_specs=[ANY] * 4 + [VMEM_SPEC, SMEM_SPEC],
        out_specs=[ANY] * 3,
        scratch_shapes=[buf, buf, buf, buf, pltpu.VMEM((2, HALF, PIECE, LANES), F32), pltpu.VMEM((LATE_END - LATE_FIRST, PIECE, LANES), F32),
                        DMA((4, 2)), pairs, DMA((LATE_END - LATE_FIRST + 4,)), triples, triples, pairs, pairs, triples, triples],
        compiler_params=pltpu.CompilerParams(collective_id=1, has_side_effects=True, vmem_limit_bytes=VMEM_LIMIT),
        cost_estimate=COST,
    )(g, m, v, p, norm, lr)


def state_kernel(g, m, v, p, norm, lr, new_p, new_m, new_v, norm_out, gb, mb, vb, pb, pn, mn, vn, in_sem, out_sem):
    me = lax.axis_index("dp")
    norm_row = norm[pl.ds(0, 1), :]
    norm_out[0] = jnp.max(norm[...])

    def window(i):
        rows = STATE_LAST if isinstance(i, int) and i == STATE_COUNT else STATE_ROWS
        slot = lax.rem(i, STATE_SLOTS)
        return slot, pl.ds(pl.multiple_of(i * STATE_ROWS, 8), rows), pl.ds(0, rows)

    def loads(i):
        slot, rows, size = window(i)
        pairs = ((g.at[rows, 0], gb), (m.at[rows], mb), (v.at[rows], vb), (p.at[rows], pb))
        return [pltpu.make_async_copy(src, buf.at[slot, size], in_sem.at[n, slot]) for n, (src, buf) in enumerate(pairs)]

    def stores(i):
        slot, rows, size = window(i)
        pairs = ((pn, new_p), (mn, new_m), (vn, new_v))
        return [pltpu.make_async_copy(buf.at[slot, size], dst.at[rows], out_sem.at[n, slot]) for n, (buf, dst) in enumerate(pairs)]

    def run(copies, wait=False):
        for copy in copies:
            copy.wait() if wait else copy.start()

    def compute(i):
        slot = lax.rem(i, STATE_SLOTS)

        @pl.loop(0, STATE_ROWS // SUB)
        def _(s):
            start = pl.multiple_of(s * SUB, 8)
            rows = pl.ds(start, SUB)
            pn[slot, rows], mn[slot, rows], vn[slot, rows] = adam_rows(
                gb[slot, rows], mb[slot, rows], vb[slot, rows], pb[slot, rows], norm_row, lr[0],
                decay_rows(me, i * STATE_ROWS + start, SUB))

    for i in range(STATE_SLOTS):
        run(loads(i))

    @pl.loop(0, STATE_COUNT)
    def _(i):
        run(loads(i), wait=True)

        @pl.when(i >= STATE_SLOTS)
        def _():
            run(stores(i - STATE_SLOTS), wait=True)

        compute(i)
        run(stores(i))

        @pl.when(i + STATE_SLOTS < STATE_COUNT)
        def _():
            run(loads(i + STATE_SLOTS))

        @pl.when(i + STATE_SLOTS == STATE_COUNT)
        def _():
            run(loads(STATE_COUNT))

    run(loads(STATE_COUNT), wait=True)
    run(stores(STATE_COUNT - STATE_SLOTS), wait=True)
    compute(STATE_COUNT)
    run(stores(STATE_COUNT))
    for n in range(STATE_SLOTS):
        run(stores(STATE_COUNT - STATE_SLOTS + 1 + n), wait=True)


def new_state(g, m, v, p, norm, lr):
    return pl.pallas_call(
        state_kernel,
        name="new_state",
        out_shape=[jax.ShapeDtypeStruct((SEG, LANES), F32)] * 3 + [jax.ShapeDtypeStruct((1,), F32)],
        in_specs=[ANY] * 4 + [VMEM_SPEC, SMEM_SPEC],
        out_specs=[ANY] * 3 + [SMEM_SPEC],
        scratch_shapes=[pltpu.VMEM((STATE_SLOTS, STATE_ROWS, LANES), F32)] * 7 + [DMA((4, STATE_SLOTS)), DMA((3, STATE_SLOTS))],
        compiler_params=pltpu.CompilerParams(vmem_limit_bytes=VMEM_LIMIT),
        cost_estimate=COST,
    )(g, m, v, p, norm, lr)


def solution(mesh):
    def local_step(*arrays):
        grads = [a.reshape(r, w * LANES) for a, r, w in zip(arrays[:7], NAMES_ROWS, WIDTHS)]
        norms = [a.reshape(s) for a, s in zip(arrays[7:10], GAINS)]
        master, exp_avg, exp_avg_sq = [a.reshape(SEG, LANES) for a in arrays[10:13]]
        lr = arrays[13].reshape(1)
        g, norm = reduce_grads(grads, norms)
        full, *late = gather_params(g, exp_avg, exp_avg_sq, master, norm, lr)

        def permute(a, bits):
            return lax.ppermute(a, "dp", [(d, d ^ bits) for d in range(NDEV)])

        by_y, by_x = permute(late[0], 4), permute(late[1], 2)
        far_x, far_y = permute(late[0], 2), permute(late[1], 4)
        own = [permute(a, 1) for a in late]
        state = list(new_state(g, exp_avg, exp_avg_sq, master, norm, lr))
        by_y, by_x, full, state[0] = lax.optimization_barrier((by_y, by_x, full, state[0]))
        across_y = permute(by_y, 2)
        across_x = permute(by_x, 4)
        across = across_y, across_x
        from_y, from_x = permute(by_y, 1), permute(by_x, 1)
        wide, down, small = (4, 5), (3, 6), (0, 1, 2)
        params = dict(zip(wide, unpack_early(full, wide, [])))
        far_x, far_y, full, params[4] = lax.optimization_barrier((far_x, far_y, full, params[4]))
        far = permute(far_x, 1), permute(far_y, 1)
        params |= dict(zip(down, unpack_early(full, down, [])))
        lates = dict(enumerate([late, own, (far_x, by_x), (far[0], from_x), (by_y, far_y), (from_y, far[1])]))
        params = unpack_late(full, lates, params)
        *across, full, params[6] = lax.optimization_barrier((*across, full, params[6]))
        from_across = [permute(a, 1) for a in across]
        rest = list(unpack_early(full, small, GAINS[:2] + [(D,)]))
        params |= dict(zip(small, rest))
        params = unpack_late(full, {6: across, 7: from_across}, params)
        params = [params[t] for t in TENSORS] + rest[len(small):]
        shapes = SHAPES + GAINS[:2] + [(D,)]
        return tuple([a.reshape(-1) for a in state[:3]] + [a.reshape(s) for a, s in zip(params, shapes)] + [state[3].reshape(())])

    return jax.shard_map(local_step, mesh=mesh, in_specs=(P("dp"),) * 13 + (P(),), out_specs=(P("dp"),) * 3 + (P(),) * 11, check_vma=False)
```
